128 devices in a mesh: patch: 128 (over x, z, y, core).
Axes of the slice: x: 4, y: 4, z: 4, core: 2. Of those that a mesh axis runs over, the one named last changes fastest.
Arguments:
- atm_flux: bfloat16 [8, 393216], P(None, 'patch'), may hold values from -6 to 6
- remap_send: int32 [128, 5, 8], P('patch'), may hold values from 0 to 23
- remap_target: int32 [128, 5, 8], P('patch'), may hold values from 0 to 31
- remap_counts: int32 [128, 5], P('patch'), may hold values from 0 to 8, as said below
- remap_weights: bfloat16 [128, 5, 8, 128, 128], P('patch'), may hold values from -0.5 to 0.5
- coupling: float32 [2, 8], replicated, may hold values from -2 to 2
- tracer: float32 [2, 128, 524288], P(None, None, 'patch'), may hold values from -6 to 6
- wet: int32 [524288], P('patch'), may hold values from 0 to 1
- mix_inverse: float32 [4096, 128, 128], P('patch')
- halo_send: int32 [128, 4, 2, 128], P('patch'), may hold values from 0 to 4095
- halo_ghost: int32 [128, 4, 2, 128], P('patch'), may hold values from 0 to 4095
- halo_rows: int32 [128, 4], P('patch'), may hold values from 0 to 2, as said below
Outputs:
- ocean_flux: float32 [8, 524288], P(None, 'patch')
- tracer_out: float32 [2, 128, 524288], P(None, None, 'patch')
The draws below stay inside these ranges and needn't reach their ends.
Inputs may be any that keep to these rules, and one draw needn't show every extreme that they name: `remap_counts`: some entry equals 8. `halo_rows`: some entry equals 2.
All inputs are finite; a program needn't handle non-finite values.
Results may differ from the reference program's by a relative error of at most 0.0003.
Values may be sent and summed in bfloat16 or wider, within the bound.
A program may use at most 64 MiB of HBM per device.

```python
import math
import jax
import jax.numpy as jnp
from jax import lax

F = 8
LEV = 128
NTR = 2
BLOCK = 128
ABLK = 24
OBLK = 32
CAP = 8
REACH = 2
HR = 2
SPAN = 5
HSPAN = 4
OC = 4096
NOC = 524288
NA = 393216
N_PATCH = 128


def force_top(key, rows, columns, top):
    counts = jax.random.randint(jax.random.fold_in(key, 21), (rows * columns,), 0, top + 1)
    spot = jax.random.randint(jax.random.fold_in(key, 22), (), 0, rows * columns)
    counts = jnp.where(jnp.arange(rows * columns) == spot, top, counts)
    return counts.reshape(rows, columns).astype(jnp.int32)


def draw_remap_counts(key, part):
    return force_top(jax.random.fold_in(key, 31), N_PATCH, SPAN, CAP)


def draw_halo_rows(key, part):
    return force_top(jax.random.fold_in(key, 41), N_PATCH, HSPAN, HR)


def draw_wet(key, part):
    percent = jax.random.randint(jax.random.fold_in(key, 51), (N_PATCH, 1), 30, 96)
    rolled = jax.random.randint(jax.random.fold_in(key, 52), (N_PATCH, OBLK * BLOCK), 0, 100)
    return (rolled < percent).astype(jnp.int32).reshape(-1)


def draw_mix_inverse(key, part):
    count = N_PATCH * OBLK
    diag = jax.random.uniform(jax.random.fold_in(key, 61), (count, LEV, 1), jnp.float32, 0.6, 1.4)
    eye = jnp.eye(LEV, dtype=jnp.float32)[None, :, :]
    spread = 0.5 * jax.random.normal(jax.random.fold_in(key, 63), (count, LEV, LEV), jnp.float32)
    return (eye * diag + spread / math.sqrt(LEV)).astype(jnp.float32)


def plant(values, stream_key, low, largest):
    longest = values.shape.index(max(values.shape))
    spots = []
    for shift in (0, 1):
        where = [jax.random.randint(jax.random.fold_in(stream_key, axis), (), 0, length) for axis, length in enumerate(values.shape)]
        where[longest] = (where[longest] + shift) % values.shape[longest]
        spots.append(tuple(where))
    return values.at[spots[0]].set(low).at[spots[1]].set(largest)


def block_scale(own_key, extent, cuts, low, largest):
    loudness = 1.0
    for axis_at, shards_of in cuts:
        draws = jax.random.uniform(jax.random.fold_in(jax.random.fold_in(own_key, 6), axis_at), (shards_of,), jnp.float32, low / len(cuts), largest / len(cuts))
        loudness = loudness * jnp.repeat(jnp.exp(draws), extent[axis_at] // shards_of).reshape((-1,) + (1,) * (len(extent) - 1 - axis_at))
    return loudness


def centred(rng, shape, width, limit, split=(), kind=jnp.bfloat16):
    gain = block_scale(rng, shape, split, -0.22, 0.18) if split else 1.0
    drawn = jax.random.normal(rng, shape, jnp.float32) * width * gain
    return jnp.minimum(jnp.maximum(drawn, -limit), limit).astype(kind)


def setup_inputs(seed: int = 0) -> dict:
    key_of = jax.random.split(jax.random.key(seed), 13)
    atm_flux = centred(key_of[0], (F, NA), 1.0, 6.0, ((1, 128),))
    remap_send = plant(jax.random.randint(key_of[1], (N_PATCH, SPAN, CAP), 0, ABLK), jax.random.fold_in(key_of[1], 1), 0, ABLK - 1).astype(jnp.int32)
    remap_target = plant(jax.random.randint(key_of[2], (N_PATCH, SPAN, CAP), 0, OBLK), jax.random.fold_in(key_of[2], 1), 0, OBLK - 1).astype(jnp.int32)
    remap_counts = draw_remap_counts(jax.random.fold_in(key_of[12], 71), 0)
    remap_weights = centred(key_of[4], (N_PATCH, SPAN, CAP, BLOCK, BLOCK), BLOCK ** -0.5, 0.5, ((0, 128),))
    coupling = centred(key_of[5], (NTR, F), F ** -0.5, 2.0, (), jnp.float32)
    tracer = centred(key_of[6], (NTR, LEV, NOC), 1.0, 6.0, ((2, 128),), jnp.float32)
    wet = draw_wet(jax.random.fold_in(key_of[12], 71), 0)
    mix_inverse = draw_mix_inverse(jax.random.fold_in(key_of[12], 71), 0)
    halo_send = plant(jax.random.randint(key_of[9], (N_PATCH, HSPAN, HR, BLOCK), 0, OC), jax.random.fold_in(key_of[9], 1), 0, OC - 1).astype(jnp.int32)
    halo_ghost = plant(jax.random.randint(key_of[10], (N_PATCH, HSPAN, HR, BLOCK), 0, OC), jax.random.fold_in(key_of[10], 1), 0, OC - 1).astype(jnp.int32)
    halo_rows = draw_halo_rows(jax.random.fold_in(key_of[12], 71), 0)
    return dict(atm_flux=atm_flux, remap_send=remap_send, remap_target=remap_target, remap_counts=remap_counts, remap_weights=remap_weights, coupling=coupling, tracer=tracer, wet=wet, mix_inverse=mix_inverse, halo_send=halo_send, halo_ghost=halo_ghost, halo_rows=halo_rows)


def reference(atm_flux, remap_send, remap_target, remap_counts, remap_weights, coupling, tracer, wet, mix_inverse, halo_send, halo_ghost, halo_rows):
    wetf = wet.astype(jnp.float32)
    offsets = jnp.arange(SPAN, dtype=jnp.int32) - REACH
    blocks = atm_flux.reshape(F, N_PATCH * ABLK, BLOCK)

    def receive(ocean):
        source = (ocean - offsets) % N_PATCH
        global_id = source[:, None] * ABLK + remap_send[source, jnp.arange(SPAN, dtype=jnp.int32)]
        pieces = blocks[:, global_id].astype(jnp.float32)
        in_use = (jnp.arange(CAP, dtype=jnp.int32)[None, :] < remap_counts[ocean][:, None]).astype(jnp.float32)
        contrib = jnp.einsum("fdci,dcij->dcfj", pieces, remap_weights[ocean].astype(jnp.float32), precision=lax.Precision.HIGHEST)
        contrib = contrib * in_use[:, :, None, None]
        table = (remap_target[ocean][..., None] == jnp.arange(OBLK, dtype=jnp.int32)).astype(jnp.float32)
        return jnp.einsum("dcb,dcfj->fbj", table, contrib, precision=lax.Precision.HIGHEST).reshape(F, OBLK * BLOCK)

    flux = lax.map(receive, jnp.arange(N_PATCH, dtype=jnp.int32))
    ocean_flux = jnp.transpose(flux, (1, 0, 2)).reshape(F, NOC) * wetf
    surface = jnp.dot(coupling, ocean_flux, precision=lax.Precision.HIGHEST)
    rhs = tracer.at[:, 0, :].add(surface)
    shaped = rhs.reshape(NTR, LEV, N_PATCH * OBLK, BLOCK)
    solved = jnp.einsum("blk,tkbc->tlbc", mix_inverse, shaped, precision=lax.Precision.HIGHEST).reshape(NTR, LEV, NOC)
    mixed = wetf * solved + (1.0 - wetf) * tracer
    sent = mixed.astype(jnp.bfloat16)
    halo_offsets = jnp.concatenate([jnp.arange(-REACH, 0, dtype=jnp.int32), jnp.arange(1, REACH + 1, dtype=jnp.int32)])
    ocean_ids = jnp.arange(N_PATCH, dtype=jnp.int32)[:, None]
    source = (ocean_ids - halo_offsets[None, :]) % N_PATCH
    source_cells = halo_send[source, jnp.arange(HSPAN, dtype=jnp.int32)[None, :]]
    source_glob = source[:, :, None, None] * OC + source_cells
    target_glob = ocean_ids[:, :, None, None] * OC + halo_ghost
    in_use = (jnp.arange(HR, dtype=jnp.int32)[None, None, :] < halo_rows[:, :, None]).astype(jnp.float32)
    values = sent[:, :, source_glob].astype(jnp.float32)
    current = mixed[:, :, target_glob]
    weight = in_use[..., None] * wetf[target_glob]
    increment = 0.25 * (values - current) * weight
    tracer_out = mixed.at[:, :, target_glob].add(increment)
    return ocean_flux, tracer_out
```

```python
import functools

import jax
import jax.numpy as jnp
from jax import lax
from jax.experimental import pallas as pl
from jax.experimental.pallas import tpu as pltpu
from jax.sharding import PartitionSpec as P

F = 8
LEV = 128
NTR = 2
BLK = 128
ABLK = 24
OBLK = 32
CAP = 8
SPAN = 5
HSPAN = 4
OC = 4096
CHUNKS = 8
PER = OBLK // CHUNKS
FLUX_OFFSETS = (-2, -1, 0, 1, 2)
HALO_OFFSETS = (-2, -1, 1, 2)
HALO_ORDER = (3, 0, 2, 1)
MESH = pl.DeviceIdType.MESH
f32 = jnp.float32
bf16 = jnp.bfloat16


def split2(v):
    hi = v.astype(bf16)
    lo = (v - hi.astype(f32)).astype(bf16)
    return hi, lo


def split3(v):
    hi, rest = v.astype(bf16), None
    rest = v - hi.astype(f32)
    mid = rest.astype(bf16)
    low = (rest - mid.astype(f32)).astype(bf16)
    return hi, mid, low


def couple(
    size,
    send_s, tgt_s, cnt_s, coup_s, atm_v, hs_v, wet_v, tracer_h, mix_h, w_h,
    mixed_o, v_o, of_o,
    x, m, w, blocks, outg, arr, contrib, ofs, surf, sent, onehot, hout, v,
    xsem, msem, wsem, osem, fs, fr, hsend, hrecv, vsem,
):
    me = lax.axis_index("patch")

    def at(offset):
        return lax.rem(me + (offset + size), size)

    barrier = pltpu.get_barrier_semaphore()
    for offset in HALO_OFFSETS:
        pl.semaphore_signal(barrier, inc=1, device_id=(at(offset),), device_id_type=MESH)

    def xcopy(i):
        cols = pl.ds(pl.multiple_of(i * (PER * BLK), PER * BLK), PER * BLK)
        return pltpu.make_async_copy(tracer_h.at[:, :, cols], x.at[:, :, cols], xsem.at[i])

    def mcopy(i):
        rows = pl.ds(i * PER, PER)
        return pltpu.make_async_copy(mix_h.at[rows], m.at[rows], msem.at[i])

    wcopy = pltpu.make_async_copy(w_h, w, wsem)
    for i in range(CHUNKS):
        xcopy(i).start()
        mcopy(i).start()
    wcopy.start()

    slots = SPAN * CAP
    row40 = lax.broadcasted_iota(jnp.int32, (slots, BLK), 0)
    lane40 = lax.broadcasted_iota(jnp.int32, (slots, BLK), 1)
    want = jnp.full((slots, BLK), -1, jnp.int32)
    for d in range(SPAN):
        for c in range(CAP):
            want = jnp.where(row40 == d * CAP + c, send_s[d, 0, c], want)
    chooser = jnp.where(want == lane40, 1.0, 0.0).astype(bf16)[:, :32]
    for a in range(ABLK):
        blocks[a * F : (a + 1) * F, :] = atm_v[:, a * BLK : (a + 1) * BLK].astype(f32)
    blocks[ABLK * F :, :] = jnp.zeros(((32 - ABLK) * F, BLK), f32)
    for k in range(F // 2):
        pair = jnp.concatenate(
            [blocks[pl.ds(2 * k, 32, stride=F), :], blocks[pl.ds(2 * k + 1, 32, stride=F), :]],
            axis=1,
        )
        chosen = jnp.dot(chooser, pair.astype(bf16), preferred_element_type=f32)
        for q in range(2):
            contrib[pl.ds(2 * k + q, slots, stride=F), :] = chosen[:, q * BLK : (q + 1) * BLK]
    for d in range(SPAN):
        rows = contrib[d * CAP * F : (d + 1) * CAP * F, :].astype(bf16)
        if FLUX_OFFSETS[d] == 0:
            arr[d] = rows
        else:
            outg[d] = rows

    pl.semaphore_wait(barrier, len(HALO_OFFSETS))

    flux = []
    for d in range(SPAN):
        if FLUX_OFFSETS[d] != 0:
            copy = pltpu.make_async_remote_copy(
                src_ref=outg.at[d], dst_ref=arr.at[d], send_sem=fs.at[d], recv_sem=fr.at[d],
                device_id=(at(FLUX_OFFSETS[d]),), device_id_type=MESH,
            )
            copy.start()
            flux.append(copy)

    def solve(i, carry):
        xcopy(i).wait()
        mcopy(i).wait()
        for j in range(PER):
            b = i * PER + j
            cols = pl.ds(pl.multiple_of(b * BLK, BLK), BLK)
            a1, a2 = split2(m[b])
            t = jnp.concatenate([x[0, :, cols], x[1, :, cols]], axis=1)
            b1, b2 = split2(t)
            lhs = jnp.concatenate(
                [jnp.concatenate([a1, a1], axis=1), jnp.concatenate([a2, a2], axis=1)], axis=0
            )
            rhs = jnp.concatenate([b1, b2], axis=0)
            both = jnp.dot(lhs, rhs, preferred_element_type=f32)
            solved = both[:LEV] + both[LEV:]
            row = wet_v[pl.ds(b, 1), :]
            wet = jnp.concatenate([row, row], axis=1) > 0
            base = jnp.where(wet, solved, t)
            x[0, :, cols] = base[:, :BLK]
            x[1, :, cols] = base[:, BLK:]
        return carry

    lax.fori_loop(0, CHUNKS, solve, 0)

    sub = lax.broadcasted_iota(jnp.int32, (BLK, 2 * BLK), 0)
    lows, highs = [], []
    for h in range(HSPAN):
        row = jnp.concatenate([hs_v[2 * h : 2 * h + 1, :], hs_v[2 * h + 1 : 2 * h + 2, :]], axis=1)
        lows.append(jnp.where(sub == (row % BLK), 1.0, 0.0).astype(bf16))
        highs.append(jnp.broadcast_to((row // BLK).astype(f32), (BLK, 2 * BLK)).astype(bf16))
    for h in range(HSPAN):
        def table(b, carry, low=lows[h], high=highs[h], h=h):
            here = high == lax.convert_element_type(b, f32).astype(bf16)
            rows = pl.ds(pl.multiple_of(b * BLK, BLK), BLK)
            onehot[h, rows, :] = jnp.where(here, low, jnp.zeros_like(low))
            return carry

        lax.fori_loop(0, OBLK, table, 0)

    lane = lax.broadcasted_iota(jnp.int32, (OBLK, BLK), 1)
    block = lax.broadcasted_iota(jnp.int32, (OBLK, BLK), 0)
    target = jnp.full((OBLK, BLK), -1, jnp.int32)
    used = jnp.zeros((OBLK, BLK), jnp.int32)
    for d in range(SPAN):
        used = jnp.where(lane // CAP == d, cnt_s[0, d], used)
        for c in range(CAP):
            target = jnp.where(lane == d * CAP + c, tgt_s[d, 0, c], target)
    here = (target == block) & (lane % CAP < used)
    place = jnp.where(here, 1.0, 0.0).astype(bf16)[:, :48]
    contrib[320:384, :] = jnp.zeros((64, BLK), f32)

    wcopy.wait()
    for copy in flux:
        copy.wait_recv()

    slot = lax.broadcasted_iota(jnp.int32, (32, BLK), 0) // F
    for d in range(SPAN):
        for g in range(2):
            c = 4 * g
            pieces = arr[d, c * F : (c + 4) * F, :].astype(f32)
            even = jnp.where(slot % 2 == 0, pieces, 0.0)
            odd = jnp.where(slot % 2 == 1, pieces, 0.0)
            lhs = jnp.concatenate([even, odd], axis=1).astype(bf16)
            rhs = jnp.concatenate(
                [
                    jnp.concatenate([w[d, c], w[d, c + 2]], axis=1),
                    jnp.concatenate([w[d, c + 1], w[d, c + 3]], axis=1),
                ],
                axis=0,
            )
            both = jnp.dot(lhs, rhs, preferred_element_type=f32)
            contrib[(d * CAP + c) * F : (d * CAP + c + 4) * F, :] = jnp.where(
                slot < 2, both[:, :BLK], both[:, BLK:]
            )

    wetf = wet_v[...].astype(f32)
    acc = [jnp.zeros((OBLK, BLK), f32) for _ in range(NTR)]
    for k in range(F // 2):
        pair = jnp.concatenate(
            [contrib[pl.ds(2 * k, 48, stride=F), :], contrib[pl.ds(2 * k + 1, 48, stride=F), :]],
            axis=1,
        )
        c1, c2, c3 = split3(pair)
        total = jnp.dot(place, c1, preferred_element_type=f32)
        total = total + jnp.dot(place, c2, preferred_element_type=f32)
        total = total + jnp.dot(place, c3, preferred_element_type=f32)
        for q in range(2):
            f = 2 * k + q
            flux_f = total[:, q * BLK : (q + 1) * BLK] * wetf
            ofs[pl.ds(f, OBLK, stride=F), :] = flux_f
            for t in range(NTR):
                acc[t] = acc[t] + coup_s[t, f] * flux_f
    for t in range(NTR):
        surf[t] = acc[t]

    def correct(b, carry):
        cols = pl.ds(pl.multiple_of(b * BLK, BLK), BLK)
        first = jnp.broadcast_to(m[b, :, 0:1], (LEV, BLK))
        for t in range(NTR):
            full = x[t, :, cols] + first * surf[t, pl.ds(b, 1), :]
            x[t, :, cols] = full
            sent[t * LEV : (t + 1) * LEV, cols] = full.astype(bf16)
        return carry

    lax.fori_loop(0, OBLK, correct, 0)

    halo = []
    for h in HALO_ORDER:
        picked = jnp.dot(sent[...], onehot[h], preferred_element_type=f32)
        hout[h] = picked.astype(bf16)
        copy = pltpu.make_async_remote_copy(
            src_ref=hout.at[h], dst_ref=v.at[h], send_sem=hsend.at[h], recv_sem=hrecv.at[h],
            device_id=(at(HALO_OFFSETS[h]),), device_id_type=MESH,
        )
        copy.start()
        halo.append(copy)

    done = [pltpu.make_async_copy(x, mixed_o, osem.at[0]), pltpu.make_async_copy(ofs, of_o, osem.at[1])]
    for copy in done:
        copy.start()
    for h, copy in zip(HALO_ORDER, halo):
        copy.wait_recv()
        out = pltpu.make_async_copy(v.at[h], v_o.at[h], vsem.at[h])
        out.start()
        done.append(out)
    for copy in flux:
        copy.wait_send()
    for copy in halo:
        copy.wait_send()
    for copy in done:
        copy.wait()


COLS = 512


def scatter(rows_s, ghost_v, wet_v, v_v, mixed_v, of_v, flux_o, out_o, table):
    blocks = COLS // BLK
    base = pl.program_id(0) * blocks
    sub = lax.broadcasted_iota(jnp.int32, (BLK, BLK), 0)
    for p in range(2 * HSPAN):
        row = ghost_v[p : p + 1, :]
        used = (p % 2) < rows_s[0, p // 2]
        row = jnp.where(used, row, -1)
        low = jnp.where(sub == (row & (BLK - 1)), 1.0, 0.0)
        high = jnp.broadcast_to(row >> 7, (BLK, BLK))
        for j in range(blocks):
            table[j * BLK : (j + 1) * BLK, p * BLK : (p + 1) * BLK] = jnp.where(
                high == base + j, low, 0.0
            ).astype(bf16)
    ones = jnp.ones((16, 2 * BLK * HSPAN), bf16)
    values = jnp.concatenate([v_v[h] for h in range(HSPAN)], axis=1)
    lhs = jnp.concatenate([values, ones], axis=0)
    total = lax.dot_general(
        lhs, table[...], (((1,), (1,)), ((), ())), preferred_element_type=f32
    )
    rows = pl.ds(pl.multiple_of(base, blocks), blocks)
    quarter = 0.25 * wet_v[rows, :].astype(f32)
    weight = jnp.concatenate([quarter[j : j + 1, :] for j in range(blocks)], axis=1)
    count = total[NTR * LEV : NTR * LEV + 1, :]
    for t in range(NTR):
        mixed = mixed_v[t]
        out_o[t] = mixed + weight * (total[t * LEV : (t + 1) * LEV] - count * mixed)
    for j in range(blocks):
        flux_o[:, j * BLK : (j + 1) * BLK] = of_v[j * F : (j + 1) * F, :]


def body(
    atm_flux, remap_send, remap_target, remap_counts, remap_weights, coupling,
    tracer, wet, mix_inverse, halo_send, halo_ghost, halo_rows,
):
    size = lax.axis_size("patch")
    wet2 = wet.reshape(OBLK, BLK)
    sends = halo_send.reshape(2 * HSPAN, BLK)
    ghosts = halo_ghost.reshape(2 * HSPAN, BLK)
    weights = remap_weights.reshape(SPAN, CAP, BLK, BLK)
    smem = pl.BlockSpec(memory_space=pltpu.SMEM)
    vmem = pl.BlockSpec(memory_space=pltpu.VMEM)
    hbm = pl.BlockSpec(memory_space=pltpu.HBM)
    dma = pltpu.SemaphoreType.DMA
    mixed, values, flux = pl.pallas_call(
        functools.partial(couple, size),
        name="couple",
        out_shape=(
            jax.ShapeDtypeStruct((NTR, LEV, OC), f32),
            jax.ShapeDtypeStruct((HSPAN, NTR * LEV, 2 * BLK), bf16),
            jax.ShapeDtypeStruct((OBLK * F, BLK), f32),
        ),
        in_specs=[smem] * 4 + [vmem] * 3 + [hbm] * 3,
        out_specs=(hbm, hbm, hbm),
        scratch_shapes=[
            pltpu.VMEM((NTR, LEV, OC), f32),
            pltpu.VMEM((OBLK, LEV, LEV), f32),
            pltpu.VMEM((SPAN, CAP, BLK, BLK), bf16),
            pltpu.VMEM((32 * F, BLK), f32),
            pltpu.VMEM((SPAN, CAP * F, BLK), bf16),
            pltpu.VMEM((SPAN, CAP * F, BLK), bf16),
            pltpu.VMEM((48 * F, BLK), f32),
            pltpu.VMEM((OBLK * F, BLK), f32),
            pltpu.VMEM((NTR, OBLK, BLK), f32),
            pltpu.VMEM((NTR * LEV, OC), bf16),
            pltpu.VMEM((HSPAN, OC, 2 * BLK), bf16),
            pltpu.VMEM((HSPAN, NTR * LEV, 2 * BLK), bf16),
            pltpu.VMEM((HSPAN, NTR * LEV, 2 * BLK), bf16),
            dma((CHUNKS,)), dma((CHUNKS,)), dma(()), dma((2,)),
            dma((SPAN,)), dma((SPAN,)), dma((HSPAN,)), dma((HSPAN,)), dma((HSPAN,)),
        ],
        compiler_params=pltpu.CompilerParams(
            collective_id=0, has_side_effects=True, vmem_limit_bytes=67043328
        ),
    )(
        jnp.transpose(remap_send, (1, 0, 2)), jnp.transpose(remap_target, (1, 0, 2)),
        remap_counts, coupling, atm_flux, sends, wet2,
        tracer, mix_inverse, weights,
    )
    whole = lambda shape: pl.BlockSpec(shape, lambda i: (0,) * len(shape))
    return pl.pallas_call(
        scatter,
        name="scatter",
        grid=(OC // COLS,),
        out_shape=(
            jax.ShapeDtypeStruct((F, OC), f32),
            jax.ShapeDtypeStruct((NTR, LEV, OC), f32),
        ),
        in_specs=[
            smem,
            whole((2 * HSPAN, BLK)),
            whole((OBLK, BLK)),
            whole((HSPAN, NTR * LEV, 2 * BLK)),
            pl.BlockSpec((NTR, LEV, COLS), lambda i: (0, 0, i)),
            pl.BlockSpec((COLS // BLK * F, BLK), lambda i: (i, 0)),
        ],
        out_specs=(
            pl.BlockSpec((F, COLS), lambda i: (0, i)),
            pl.BlockSpec((NTR, LEV, COLS), lambda i: (0, 0, i)),
        ),
        scratch_shapes=[pltpu.VMEM((COLS, 2 * BLK * HSPAN), bf16)],
        compiler_params=pltpu.CompilerParams(vmem_limit_bytes=67043328),
    )(halo_rows, ghosts, wet2, values, mixed, flux)


def solution(mesh):
    return jax.shard_map(
        body,
        mesh=mesh,
        in_specs=(
            P(None, "patch"),
            P("patch", None, None),
            P("patch", None, None),
            P("patch", None),
            P("patch", None, None, None, None),
            P(),
            P(None, None, "patch"),
            P("patch"),
            P("patch", None, None),
            P("patch", None, None, None),
            P("patch", None, None, None),
            P("patch", None),
        ),
        out_specs=(P(None, "patch"), P(None, None, "patch")),
        check_vma=False,
    )
```

```python
import functools

import jax
import jax.numpy as jnp
from jax import lax
from jax.experimental import pallas as pl
from jax.experimental.pallas import tpu as pltpu
from jax.sharding import PartitionSpec as P

F = 8
LEV = 128
NTR = 2
BLK = 128
ABLK = 24
OBLK = 32
CAP = 8
SPAN = 5
HSPAN = 4
OC = 4096
PER = 4
FLUX_OFFSETS = (-2, -1, 0, 1, 2)
HALO_OFFSETS = (-2, -1, 1, 2)
HALO_ORDER = (3, 0, 2, 1)
MESH = pl.DeviceIdType.MESH
f32 = jnp.float32
bf16 = jnp.bfloat16


def split2(v):
    hi = v.astype(bf16)
    lo = (v - hi.astype(f32)).astype(bf16)
    return hi, lo


def split3(v):
    hi, rest = v.astype(bf16), None
    rest = v - hi.astype(f32)
    mid = rest.astype(bf16)
    low = (rest - mid.astype(f32)).astype(bf16)
    return hi, mid, low


def couple(
    size,
    send_s, tgt_s, cnt_s, coup_s, rows_s, atm_v, hs_v, hg_v, wet_v, tracer_h, mix_h, w_h,
    x, ofs, last_v, last_low, last_high, quarter_o,
    m, w, blocks, outg, arr, contrib, surf, scale, sent, low_t, high_t, hout, v,
    xsem, msem, wsem, fs, fr, hsend, hrecv,
):
    me = lax.axis_index("patch")

    def at(offset):
        return lax.rem(me + (offset + size), size)

    barrier = pltpu.get_barrier_semaphore()
    for offset in HALO_OFFSETS:
        pl.semaphore_signal(barrier, inc=1, device_id=(at(offset),), device_id_type=MESH)

    def xcopy(b, t):
        cols = pl.ds(pl.multiple_of(b * BLK, BLK), BLK)
        return pltpu.make_async_copy(tracer_h.at[t, :, cols], x.at[b, t], xsem.at[b, t])

    def mcopy(i):
        rows = pl.ds(i * PER, PER)
        return pltpu.make_async_copy(mix_h.at[rows], m.at[rows], msem.at[i])

    wcopy = pltpu.make_async_copy(w_h, w, wsem)
    for i in range(OBLK // PER):
        mcopy(i).start()
        for b in range(i * PER, (i + 1) * PER):
            for t in range(NTR):
                xcopy(b, t).start()
    wcopy.start()

    slots = SPAN * CAP
    row40 = lax.broadcasted_iota(jnp.int32, (slots, BLK), 0)
    lane40 = lax.broadcasted_iota(jnp.int32, (slots, BLK), 1)
    want = jnp.full((slots, BLK), -1, jnp.int32)
    for d in range(SPAN):
        for c in range(CAP):
            want = jnp.where(row40 == d * CAP + c, send_s[d, 0, c], want)
    chooser = jnp.where(want == lane40, 1.0, 0.0).astype(bf16)[:, :32]
    for a in range(ABLK):
        blocks[a * F : (a + 1) * F, :] = atm_v[:, a * BLK : (a + 1) * BLK].astype(f32)
    blocks[ABLK * F :, :] = jnp.zeros(((32 - ABLK) * F, BLK), f32)
    for k in range(F // 2):
        pair = jnp.concatenate(
            [blocks[pl.ds(2 * k, 32, stride=F), :], blocks[pl.ds(2 * k + 1, 32, stride=F), :]],
            axis=1,
        )
        chosen = jnp.dot(chooser, pair.astype(bf16), preferred_element_type=f32)
        for q in range(2):
            contrib[pl.ds(2 * k + q, slots, stride=F), :] = chosen[:, q * BLK : (q + 1) * BLK]
    for d in range(SPAN):
        rows = contrib[d * CAP * F : (d + 1) * CAP * F, :].astype(bf16)
        if FLUX_OFFSETS[d] == 0:
            arr[d] = rows
        else:
            outg[d] = rows

    pl.semaphore_wait(barrier, len(HALO_OFFSETS))

    flux = []
    for d in range(SPAN):
        if FLUX_OFFSETS[d] != 0:
            copy = pltpu.make_async_remote_copy(
                src_ref=outg.at[d], dst_ref=arr.at[d], send_sem=fs.at[d], recv_sem=fr.at[d],
                device_id=(at(FLUX_OFFSETS[d]),), device_id_type=MESH,
            )
            copy.start()
            flux.append(copy)

    def solve(i, carry):
        mcopy(i).wait()
        for j in range(PER):
            b = i * PER + j
            for t in range(NTR):
                xcopy(b, t).wait()
            a1, a2 = split2(m[b])
            t = jnp.concatenate([x[b, 0], x[b, 1]], axis=1)
            b1, b2 = split2(t)
            lhs = jnp.concatenate(
                [jnp.concatenate([a1, a1], axis=1), jnp.concatenate([a2, a2], axis=1)], axis=0
            )
            rhs = jnp.concatenate([b1, b2], axis=0)
            both = jnp.dot(lhs, rhs, preferred_element_type=f32)
            solved = both[:LEV] + both[LEV:]
            row = wet_v[pl.ds(b, 1), :]
            wet = jnp.concatenate([row, row], axis=1) > 0
            base = jnp.where(wet, solved, t)
            x[b, 0] = base[:, :BLK]
            x[b, 1] = base[:, BLK:]
        return carry

    lax.fori_loop(0, OBLK // PER, solve, 0)

    lane128 = lax.broadcasted_iota(jnp.int32, (BLK, BLK), 1).astype(f32)
    block32 = lax.broadcasted_iota(jnp.int32, (OBLK, BLK), 0)
    count = jnp.zeros((OBLK, BLK), f32)
    for h in range(HSPAN):
        for r in range(2):
            ghost = hg_v[2 * h + r : 2 * h + r + 1, :]
            spread = jnp.broadcast_to(ghost & (BLK - 1), (BLK, BLK)).astype(f32)
            low = jnp.where(jnp.transpose(spread) == lane128, 1.0, 0.0).astype(bf16)
            high = jnp.where(r < rows_s[0, h], ghost >> 7, -1)
            low_t[h, r * BLK : (r + 1) * BLK, :] = low
            spread = jnp.broadcast_to(high, (BLK, BLK)).astype(f32)
            high_t[h, r * BLK : (r + 1) * BLK, :] = jnp.transpose(spread).astype(bf16)
            here = jnp.where(block32 == high, 1.0, 0.0).astype(bf16)
            count = count + jnp.dot(here, low, preferred_element_type=f32)
    quarter = 0.25 * wet_v[...].astype(f32)
    quarter_o[...] = quarter
    scale[...] = 1.0 - quarter * count
    last = HALO_ORDER[-1]
    last_low[...] = low_t[last]
    last_high[...] = high_t[last]

    sub = lax.broadcasted_iota(jnp.int32, (BLK, 2 * BLK), 0)

    def send_table(h):
        row = jnp.concatenate([hs_v[2 * h : 2 * h + 1, :], hs_v[2 * h + 1 : 2 * h + 2, :]], axis=1)
        low = jnp.where(sub == (row & (BLK - 1)), 1.0, 0.0).astype(bf16)
        high = jnp.broadcast_to((row >> 7).astype(f32), (BLK, 2 * BLK)).astype(bf16)
        return low, high

    lane = lax.broadcasted_iota(jnp.int32, (OBLK, BLK), 1)
    target = jnp.full((OBLK, BLK), -1, jnp.int32)
    used = jnp.zeros((OBLK, BLK), jnp.int32)
    for d in range(SPAN):
        used = jnp.where(lane // CAP == d, cnt_s[0, d], used)
        for c in range(CAP):
            target = jnp.where(lane == d * CAP + c, tgt_s[d, 0, c], target)
    here = (target == block32) & (lane % CAP < used)
    place = jnp.where(here, 1.0, 0.0).astype(bf16)[:, :48]
    contrib[320:384, :] = jnp.zeros((64, BLK), f32)

    wcopy.wait()
    for copy in flux:
        copy.wait_recv()

    slot = lax.broadcasted_iota(jnp.int32, (32, BLK), 0) // F
    for d in range(SPAN):
        for g in range(2):
            c = 4 * g
            pieces = arr[d, c * F : (c + 4) * F, :].astype(f32)
            even = jnp.where(slot % 2 == 0, pieces, 0.0)
            odd = jnp.where(slot % 2 == 1, pieces, 0.0)
            lhs = jnp.concatenate([even, odd], axis=1).astype(bf16)
            rhs = jnp.concatenate(
                [
                    jnp.concatenate([w[d, c], w[d, c + 2]], axis=1),
                    jnp.concatenate([w[d, c + 1], w[d, c + 3]], axis=1),
                ],
                axis=0,
            )
            both = jnp.dot(lhs, rhs, preferred_element_type=f32)
            contrib[(d * CAP + c) * F : (d * CAP + c + 4) * F, :] = jnp.where(
                slot < 2, both[:, :BLK], both[:, BLK:]
            )

    wetf = wet_v[...].astype(f32)
    acc = [jnp.zeros((OBLK, BLK), f32) for _ in range(NTR)]
    for k in range(F // 2):
        pair = jnp.concatenate(
            [contrib[pl.ds(2 * k, 48, stride=F), :], contrib[pl.ds(2 * k + 1, 48, stride=F), :]],
            axis=1,
        )
        c1, c2, c3 = split3(pair)
        total = jnp.dot(place, c1, preferred_element_type=f32)
        total = total + jnp.dot(place, c2, preferred_element_type=f32)
        total = total + jnp.dot(place, c3, preferred_element_type=f32)
        for q in range(2):
            f = 2 * k + q
            flux_f = total[:, q * BLK : (q + 1) * BLK] * wetf
            ofs[pl.ds(f, OBLK, stride=F), :] = flux_f
            for t in range(NTR):
                acc[t] = acc[t] + coup_s[t, f] * flux_f
    for t in range(NTR):
        surf[t] = acc[t]

    halo = []
    for n, h in enumerate(HALO_ORDER):
        low, high = send_table(h)
        picked = jnp.zeros((NTR * LEV, 2 * BLK), f32)
        for k in range(OBLK // 2):
            tables, tiles = [], []
            for b in (2 * k, 2 * k + 1):
                tables.append(jnp.where(high == jnp.array(b, bf16), low, jnp.zeros_like(low)))
                if n == 0:
                    first = jnp.broadcast_to(m[b, :, 0:1], (LEV, BLK))
                    tiles.append(
                        jnp.concatenate(
                            [x[b, t] + first * surf[t, b : b + 1, :] for t in range(NTR)], axis=0
                        ).astype(bf16)
                    )
            if n == 0:
                tile = jnp.concatenate(tiles, axis=1)
                sent[k] = tile
            else:
                tile = sent[k]
            picked = picked + jnp.dot(
                tile, jnp.concatenate(tables, axis=0), preferred_element_type=f32
            )
        hout[h] = picked.astype(bf16)
        copy = pltpu.make_async_remote_copy(
            src_ref=hout.at[h], dst_ref=v.at[h], send_sem=hsend.at[h], recv_sem=hrecv.at[h],
            device_id=(at(HALO_OFFSETS[h]),), device_id_type=MESH,
        )
        copy.start()
        halo.append(copy)

    def finish(b, carry):
        first = jnp.broadcast_to(m[b, :, 0:1], (LEV, BLK))
        keep = scale[pl.ds(b, 1), :]
        for t in range(NTR):
            x[b, t] = (x[b, t] + first * surf[t, pl.ds(b, 1), :]) * keep
        return carry

    lax.fori_loop(0, OBLK, finish, 0)

    for h, copy in zip(HALO_ORDER, halo):
        copy.wait_recv()
        if h == last:
            last_v[...] = v[h]
        else:
            def spread_values(k, carry, h=h):
                add_values(k, x, v[h], low_t[h], high_t[h], quarter_o, x)
                return carry

            lax.fori_loop(0, OBLK // 2, spread_values, 0)
    for copy in flux:
        copy.wait_send()
    for copy in halo:
        copy.wait_send()


def add_values(k, x, values, low, high, quarter_v, out):
    tables = []
    for j in range(2):
        b = lax.convert_element_type(2 * k + j, f32).astype(bf16)
        tables.append(jnp.where(high == b, low, jnp.zeros_like(low)))
    total = jnp.dot(values, jnp.concatenate(tables, axis=1), preferred_element_type=f32)
    for j in range(2):
        b = 2 * k + j
        weight = quarter_v[pl.ds(b, 1), :]
        for t in range(NTR):
            part = total[t * LEV : (t + 1) * LEV, j * BLK : (j + 1) * BLK]
            out[b, t] = x[b, t] + weight * part


def scatter(x, ofs, values_v, low_v, high_v, quarter_v, flux_o, out_o, stage, line, sem, fsem):
    for b in range(OBLK):
        line[:, b * BLK : (b + 1) * BLK] = ofs[b * F : (b + 1) * F, :]
    fcopy = pltpu.make_async_copy(line, flux_o, fsem)
    fcopy.start()

    def ocopy(b, t):
        cols = pl.ds(pl.multiple_of(b * BLK, BLK), BLK)
        return pltpu.make_async_copy(stage.at[b, t], out_o.at[t, :, cols], sem.at[b, t])

    def step(k, carry):
        add_values(k, x, values_v[...], low_v[...], high_v[...], quarter_v, stage)
        for j in range(2):
            for t in range(NTR):
                ocopy(2 * k + j, t).start()
        return carry

    lax.fori_loop(0, OBLK // 2, step, 0)

    def drain(b, carry):
        for t in range(NTR):
            ocopy(b, t).wait()
        return carry

    lax.fori_loop(0, OBLK, drain, 0)
    fcopy.wait()


def body(
    atm_flux, remap_send, remap_target, remap_counts, remap_weights, coupling,
    tracer, wet, mix_inverse, halo_send, halo_ghost, halo_rows,
):
    size = lax.axis_size("patch")
    wet2 = wet.reshape(OBLK, BLK)
    sends = halo_send.reshape(2 * HSPAN, BLK)
    ghosts = halo_ghost.reshape(2 * HSPAN, BLK)
    weights = remap_weights.reshape(SPAN, CAP, BLK, BLK)
    far = lambda a: pltpu.with_memory_space_constraint(a, pltpu.HBM)
    smem = pl.BlockSpec(memory_space=pltpu.SMEM)
    vmem = pl.BlockSpec(memory_space=pltpu.VMEM)
    hbm = pl.BlockSpec(memory_space=pltpu.HBM)
    dma = pltpu.SemaphoreType.DMA
    picks = 2 * BLK
    between = pl.pallas_call(
        functools.partial(couple, size),
        name="couple",
        out_shape=(
            jax.ShapeDtypeStruct((OBLK, NTR, LEV, BLK), f32),
            jax.ShapeDtypeStruct((OBLK * F, BLK), f32),
            jax.ShapeDtypeStruct((NTR * LEV, picks), bf16),
            jax.ShapeDtypeStruct((picks, BLK), bf16),
            jax.ShapeDtypeStruct((picks, BLK), bf16),
            jax.ShapeDtypeStruct((OBLK, BLK), f32),
        ),
        in_specs=[smem] * 5 + [vmem] * 4 + [hbm] * 3,
        out_specs=(vmem,) * 6,
        scratch_shapes=[
            pltpu.VMEM((OBLK, LEV, LEV), f32),
            pltpu.VMEM((SPAN, CAP, BLK, BLK), bf16),
            pltpu.VMEM((32 * F, BLK), f32),
            pltpu.VMEM((SPAN, CAP * F, BLK), bf16),
            pltpu.VMEM((SPAN, CAP * F, BLK), bf16),
            pltpu.VMEM((48 * F, BLK), f32),
            pltpu.VMEM((NTR, OBLK, BLK), f32),
            pltpu.VMEM((OBLK, BLK), f32),
            pltpu.VMEM((OBLK // 2, NTR * LEV, 2 * BLK), bf16),
            pltpu.VMEM((HSPAN, picks, BLK), bf16),
            pltpu.VMEM((HSPAN, picks, BLK), bf16),
            pltpu.VMEM((HSPAN, NTR * LEV, picks), bf16),
            pltpu.VMEM((HSPAN, NTR * LEV, picks), bf16),
            dma((OBLK, NTR)), dma((OBLK // PER,)), dma(()),
            dma((SPAN,)), dma((SPAN,)), dma((HSPAN,)), dma((HSPAN,)),
        ],
        compiler_params=pltpu.CompilerParams(
            collective_id=0, has_side_effects=True, vmem_limit_bytes=24 * 1024 * 1024
        ),
    )(
        far(jnp.transpose(remap_send, (1, 0, 2))), far(jnp.transpose(remap_target, (1, 0, 2))),
        far(remap_counts), far(coupling), far(halo_rows), far(atm_flux), far(sends), far(ghosts),
        far(wet2), far(tracer), far(mix_inverse), far(weights),
    )
    return pl.pallas_call(
        scatter,
        name="scatter",
        out_shape=(
            jax.ShapeDtypeStruct((F, OC), f32),
            jax.ShapeDtypeStruct((NTR, LEV, OC), f32),
        ),
        in_specs=[vmem] * 6,
        out_specs=(hbm, hbm),
        scratch_shapes=[
            pltpu.VMEM((OBLK, NTR, LEV, BLK), f32),
            pltpu.VMEM((F, OC), f32),
            dma((OBLK, NTR)), dma(()),
        ],
        compiler_params=pltpu.CompilerParams(vmem_limit_bytes=16 * 1024 * 1024),
    )(*between)


def solution(mesh):
    return jax.shard_map(
        body,
        mesh=mesh,
        in_specs=(
            P(None, "patch"),
            P("patch", None, None),
            P("patch", None, None),
            P("patch", None),
            P("patch", None, None, None, None),
            P(),
            P(None, None, "patch"),
            P("patch"),
            P("patch", None, None),
            P("patch", None, None, None),
            P("patch", None, None, None),
            P("patch", None),
        ),
        out_specs=(P(None, "patch"), P(None, None, "patch")),
        check_vma=False,
    )
```

```python
import functools

import jax
import jax.numpy as jnp
from jax import lax
from jax.experimental import pallas as pl
from jax.experimental.pallas import tpu as pltpu
from jax.sharding import PartitionSpec as P

F = 8
LEV = 128
NTR = 2
BLK = 128
ABLK = 24
OBLK = 32
CAP = 8
SPAN = 5
HSPAN = 4
OC = 4096
PER = 8
FLUX_OFFSETS = (-2, -1, 0, 1, 2)
HALO_OFFSETS = (-2, -1, 1, 2)
HALO_ORDER = (3, 0, 2, 1)
MESH = pl.DeviceIdType.MESH
f32 = jnp.float32
bf16 = jnp.bfloat16


def split2(v):
    hi = v.astype(bf16)
    lo = (v - hi.astype(f32)).astype(bf16)
    return hi, lo


def split3(v):
    hi, rest = v.astype(bf16), None
    rest = v - hi.astype(f32)
    mid = rest.astype(bf16)
    low = (rest - mid.astype(f32)).astype(bf16)
    return hi, mid, low


def couple(
    size,
    send_s, tgt_s, cnt_s, coup_s, rows_s, atm_v, hs_v, hg_v, wet_v, tracer_h, mix_h, w_h,
    x, ofs, last_v, last_low, last_high, quarter_o,
    m, w, blocks, outg, arr, contrib, surf, scale, sent, low_t, high_t, hout, v,
    xsem, msem, wsem, fs, fr, hsend, hrecv,
):
    me = lax.axis_index("patch")

    def at(offset):
        return lax.rem(me + (offset + size), size)

    barrier = pltpu.get_barrier_semaphore()
    for offset in HALO_OFFSETS:
        pl.semaphore_signal(barrier, inc=1, device_id=(at(offset),), device_id_type=MESH)

    def xcopy(b, t):
        cols = pl.ds(pl.multiple_of(b * BLK, BLK), BLK)
        return pltpu.make_async_copy(tracer_h.at[t, :, cols], x.at[b, t], xsem.at[b, t])

    def mcopy(i):
        rows = pl.ds(i * PER, PER)
        return pltpu.make_async_copy(mix_h.at[rows], m.at[rows], msem.at[i])

    wcopy = pltpu.make_async_copy(w_h, w, wsem)
    for i in range(OBLK // PER):
        mcopy(i).start()
        for b in range(i * PER, (i + 1) * PER):
            for t in range(NTR):
                xcopy(b, t).start()
    wcopy.start()

    slots = SPAN * CAP
    row40 = lax.broadcasted_iota(jnp.int32, (slots, BLK), 0)
    lane40 = lax.broadcasted_iota(jnp.int32, (slots, BLK), 1)
    want = jnp.full((slots, BLK), -1, jnp.int32)
    for d in range(SPAN):
        for c in range(CAP):
            want = jnp.where(row40 == d * CAP + c, send_s[d, 0, c], want)
    chooser = jnp.where(want == lane40, 1.0, 0.0).astype(bf16)[:, :32]
    for a in range(ABLK):
        blocks[a * F : (a + 1) * F, :] = atm_v[:, a * BLK : (a + 1) * BLK].astype(f32)
    blocks[ABLK * F :, :] = jnp.zeros(((32 - ABLK) * F, BLK), f32)
    for k in range(F // 2):
        pair = jnp.concatenate(
            [blocks[pl.ds(2 * k, 32, stride=F), :], blocks[pl.ds(2 * k + 1, 32, stride=F), :]],
            axis=1,
        )
        chosen = jnp.dot(chooser, pair.astype(bf16), preferred_element_type=f32)
        for q in range(2):
            contrib[pl.ds(2 * k + q, slots, stride=F), :] = chosen[:, q * BLK : (q + 1) * BLK]
    for d in range(SPAN):
        rows = contrib[d * CAP * F : (d + 1) * CAP * F, :].astype(bf16)
        if FLUX_OFFSETS[d] == 0:
            arr[d] = rows
        else:
            outg[d] = rows

    pl.semaphore_wait(barrier, len(HALO_OFFSETS))

    flux = []
    for d in range(SPAN):
        if FLUX_OFFSETS[d] != 0:
            copy = pltpu.make_async_remote_copy(
                src_ref=outg.at[d], dst_ref=arr.at[d], send_sem=fs.at[d], recv_sem=fr.at[d],
                device_id=(at(FLUX_OFFSETS[d]),), device_id_type=MESH,
            )
            copy.start()
            flux.append(copy)

    for b in range(OBLK):
        if b % PER == 0:
            mcopy(b // PER).wait()
            for n in range(PER):
                for t in range(NTR):
                    xcopy(b + n, t).wait()
        a1, a2 = split2(m[b])
        t = jnp.concatenate([x[b, 0], x[b, 1]], axis=1)
        b1, b2 = split2(t)
        lhs = jnp.concatenate(
            [jnp.concatenate([a1, a1], axis=1), jnp.concatenate([a2, a2], axis=1)], axis=0
        )
        rhs = jnp.concatenate([b1, b2], axis=0)
        both = jnp.dot(lhs, rhs, preferred_element_type=f32)
        solved = both[:LEV] + both[LEV:]
        row = wet_v[b : b + 1, :]
        wet = jnp.concatenate([row, row], axis=1) > 0
        base = jnp.where(wet, solved, t)
        x[b, 0] = base[:, :BLK]
        x[b, 1] = base[:, BLK:]

    lane128 = lax.broadcasted_iota(jnp.int32, (BLK, BLK), 1).astype(f32)
    block32 = lax.broadcasted_iota(jnp.int32, (OBLK, BLK), 0)
    count = jnp.zeros((OBLK, BLK), f32)
    for h in range(HSPAN):
        for r in range(2):
            ghost = hg_v[2 * h + r : 2 * h + r + 1, :]
            spread = jnp.broadcast_to(ghost & (BLK - 1), (BLK, BLK)).astype(f32)
            low = jnp.where(jnp.transpose(spread) == lane128, 1.0, 0.0).astype(bf16)
            high = jnp.where(r < rows_s[0, h], ghost >> 7, -1)
            low_t[h, r * BLK : (r + 1) * BLK, :] = low
            spread = jnp.broadcast_to(high, (BLK, BLK)).astype(f32)
            high_t[h, r * BLK : (r + 1) * BLK, :] = jnp.transpose(spread).astype(bf16)
            here = jnp.where(block32 == high, 1.0, 0.0).astype(bf16)
            count = count + jnp.dot(here, low, preferred_element_type=f32)
    quarter = 0.25 * wet_v[...].astype(f32)
    quarter_o[...] = quarter
    scale[...] = 1.0 - quarter * count
    last = HALO_ORDER[-1]
    last_low[...] = low_t[last]
    last_high[...] = high_t[last]

    sub = lax.broadcasted_iota(jnp.int32, (BLK, 2 * BLK), 0)

    def send_table(h):
        row = jnp.concatenate([hs_v[2 * h : 2 * h + 1, :], hs_v[2 * h + 1 : 2 * h + 2, :]], axis=1)
        low = jnp.where(sub == (row & (BLK - 1)), 1.0, 0.0).astype(bf16)
        high = jnp.broadcast_to((row >> 7).astype(f32), (BLK, 2 * BLK)).astype(bf16)
        return low, high

    lane = lax.broadcasted_iota(jnp.int32, (OBLK, BLK), 1)
    target = jnp.full((OBLK, BLK), -1, jnp.int32)
    used = jnp.zeros((OBLK, BLK), jnp.int32)
    for d in range(SPAN):
        used = jnp.where(lane // CAP == d, cnt_s[0, d], used)
        for c in range(CAP):
            target = jnp.where(lane == d * CAP + c, tgt_s[d, 0, c], target)
    here = (target == block32) & (lane % CAP < used)
    place = jnp.where(here, 1.0, 0.0).astype(bf16)[:, :48]
    contrib[320:384, :] = jnp.zeros((64, BLK), f32)

    wcopy.wait()
    for copy in flux:
        copy.wait_recv()

    slot = lax.broadcasted_iota(jnp.int32, (32, BLK), 0) // F
    for d in range(SPAN):
        for g in range(2):
            c = 4 * g
            pieces = arr[d, c * F : (c + 4) * F, :].astype(f32)
            even = jnp.where(slot % 2 == 0, pieces, 0.0)
            odd = jnp.where(slot % 2 == 1, pieces, 0.0)
            lhs = jnp.concatenate([even, odd], axis=1).astype(bf16)
            rhs = jnp.concatenate(
                [
                    jnp.concatenate([w[d, c], w[d, c + 2]], axis=1),
                    jnp.concatenate([w[d, c + 1], w[d, c + 3]], axis=1),
                ],
                axis=0,
            )
            both = jnp.dot(lhs, rhs, preferred_element_type=f32)
            contrib[(d * CAP + c) * F : (d * CAP + c + 4) * F, :] = jnp.where(
                slot < 2, both[:, :BLK], both[:, BLK:]
            )

    wetf = wet_v[...].astype(f32)
    acc = [jnp.zeros((OBLK, BLK), f32) for _ in range(NTR)]
    for k in range(F // 2):
        pair = jnp.concatenate(
            [contrib[pl.ds(2 * k, 48, stride=F), :], contrib[pl.ds(2 * k + 1, 48, stride=F), :]],
            axis=1,
        )
        c1, c2, c3 = split3(pair)
        total = jnp.dot(place, c1, preferred_element_type=f32)
        total = total + jnp.dot(place, c2, preferred_element_type=f32)
        total = total + jnp.dot(place, c3, preferred_element_type=f32)
        for q in range(2):
            f = 2 * k + q
            flux_f = total[:, q * BLK : (q + 1) * BLK] * wetf
            ofs[pl.ds(f, OBLK, stride=F), :] = flux_f
            for t in range(NTR):
                acc[t] = acc[t] + coup_s[t, f] * flux_f
    for t in range(NTR):
        surf[t] = acc[t]

    halo = []
    for n, h in enumerate(HALO_ORDER):
        low, high = send_table(h)
        picked = jnp.zeros((NTR * LEV, 2 * BLK), f32)
        for k in range(OBLK // 2):
            tables, tiles = [], []
            for b in (2 * k, 2 * k + 1):
                tables.append(jnp.where(high == jnp.array(b, bf16), low, jnp.zeros_like(low)))
                if n == 0:
                    first = jnp.broadcast_to(m[b, :, 0:1], (LEV, BLK))
                    mixed = [x[b, t] + first * surf[t, b : b + 1, :] for t in range(NTR)]
                    for t in range(NTR):
                        x[b, t] = mixed[t] * scale[b : b + 1, :]
                    tiles.append(jnp.concatenate(mixed, axis=0).astype(bf16))
            if n == 0:
                tile = jnp.concatenate(tiles, axis=1)
                sent[k] = tile
            else:
                tile = sent[k]
            picked = picked + jnp.dot(
                tile, jnp.concatenate(tables, axis=0), preferred_element_type=f32
            )
        hout[h] = picked.astype(bf16)
        copy = pltpu.make_async_remote_copy(
            src_ref=hout.at[h], dst_ref=v.at[h], send_sem=hsend.at[h], recv_sem=hrecv.at[h],
            device_id=(at(HALO_OFFSETS[h]),), device_id_type=MESH,
        )
        copy.start()
        halo.append(copy)

    for h, copy in zip(HALO_ORDER, halo):
        copy.wait_recv()
        if h == last:
            last_v[...] = v[h]
        else:
            for k in range(OBLK // 2):
                add_values(k, x, v[h], low_t[h], high_t[h], quarter_o, x)
    for copy in flux:
        copy.wait_send()
    for copy in halo:
        copy.wait_send()


def add_values(k, x, values, low, high, quarter_v, out):
    tables = []
    for j in range(2):
        here = high == jnp.array(2 * k + j, bf16)
        tables.append(jnp.where(here, low, jnp.zeros_like(low)))
    total = jnp.dot(values, jnp.concatenate(tables, axis=1), preferred_element_type=f32)
    for j in range(2):
        b = 2 * k + j
        weight = quarter_v[b : b + 1, :]
        for t in range(NTR):
            part = total[t * LEV : (t + 1) * LEV, j * BLK : (j + 1) * BLK]
            out[b, t] = x[b, t] + weight * part


def scatter(x, ofs, values_v, low_v, high_v, quarter_v, flux_o, out_o, stage, line, sem, fsem):
    for b in range(OBLK):
        line[:, b * BLK : (b + 1) * BLK] = ofs[b * F : (b + 1) * F, :]
    fcopy = pltpu.make_async_copy(line, flux_o, fsem)
    fcopy.start()

    def ocopy(b, t):
        cols = pl.ds(pl.multiple_of(b * BLK, BLK), BLK)
        return pltpu.make_async_copy(stage.at[b, t], out_o.at[t, :, cols], sem.at[b, t])

    for k in range(OBLK // 2):
        add_values(k, x, values_v[...], low_v[...], high_v[...], quarter_v, stage)
        for j in range(2):
            for t in range(NTR):
                ocopy(2 * k + j, t).start()

    def drain(b, carry):
        for t in range(NTR):
            ocopy(b, t).wait()
        return carry

    lax.fori_loop(0, OBLK, drain, 0)
    fcopy.wait()


def body(
    atm_flux, remap_send, remap_target, remap_counts, remap_weights, coupling,
    tracer, wet, mix_inverse, halo_send, halo_ghost, halo_rows,
):
    size = lax.axis_size("patch")
    wet2 = wet.reshape(OBLK, BLK)
    sends = halo_send.reshape(2 * HSPAN, BLK)
    ghosts = halo_ghost.reshape(2 * HSPAN, BLK)
    weights = remap_weights.reshape(SPAN, CAP, BLK, BLK)
    far = lambda a: pltpu.with_memory_space_constraint(a, pltpu.HBM)
    smem = pl.BlockSpec(memory_space=pltpu.SMEM)
    vmem = pl.BlockSpec(memory_space=pltpu.VMEM)
    hbm = pl.BlockSpec(memory_space=pltpu.HBM)
    dma = pltpu.SemaphoreType.DMA
    picks = 2 * BLK
    between = pl.pallas_call(
        functools.partial(couple, size),
        name="couple",
        out_shape=(
            jax.ShapeDtypeStruct((OBLK, NTR, LEV, BLK), f32),
            jax.ShapeDtypeStruct((OBLK * F, BLK), f32),
            jax.ShapeDtypeStruct((NTR * LEV, picks), bf16),
            jax.ShapeDtypeStruct((picks, BLK), bf16),
            jax.ShapeDtypeStruct((picks, BLK), bf16),
            jax.ShapeDtypeStruct((OBLK, BLK), f32),
        ),
        in_specs=[smem] * 5 + [vmem] * 4 + [hbm] * 3,
        out_specs=(vmem,) * 6,
        scratch_shapes=[
            pltpu.VMEM((OBLK, LEV, LEV), f32),
            pltpu.VMEM((SPAN, CAP, BLK, BLK), bf16),
            pltpu.VMEM((32 * F, BLK), f32),
            pltpu.VMEM((SPAN, CAP * F, BLK), bf16),
            pltpu.VMEM((SPAN, CAP * F, BLK), bf16),
            pltpu.VMEM((48 * F, BLK), f32),
            pltpu.VMEM((NTR, OBLK, BLK), f32),
            pltpu.VMEM((OBLK, BLK), f32),
            pltpu.VMEM((OBLK // 2, NTR * LEV, 2 * BLK), bf16),
            pltpu.VMEM((HSPAN, picks, BLK), bf16),
            pltpu.VMEM((HSPAN, picks, BLK), bf16),
            pltpu.VMEM((HSPAN, NTR * LEV, picks), bf16),
            pltpu.VMEM((HSPAN, NTR * LEV, picks), bf16),
            dma((OBLK, NTR)), dma((OBLK // PER,)), dma(()),
            dma((SPAN,)), dma((SPAN,)), dma((HSPAN,)), dma((HSPAN,)),
        ],
        compiler_params=pltpu.CompilerParams(
            collective_id=0, has_side_effects=True, vmem_limit_bytes=24 * 1024 * 1024
        ),
    )(
        far(jnp.transpose(remap_send, (1, 0, 2))), far(jnp.transpose(remap_target, (1, 0, 2))),
        far(remap_counts), far(coupling), far(halo_rows), far(atm_flux), far(sends), far(ghosts),
        far(wet2), far(tracer), far(mix_inverse), far(weights),
    )
    return pl.pallas_call(
        scatter,
        name="scatter",
        out_shape=(
            jax.ShapeDtypeStruct((F, OC), f32),
            jax.ShapeDtypeStruct((NTR, LEV, OC), f32),
        ),
        in_specs=[vmem] * 6,
        out_specs=(hbm, hbm),
        scratch_shapes=[
            pltpu.VMEM((OBLK, NTR, LEV, BLK), f32),
            pltpu.VMEM((F, OC), f32),
            dma((OBLK, NTR)), dma(()),
        ],
        compiler_params=pltpu.CompilerParams(vmem_limit_bytes=16 * 1024 * 1024),
    )(*between)


def solution(mesh):
    return jax.shard_map(
        body,
        mesh=mesh,
        in_specs=(
            P(None, "patch"),
            P("patch", None, None),
            P("patch", None, None),
            P("patch", None),
            P("patch", None, None, None, None),
            P(),
            P(None, None, "patch"),
            P("patch"),
            P("patch", None, None),
            P("patch", None, None, None),
            P("patch", None, None, None),
            P("patch", None),
        ),
        out_specs=(P(None, "patch"), P(None, None, "patch")),
        check_vma=False,
    )
```

```python
import functools

import jax
import jax.numpy as jnp
from jax import lax
from jax.experimental import pallas as pl
from jax.experimental.pallas import tpu as pltpu
from jax.sharding import PartitionSpec as P

F = 8
LEV = 128
NTR = 2
BLK = 128
ABLK = 24
OBLK = 32
CAP = 8
SPAN = 5
HSPAN = 4
OC = 4096
PER = 8
FLUX_OFFSETS = (-2, -1, 0, 1, 2)
HALO_OFFSETS = (-2, -1, 1, 2)
SEND_ORDERS = ((3, 0, 2, 1), (0, 1, 3, 2), (3, 0, 2, 1), (3, 2, 0, 1))
WAIT_ORDERS = (((3, 2, 1, 0), (3, 2, 0, 1)), ((0, 1, 3, 2), (0, 1, 2, 3)))
LINE = 4
MESH = pl.DeviceIdType.MESH
f32 = jnp.float32
bf16 = jnp.bfloat16


def split2(v):
    hi = v.astype(bf16)
    lo = (v - hi.astype(f32)).astype(bf16)
    return hi, lo


def split3(v):
    hi, rest = v.astype(bf16), None
    rest = v - hi.astype(f32)
    mid = rest.astype(bf16)
    low = (rest - mid.astype(f32)).astype(bf16)
    return hi, mid, low


def couple(
    size,
    send_h, tgt_h, cnt_h, coup_h, rows_h, atm_h, hs_h, hg_h, wet_h, tracer_h, mix_h, w_h,
    x, line, last_v, last_low, last_high, quarter_o,
    send_s, tgt_s, cnt_s, coup_s, rows_s, atm_v, hs_v, hg_v, wet_v,
    m, w, blocks, outg, arr, contrib, ofs, surf, scale, sent, low_t, high_t, hout, v,
    small, xsem, msem, wsem, fs, fr, hsend, hrecv,
):
    me = lax.axis_index("patch")

    def at(offset):
        return lax.rem(me + (offset + size), size)

    barrier = pltpu.get_barrier_semaphore()
    for offset in HALO_OFFSETS:
        pl.semaphore_signal(barrier, inc=1, device_id=(at(offset),), device_id_type=MESH)

    chip = lax.rem(me // 2, LINE)
    top = (chip + 1) // LINE
    foot = (LINE - chip) // LINE
    upper = chip // (LINE // 2)
    core = lax.rem(me, 2)

    def choose(i):
        high, low = WAIT_ORDERS
        above = high[0][i] * (1 - core) + high[1][i] * core
        below = low[0][i] * (1 - core) + low[1][i] * core
        return above * upper + below * (1 - upper)

    order = [choose(i) for i in range(HSPAN)]
    second = (1 - foot) * (1 - upper)
    third = (1 - top) * upper
    places = (foot, second, third, top)
    sends = [sum(SEND_ORDERS[y][i] * places[y] for y in range(LINE)) for i in range(HSPAN)]

    pairs = (
        (send_h, send_s), (atm_h, atm_v), (wet_h, wet_v), (hs_h, hs_v), (hg_h, hg_v),
        (tgt_h, tgt_s), (cnt_h, cnt_s), (coup_h, coup_s), (rows_h, rows_s),
    )
    smalls = [pltpu.make_async_copy(src, dst, small.at[i]) for i, (src, dst) in enumerate(pairs)]
    for copy in smalls:
        copy.start()

    def xcopy(b, t):
        cols = pl.ds(pl.multiple_of(b * BLK, BLK), BLK)
        return pltpu.make_async_copy(tracer_h.at[t, :, cols], x.at[b, t], xsem.at[b // PER])

    def mcopy(i):
        rows = pl.ds(i * PER, PER)
        return pltpu.make_async_copy(mix_h.at[rows], m.at[rows], msem.at[i])

    wcopy = pltpu.make_async_copy(w_h, w, wsem)

    def fetch(i):
        mcopy(i).start()
        for b in range(i * PER, (i + 1) * PER):
            for t in range(NTR):
                xcopy(b, t).start()

    for copy in smalls[:3]:
        copy.wait()
    fetch(0)
    fetch(1)
    slots = SPAN * CAP
    row40 = lax.broadcasted_iota(jnp.int32, (slots, BLK), 0)
    lane40 = lax.broadcasted_iota(jnp.int32, (slots, BLK), 1)
    want = jnp.full((slots, BLK), -1, jnp.int32)
    for d in range(SPAN):
        for c in range(CAP):
            want = jnp.where(row40 == d * CAP + c, send_s[d, 0, c], want)
    chooser = jnp.where(want == lane40, 1.0, 0.0).astype(bf16)[:, :32]
    for a in range(ABLK):
        blocks[a * F : (a + 1) * F, :] = atm_v[:, a * BLK : (a + 1) * BLK].astype(f32)
    blocks[ABLK * F :, :] = jnp.zeros(((32 - ABLK) * F, BLK), f32)
    for k in range(F // 2):
        pair = jnp.concatenate(
            [blocks[pl.ds(2 * k, 32, stride=F), :], blocks[pl.ds(2 * k + 1, 32, stride=F), :]],
            axis=1,
        )
        chosen = jnp.dot(chooser, pair.astype(bf16), preferred_element_type=f32)
        for q in range(2):
            contrib[pl.ds(2 * k + q, slots, stride=F), :] = chosen[:, q * BLK : (q + 1) * BLK]
    for d in range(SPAN):
        rows = contrib[d * CAP * F : (d + 1) * CAP * F, :].astype(bf16)
        if FLUX_OFFSETS[d] == 0:
            arr[d] = rows
        else:
            outg[d] = rows

    for i in range(2, OBLK // PER):
        fetch(i)
    wcopy.start()

    def solve(i):
        mcopy(i).wait()
        chunk = x.at[pl.ds(i * PER, PER)]
        pltpu.make_async_copy(chunk, chunk, xsem.at[i]).wait()
        for b in range(i * PER, (i + 1) * PER):
            a1, a2 = split2(m[b])
            t = jnp.concatenate([x[b, 0], x[b, 1]], axis=1)
            b1, b2 = split2(t)
            lhs = jnp.concatenate(
                [jnp.concatenate([a1, a1], axis=1), jnp.concatenate([a2, a2], axis=1)], axis=0
            )
            rhs = jnp.concatenate([b1, b2], axis=0)
            both = jnp.dot(lhs, rhs, preferred_element_type=f32)
            solved = both[:LEV] + both[LEV:]
            row = wet_v[b : b + 1, :]
            wet = jnp.concatenate([row, row], axis=1) > 0
            base = jnp.where(wet, solved, t)
            x[b, 0] = base[:, :BLK]
            x[b, 1] = base[:, BLK:]

    pl.semaphore_wait(barrier, len(HALO_OFFSETS))

    flux = []
    for d in range(SPAN):
        if FLUX_OFFSETS[d] != 0:
            copy = pltpu.make_async_remote_copy(
                src_ref=outg.at[d], dst_ref=arr.at[d], send_sem=fs.at[d], recv_sem=fr.at[d],
                device_id=(at(FLUX_OFFSETS[d]),), device_id_type=MESH,
            )
            copy.start()
            flux.append(copy)

    for i in range(OBLK // PER):
        solve(i)
    for copy in smalls[3:]:
        copy.wait()

    lane128 = lax.broadcasted_iota(jnp.int32, (BLK, BLK), 1).astype(f32)
    block32 = lax.broadcasted_iota(jnp.int32, (OBLK, BLK), 0)
    count = jnp.zeros((OBLK, BLK), f32)
    for h in range(HSPAN):
        for r in range(2):
            ghost = hg_v[2 * h + r : 2 * h + r + 1, :]
            spread = jnp.broadcast_to(ghost & (BLK - 1), (BLK, BLK)).astype(f32)
            low = jnp.where(jnp.transpose(spread) == lane128, 1.0, 0.0).astype(bf16)
            high = jnp.where(r < rows_s[0, h], ghost >> 7, -1)
            low_t[h, r * BLK : (r + 1) * BLK, :] = low
            spread = jnp.broadcast_to(high, (BLK, BLK)).astype(f32)
            high_t[h, r * BLK : (r + 1) * BLK, :] = jnp.transpose(spread).astype(bf16)
            here = jnp.where(block32 == high, 1.0, 0.0).astype(bf16)
            count = count + jnp.dot(here, low, preferred_element_type=f32)
    quarter = 0.25 * wet_v[...].astype(f32)
    quarter_o[...] = quarter
    scale[...] = 1.0 - quarter * count

    lane = lax.broadcasted_iota(jnp.int32, (OBLK, BLK), 1)
    target = jnp.full((OBLK, BLK), -1, jnp.int32)
    used = jnp.zeros((OBLK, BLK), jnp.int32)
    for d in range(SPAN):
        used = jnp.where(lane // CAP == d, cnt_s[0, d], used)
        for c in range(CAP):
            target = jnp.where(lane == d * CAP + c, tgt_s[d, 0, c], target)
    here = (target == block32) & (lane % CAP < used)
    place = jnp.where(here, 1.0, 0.0).astype(bf16)[:, :48]
    contrib[320:384, :] = jnp.zeros((64, BLK), f32)

    wcopy.wait()
    slot = lax.broadcasted_iota(jnp.int32, (32, BLK), 0) // F
    for i in range(SPAN):
        d = i + top * (SPAN - 1 - 2 * i)
        if i != SPAN // 2:
            pltpu.make_async_remote_copy(
                src_ref=outg.at[d], dst_ref=arr.at[d], send_sem=fs.at[d], recv_sem=fr.at[d],
                device_id=(at(1),), device_id_type=MESH,
            ).wait_recv()
        for g in range(2):
            c = 4 * g
            pieces = arr[d, c * F : (c + 4) * F, :].astype(f32)
            even = jnp.where(slot % 2 == 0, pieces, 0.0)
            odd = jnp.where(slot % 2 == 1, pieces, 0.0)
            lhs = jnp.concatenate([even, odd], axis=1).astype(bf16)
            rhs = jnp.concatenate(
                [
                    jnp.concatenate([w[d, c], w[d, c + 2]], axis=1),
                    jnp.concatenate([w[d, c + 1], w[d, c + 3]], axis=1),
                ],
                axis=0,
            )
            both = jnp.dot(lhs, rhs, preferred_element_type=f32)
            rows = pl.ds(pl.multiple_of((d * CAP + c) * F, 4 * F), 4 * F)
            contrib[rows, :] = jnp.where(slot < 2, both[:, :BLK], both[:, BLK:])

    wetf = wet_v[...].astype(f32)
    acc = [jnp.zeros((OBLK, BLK), f32) for _ in range(NTR)]
    for k in range(F // 2):
        pair = jnp.concatenate(
            [contrib[pl.ds(2 * k, 48, stride=F), :], contrib[pl.ds(2 * k + 1, 48, stride=F), :]],
            axis=1,
        )
        c1, c2, c3 = split3(pair)
        total = jnp.dot(place, c1, preferred_element_type=f32)
        total = total + jnp.dot(place, c2, preferred_element_type=f32)
        total = total + jnp.dot(place, c3, preferred_element_type=f32)
        for q in range(2):
            f = 2 * k + q
            flux_f = total[:, q * BLK : (q + 1) * BLK] * wetf
            ofs[pl.ds(f, OBLK, stride=F), :] = flux_f
            for t in range(NTR):
                acc[t] = acc[t] + coup_s[t, f] * flux_f
    for t in range(NTR):
        surf[t] = acc[t]

    sub = lax.broadcasted_iota(jnp.int32, (BLK, 2 * BLK), 0)

    def halo_copy(h, t):
        offset = h - 2 + h // 2
        return pltpu.make_async_remote_copy(
            src_ref=hout.at[h, t], dst_ref=v.at[h, t],
            send_sem=hsend.at[h, t], recv_sem=hrecv.at[h, t],
            device_id=(at(offset),), device_id_type=MESH,
        )

    for n, h in enumerate(sends):
        row = jnp.concatenate([hs_v[pl.ds(2 * h, 1), :], hs_v[pl.ds(2 * h + 1, 1), :]], axis=1)
        low = jnp.where(sub == (row & (BLK - 1)), 1.0, 0.0).astype(bf16)
        high = jnp.broadcast_to((row >> 7).astype(f32), (BLK, 2 * BLK)).astype(bf16)
        for part in ((0,), (1,)) if n == 0 else ((0, 1),):
            rows = slice(part[0] * LEV, (part[-1] + 1) * LEV)
            picked = jnp.zeros((len(part) * LEV, 2 * BLK), f32)
            for k in range(OBLK // 2):
                tables, tiles = [], []
                for b in (2 * k, 2 * k + 1):
                    tables.append(jnp.where(high == jnp.array(b, bf16), low, jnp.zeros_like(low)))
                    if n == 0:
                        first = jnp.broadcast_to(m[b, :, 0:1], (LEV, BLK))
                        for t in part:
                            mixed = x[b, t] + first * surf[t, b : b + 1, :]
                            x[b, t] = mixed * scale[b : b + 1, :]
                            tiles.append(mixed.astype(bf16))
                if n == 0:
                    tile = jnp.concatenate(tiles, axis=1)
                    sent[k, rows] = tile
                else:
                    tile = sent[k, rows]
                picked = picked + jnp.dot(
                    tile, jnp.concatenate(tables, axis=0), preferred_element_type=f32
                )
            for j, t in enumerate(part):
                hout[h, t] = picked[j * LEV : (j + 1) * LEV].astype(bf16)
                halo_copy(h, t).start()

    for b in range(OBLK):
        line[:, b * BLK : (b + 1) * BLK] = ofs[b * F : (b + 1) * F, :]
    last = order[-1]
    last_low[...] = low_t[last]
    last_high[...] = high_t[last]

    for h in order[:-1]:
        for t in range(NTR):
            halo_copy(h, t).wait_recv()
        values = jnp.concatenate([v[h, 0], v[h, 1]], axis=0)
        add_values(x, values, low_t[h], high_t[h], quarter_o)
    for t in range(NTR):
        halo_copy(last, t).wait_recv()
        last_v[t * LEV : (t + 1) * LEV] = v[last, t]
    for copy in flux:
        copy.wait_send()
    for h in order:
        for t in range(NTR):
            halo_copy(h, t).wait_send()


def add_values(x, values, low, high, quarter_v, out=None, ready=None):
    out = x if out is None else out
    for k in range(OBLK // 2):
        tables = []
        for b in (2 * k, 2 * k + 1):
            here = high == jnp.array(b, bf16)
            tables.append(jnp.where(here, low, jnp.zeros_like(low)))
        total = jnp.dot(values, jnp.concatenate(tables, axis=1), preferred_element_type=f32)
        for j, b in enumerate((2 * k, 2 * k + 1)):
            weight = quarter_v[b : b + 1, :]
            for t in range(NTR):
                piece = total[t * LEV : (t + 1) * LEV, j * BLK : (j + 1) * BLK]
                out[b, t] = x[b, t] + weight * piece
                if ready is not None:
                    ready(b, t)


def scatter(x, line, values_v, low_v, high_v, quarter_v, flux_o, out_o, stage, sem, fsem):
    fcopy = pltpu.make_async_copy(line, flux_o, fsem)
    fcopy.start()

    def ready(b, t):
        cols = slice(b * BLK, (b + 1) * BLK)
        pltpu.make_async_copy(stage.at[b, t], out_o.at[t, :, cols], sem).start()

    add_values(x, values_v[...], low_v[...], high_v[...], quarter_v, stage, ready)
    pltpu.make_async_copy(out_o, out_o, sem).wait()
    fcopy.wait()


def body(
    atm_flux, remap_send, remap_target, remap_counts, remap_weights, coupling,
    tracer, wet, mix_inverse, halo_send, halo_ghost, halo_rows,
):
    size = lax.axis_size("patch")
    far = lambda a: pltpu.with_memory_space_constraint(a, pltpu.HBM)
    vmem = pl.BlockSpec(memory_space=pltpu.VMEM)
    hbm = pl.BlockSpec(memory_space=pltpu.HBM)
    dma = pltpu.SemaphoreType.DMA
    i32 = jnp.int32
    picks = 2 * BLK
    between = pl.pallas_call(
        functools.partial(couple, size),
        name="couple",
        out_shape=(
            jax.ShapeDtypeStruct((OBLK, NTR, LEV, BLK), f32),
            jax.ShapeDtypeStruct((F, OC), f32),
            jax.ShapeDtypeStruct((NTR * LEV, picks), bf16),
            jax.ShapeDtypeStruct((picks, BLK), bf16),
            jax.ShapeDtypeStruct((picks, BLK), bf16),
            jax.ShapeDtypeStruct((OBLK, BLK), f32),
        ),
        in_specs=[hbm] * 12,
        out_specs=(vmem,) * 6,
        scratch_shapes=[
            pltpu.SMEM((SPAN, 1, CAP), i32),
            pltpu.SMEM((SPAN, 1, CAP), i32),
            pltpu.SMEM((1, SPAN), i32),
            pltpu.SMEM((NTR, F), f32),
            pltpu.SMEM((1, HSPAN), i32),
            pltpu.VMEM((F, ABLK * BLK), bf16),
            pltpu.VMEM((2 * HSPAN, BLK), i32),
            pltpu.VMEM((2 * HSPAN, BLK), i32),
            pltpu.VMEM((OBLK, BLK), i32),
            pltpu.VMEM((OBLK, LEV, LEV), f32),
            pltpu.VMEM((SPAN, CAP, BLK, BLK), bf16),
            pltpu.VMEM((32 * F, BLK), f32),
            pltpu.VMEM((SPAN, CAP * F, BLK), bf16),
            pltpu.VMEM((SPAN, CAP * F, BLK), bf16),
            pltpu.VMEM((48 * F, BLK), f32),
            pltpu.VMEM((OBLK * F, BLK), f32),
            pltpu.VMEM((NTR, OBLK, BLK), f32),
            pltpu.VMEM((OBLK, BLK), f32),
            pltpu.VMEM((OBLK // 2, NTR * LEV, 2 * BLK), bf16),
            pltpu.VMEM((HSPAN, picks, BLK), bf16),
            pltpu.VMEM((HSPAN, picks, BLK), bf16),
            pltpu.VMEM((HSPAN, NTR, LEV, picks), bf16),
            pltpu.VMEM((HSPAN, NTR, LEV, picks), bf16),
            dma((9,)), dma((OBLK // PER,)), dma((OBLK // PER,)), dma(()),
            dma((SPAN,)), dma((SPAN,)), dma((HSPAN, NTR)), dma((HSPAN, NTR)),
        ],
        compiler_params=pltpu.CompilerParams(
            collective_id=0, has_side_effects=True, vmem_limit_bytes=24 * 1024 * 1024
        ),
    )(
        far(jnp.transpose(remap_send, (1, 0, 2))), far(jnp.transpose(remap_target, (1, 0, 2))),
        far(remap_counts), far(coupling), far(halo_rows), far(atm_flux),
        far(halo_send.reshape(2 * HSPAN, BLK)), far(halo_ghost.reshape(2 * HSPAN, BLK)),
        far(wet.reshape(OBLK, BLK)), far(tracer), far(mix_inverse),
        far(remap_weights.reshape(SPAN, CAP, BLK, BLK)),
    )
    return pl.pallas_call(
        scatter,
        name="scatter",
        out_shape=(
            jax.ShapeDtypeStruct((F, OC), f32),
            jax.ShapeDtypeStruct((NTR, LEV, OC), f32),
        ),
        in_specs=[vmem] * 6,
        out_specs=(hbm, hbm),
        scratch_shapes=[pltpu.VMEM((OBLK, NTR, LEV, BLK), f32), dma(()), dma(())],
        compiler_params=pltpu.CompilerParams(vmem_limit_bytes=16 * 1024 * 1024),
    )(*between)


def solution(mesh):
    return jax.shard_map(
        body,
        mesh=mesh,
        in_specs=(
            P(None, "patch"),
            P("patch", None, None),
            P("patch", None, None),
            P("patch", None),
            P("patch", None, None, None, None),
            P(),
            P(None, None, "patch"),
            P("patch"),
            P("patch", None, None),
            P("patch", None, None, None),
            P("patch", None, None, None),
            P("patch", None),
        ),
        out_specs=(P(None, "patch"), P(None, None, "patch")),
        check_vma=False,
    )
```

```python
import functools

import jax
import jax.numpy as jnp
from jax import lax
from jax.experimental import pallas as pl
from jax.experimental.pallas import tpu as pltpu
from jax.sharding import PartitionSpec as P

F = 8
LEV = 128
NTR = 2
BLK = 128
ABLK = 24
OBLK = 32
CAP = 8
SPAN = 5
HSPAN = 4
OC = 4096
PER = 8
FLUX_OFFSETS = (-2, -1, 0, 1, 2)
HALO_OFFSETS = (-2, -1, 1, 2)
SEND_ORDERS = ((3, 0, 2, 1), (0, 1, 3, 2), (3, 0, 2, 1), (3, 2, 0, 1))
WAIT_ORDERS = (((3, 2, 1, 0), (3, 2, 0, 1)), ((0, 1, 3, 2), (0, 1, 2, 3)))
LINE = 4
MESH = pl.DeviceIdType.MESH
f32 = jnp.float32
bf16 = jnp.bfloat16


def split2(v):
    hi = v.astype(bf16)
    lo = (v - hi.astype(f32)).astype(bf16)
    return hi, lo


def split3(v):
    hi, rest = v.astype(bf16), None
    rest = v - hi.astype(f32)
    mid = rest.astype(bf16)
    low = (rest - mid.astype(f32)).astype(bf16)
    return hi, mid, low


def couple(
    size,
    send_h, tgt_h, cnt_h, coup_h, rows_h, atm_h, hs_h, hg_h, wet_h, tracer_h, mix_h, w_h,
    x, line, last_v, last_low, last_high, quarter_o,
    send_s, tgt_s, cnt_s, coup_s, rows_s, atm_v, hs_v, hg_v, wet_v,
    m, w, blocks, outg, relay, arr, contrib, ofs, surf, scale, sent, low_t, high_t, hout, v,
    small, xsem, msem, wsem, fs, fr, rs, rr, hsend, hrecv,
):
    me = lax.axis_index("patch")

    def at(offset):
        return lax.rem(me + (offset + size), size)

    core = lax.rem(me, 2)
    near = size - size // LINE
    at_start = me < 2
    at_end = me >= size - 2
    at_relay = (me >= near) & (me < near + 2)

    barrier = pltpu.get_barrier_semaphore()

    def hello(device):
        pl.semaphore_signal(barrier, inc=1, device_id=(device,), device_id_type=MESH)

    for offset in HALO_OFFSETS:
        if offset < 0:
            hello(at(offset))
        else:
            pl.when(me + offset < size)(functools.partial(hello, at(offset)))
    pl.when(at_end)(functools.partial(hello, near))
    pl.when(me == size - 1)(functools.partial(hello, near + 1))
    pl.when(at_start)(functools.partial(hello, near + core))
    pl.when(at_relay)(functools.partial(hello, core))

    chip = lax.rem(me // 2, LINE)
    top = (chip + 1) // LINE
    foot = (LINE - chip) // LINE
    upper = chip // (LINE // 2)
    def choose(i):
        high, low = WAIT_ORDERS
        above = high[0][i] * (1 - core) + high[1][i] * core
        below = low[0][i] * (1 - core) + low[1][i] * core
        return above * upper + below * (1 - upper)

    order = [choose(i) for i in range(HSPAN)]
    second = (1 - foot) * (1 - upper)
    third = (1 - top) * upper
    places = (foot, second, third, top)
    sends = [sum(SEND_ORDERS[y][i] * places[y] for y in range(LINE)) for i in range(HSPAN)]

    pairs = (
        (send_h, send_s), (atm_h, atm_v), (wet_h, wet_v), (hs_h, hs_v), (hg_h, hg_v),
        (tgt_h, tgt_s), (cnt_h, cnt_s), (coup_h, coup_s), (rows_h, rows_s),
    )
    smalls = [pltpu.make_async_copy(src, dst, small.at[i]) for i, (src, dst) in enumerate(pairs)]
    for copy in smalls:
        copy.start()

    def xcopy(b, t):
        cols = pl.ds(pl.multiple_of(b * BLK, BLK), BLK)
        return pltpu.make_async_copy(tracer_h.at[t, :, cols], x.at[b, t], xsem.at[b // PER])

    def mcopy(i):
        rows = pl.ds(i * PER, PER)
        return pltpu.make_async_copy(mix_h.at[rows], m.at[rows], msem.at[i])

    wcopy = pltpu.make_async_copy(w_h, w, wsem)

    def fetch(i):
        mcopy(i).start()
        for b in range(i * PER, (i + 1) * PER):
            for t in range(NTR):
                xcopy(b, t).start()

    for copy in smalls[:3]:
        copy.wait()
    fetch(0)
    fetch(1)
    slots = SPAN * CAP
    row40 = lax.broadcasted_iota(jnp.int32, (slots, BLK), 0)
    lane40 = lax.broadcasted_iota(jnp.int32, (slots, BLK), 1)
    want = jnp.full((slots, BLK), -1, jnp.int32)
    for d in range(SPAN):
        for c in range(CAP):
            want = jnp.where(row40 == d * CAP + c, send_s[d, 0, c], want)
    chooser = jnp.where(want == lane40, 1.0, 0.0).astype(bf16)[:, :32]
    for a in range(ABLK):
        blocks[a * F : (a + 1) * F, :] = atm_v[:, a * BLK : (a + 1) * BLK].astype(f32)
    blocks[ABLK * F :, :] = jnp.zeros(((32 - ABLK) * F, BLK), f32)
    for k in range(F // 2):
        pair = jnp.concatenate(
            [blocks[pl.ds(2 * k, 32, stride=F), :], blocks[pl.ds(2 * k + 1, 32, stride=F), :]],
            axis=1,
        )
        chosen = jnp.dot(chooser, pair.astype(bf16), preferred_element_type=f32)
        for q in range(2):
            contrib[pl.ds(2 * k + q, slots, stride=F), :] = chosen[:, q * BLK : (q + 1) * BLK]
    for d in range(SPAN):
        rows = contrib[d * CAP * F : (d + 1) * CAP * F, :].astype(bf16)
        if FLUX_OFFSETS[d] == 0:
            arr[d] = rows
        else:
            outg[d] = rows

    for i in range(2, OBLK // PER):
        fetch(i)
    wcopy.start()

    def solve(i):
        mcopy(i).wait()
        chunk = x.at[pl.ds(i * PER, PER)]
        pltpu.make_async_copy(chunk, chunk, xsem.at[i]).wait()
        for b in range(i * PER, (i + 1) * PER):
            a1, a2 = split2(m[b])
            t = jnp.concatenate([x[b, 0], x[b, 1]], axis=1)
            b1, b2 = split2(t)
            lhs = jnp.concatenate(
                [jnp.concatenate([a1, a1], axis=1), jnp.concatenate([a2, a2], axis=1)], axis=0
            )
            rhs = jnp.concatenate([b1, b2], axis=0)
            both = jnp.dot(lhs, rhs, preferred_element_type=f32)
            solved = both[:LEV] + both[LEV:]
            row = wet_v[b : b + 1, :]
            wet = jnp.concatenate([row, row], axis=1) > 0
            base = jnp.where(wet, solved, t)
            x[b, 0] = base[:, :BLK]
            x[b, 1] = base[:, BLK:]

    greeted = len(HALO_OFFSETS)
    for who, amount in ((0, greeted - 1), (near, greeted + 3), (near + 1, greeted + 2)):
        pl.when(me == who)(functools.partial(pl.semaphore_wait, barrier, amount))
    pl.when((me != 0) & jnp.logical_not(at_relay))(
        functools.partial(pl.semaphore_wait, barrier, greeted)
    )

    def flux_copy(d):
        return pltpu.make_async_remote_copy(
            src_ref=outg.at[d], dst_ref=arr.at[d], send_sem=fs.at[d], recv_sem=fr.at[d],
            device_id=(at(FLUX_OFFSETS[d]),), device_id_type=MESH,
        )

    def to_relay(d):
        return pltpu.make_async_remote_copy(
            src_ref=outg.at[d], dst_ref=relay.at[d], send_sem=fs.at[d], recv_sem=rr.at[d],
            device_id=(near + core,), device_id_type=MESH,
        )

    def from_relay(d, device):
        return pltpu.make_async_remote_copy(
            src_ref=relay.at[d], dst_ref=arr.at[d], send_sem=rs.at[d], recv_sem=fr.at[d],
            device_id=(device,), device_id_type=MESH,
        )

    flux = []
    for d in range(SPAN):
        offset = FLUX_OFFSETS[d]
        if offset == 0:
            continue
        flux.append(flux_copy(d))
        if offset > 0:
            flux[-1].start()
        else:
            pl.when(me + offset >= 0)(flux[-1].start)
            pl.when(me + offset < 0)(to_relay(d).start)

    @pl.when(at_relay)
    def _():
        to_relay(0).wait_recv()
        from_relay(0, size - 2 + core).start()

    @pl.when(me == near)
    def _():
        to_relay(1).wait_recv()
        from_relay(1, size - 1).start()

    for i in range(OBLK // PER):
        solve(i)
    for copy in smalls[3:]:
        copy.wait()

    lane128 = lax.broadcasted_iota(jnp.int32, (BLK, BLK), 1).astype(f32)
    block32 = lax.broadcasted_iota(jnp.int32, (OBLK, BLK), 0)
    count = jnp.zeros((OBLK, BLK), f32)
    for h in range(HSPAN):
        for r in range(2):
            ghost = hg_v[2 * h + r : 2 * h + r + 1, :]
            spread = jnp.broadcast_to(ghost & (BLK - 1), (BLK, BLK)).astype(f32)
            low = jnp.where(jnp.transpose(spread) == lane128, 1.0, 0.0).astype(bf16)
            high = jnp.where(r < rows_s[0, h], ghost >> 7, -1)
            low_t[h, r * BLK : (r + 1) * BLK, :] = low
            spread = jnp.broadcast_to(high, (BLK, BLK)).astype(f32)
            high_t[h, r * BLK : (r + 1) * BLK, :] = jnp.transpose(spread).astype(bf16)
            here = jnp.where(block32 == high, 1.0, 0.0).astype(bf16)
            count = count + jnp.dot(here, low, preferred_element_type=f32)
    quarter = 0.25 * wet_v[...].astype(f32)
    quarter_o[...] = quarter
    scale[...] = 1.0 - quarter * count

    lane = lax.broadcasted_iota(jnp.int32, (OBLK, BLK), 1)
    target = jnp.full((OBLK, BLK), -1, jnp.int32)
    used = jnp.zeros((OBLK, BLK), jnp.int32)
    for d in range(SPAN):
        used = jnp.where(lane // CAP == d, cnt_s[0, d], used)
        for c in range(CAP):
            target = jnp.where(lane == d * CAP + c, tgt_s[d, 0, c], target)
    here = (target == block32) & (lane % CAP < used)
    place = jnp.where(here, 1.0, 0.0).astype(bf16)[:, :48]
    contrib[320:384, :] = jnp.zeros((64, BLK), f32)

    wcopy.wait()
    slot = lax.broadcasted_iota(jnp.int32, (32, BLK), 0) // F
    for i in range(SPAN):
        d = i + top * (SPAN - 1 - 2 * i)
        if i != SPAN // 2:
            pltpu.make_async_remote_copy(
                src_ref=outg.at[d], dst_ref=arr.at[d], send_sem=fs.at[d], recv_sem=fr.at[d],
                device_id=(at(1),), device_id_type=MESH,
            ).wait_recv()
        for g in range(2):
            c = 4 * g
            pieces = arr[d, c * F : (c + 4) * F, :].astype(f32)
            even = jnp.where(slot % 2 == 0, pieces, 0.0)
            odd = jnp.where(slot % 2 == 1, pieces, 0.0)
            lhs = jnp.concatenate([even, odd], axis=1).astype(bf16)
            rhs = jnp.concatenate(
                [
                    jnp.concatenate([w[d, c], w[d, c + 2]], axis=1),
                    jnp.concatenate([w[d, c + 1], w[d, c + 3]], axis=1),
                ],
                axis=0,
            )
            both = jnp.dot(lhs, rhs, preferred_element_type=f32)
            rows = pl.ds(pl.multiple_of((d * CAP + c) * F, 4 * F), 4 * F)
            contrib[rows, :] = jnp.where(slot < 2, both[:, :BLK], both[:, BLK:])

    wetf = wet_v[...].astype(f32)
    acc = [jnp.zeros((OBLK, BLK), f32) for _ in range(NTR)]
    for k in range(F // 2):
        pair = jnp.concatenate(
            [contrib[pl.ds(2 * k, 48, stride=F), :], contrib[pl.ds(2 * k + 1, 48, stride=F), :]],
            axis=1,
        )
        c1, c2, c3 = split3(pair)
        total = jnp.dot(place, c1, preferred_element_type=f32)
        total = total + jnp.dot(place, c2, preferred_element_type=f32)
        total = total + jnp.dot(place, c3, preferred_element_type=f32)
        for q in range(2):
            f = 2 * k + q
            flux_f = total[:, q * BLK : (q + 1) * BLK] * wetf
            ofs[pl.ds(f, OBLK, stride=F), :] = flux_f
            for t in range(NTR):
                acc[t] = acc[t] + coup_s[t, f] * flux_f
    for t in range(NTR):
        surf[t] = acc[t]

    sub = lax.broadcasted_iota(jnp.int32, (BLK, 2 * BLK), 0)

    def halo_copy(h, t):
        offset = h - 2 + h // 2
        return pltpu.make_async_remote_copy(
            src_ref=hout.at[h, t], dst_ref=v.at[h, t],
            send_sem=hsend.at[h, t], recv_sem=hrecv.at[h, t],
            device_id=(at(offset),), device_id_type=MESH,
        )

    for n, h in enumerate(sends):
        row = jnp.concatenate([hs_v[pl.ds(2 * h, 1), :], hs_v[pl.ds(2 * h + 1, 1), :]], axis=1)
        low = jnp.where(sub == (row & (BLK - 1)), 1.0, 0.0).astype(bf16)
        high = jnp.broadcast_to((row >> 7).astype(f32), (BLK, 2 * BLK)).astype(bf16)
        for part in ((0,), (1,)) if n == 0 else ((0, 1),):
            rows = slice(part[0] * LEV, (part[-1] + 1) * LEV)
            picked = jnp.zeros((len(part) * LEV, 2 * BLK), f32)
            for k in range(OBLK // 2):
                tables, tiles = [], []
                for b in (2 * k, 2 * k + 1):
                    tables.append(jnp.where(high == jnp.array(b, bf16), low, jnp.zeros_like(low)))
                    if n == 0:
                        first = jnp.broadcast_to(m[b, :, 0:1], (LEV, BLK))
                        for t in part:
                            mixed = x[b, t] + first * surf[t, b : b + 1, :]
                            x[b, t] = mixed * scale[b : b + 1, :]
                            tiles.append(mixed.astype(bf16))
                if n == 0:
                    tile = jnp.concatenate(tiles, axis=1)
                    sent[k, rows] = tile
                else:
                    tile = sent[k, rows]
                picked = picked + jnp.dot(
                    tile, jnp.concatenate(tables, axis=0), preferred_element_type=f32
                )
            for j, t in enumerate(part):
                hout[h, t] = picked[j * LEV : (j + 1) * LEV].astype(bf16)
                halo_copy(h, t).start()

    for b in range(OBLK):
        line[:, b * BLK : (b + 1) * BLK] = ofs[b * F : (b + 1) * F, :]
    last = order[-1]
    last_low[...] = low_t[last]
    last_high[...] = high_t[last]

    for h in order[:-1]:
        for t in range(NTR):
            halo_copy(h, t).wait_recv()
        values = jnp.concatenate([v[h, 0], v[h, 1]], axis=0)
        add_values(x, values, low_t[h], high_t[h], quarter_o)
    for t in range(NTR):
        halo_copy(last, t).wait_recv()
        last_v[t * LEV : (t + 1) * LEV] = v[last, t]
    for copy in flux:
        copy.wait_send()
    pl.when(at_relay)(from_relay(0, size - 2 + core).wait_send)
    pl.when(me == near)(from_relay(1, size - 1).wait_send)
    for h in order:
        for t in range(NTR):
            halo_copy(h, t).wait_send()


def add_values(x, values, low, high, quarter_v, out=None, ready=None):
    out = x if out is None else out
    for k in range(OBLK // 2):
        tables = []
        for b in (2 * k, 2 * k + 1):
            here = high == jnp.array(b, bf16)
            tables.append(jnp.where(here, low, jnp.zeros_like(low)))
        total = jnp.dot(values, jnp.concatenate(tables, axis=1), preferred_element_type=f32)
        for j, b in enumerate((2 * k, 2 * k + 1)):
            weight = quarter_v[b : b + 1, :]
            for t in range(NTR):
                piece = total[t * LEV : (t + 1) * LEV, j * BLK : (j + 1) * BLK]
                out[b, t] = x[b, t] + weight * piece
                if ready is not None:
                    ready(b, t)


def scatter(x, line, values_v, low_v, high_v, quarter_v, flux_o, out_o, stage, sem, fsem):
    fcopy = pltpu.make_async_copy(line, flux_o, fsem)
    fcopy.start()

    def ready(b, t):
        cols = slice(b * BLK, (b + 1) * BLK)
        pltpu.make_async_copy(stage.at[b, t], out_o.at[t, :, cols], sem).start()

    add_values(x, values_v[...], low_v[...], high_v[...], quarter_v, stage, ready)
    pltpu.make_async_copy(out_o, out_o, sem).wait()
    fcopy.wait()


def body(
    atm_flux, remap_send, remap_target, remap_counts, remap_weights, coupling,
    tracer, wet, mix_inverse, halo_send, halo_ghost, halo_rows,
):
    size = lax.axis_size("patch")
    far = lambda a: pltpu.with_memory_space_constraint(a, pltpu.HBM)
    vmem = pl.BlockSpec(memory_space=pltpu.VMEM)
    hbm = pl.BlockSpec(memory_space=pltpu.HBM)
    dma = pltpu.SemaphoreType.DMA
    i32 = jnp.int32
    picks = 2 * BLK
    between = pl.pallas_call(
        functools.partial(couple, size),
        name="couple",
        out_shape=(
            jax.ShapeDtypeStruct((OBLK, NTR, LEV, BLK), f32),
            jax.ShapeDtypeStruct((F, OC), f32),
            jax.ShapeDtypeStruct((NTR * LEV, picks), bf16),
            jax.ShapeDtypeStruct((picks, BLK), bf16),
            jax.ShapeDtypeStruct((picks, BLK), bf16),
            jax.ShapeDtypeStruct((OBLK, BLK), f32),
        ),
        in_specs=[hbm] * 12,
        out_specs=(vmem,) * 6,
        scratch_shapes=[
            pltpu.SMEM((SPAN, 1, CAP), i32),
            pltpu.SMEM((SPAN, 1, CAP), i32),
            pltpu.SMEM((1, SPAN), i32),
            pltpu.SMEM((NTR, F), f32),
            pltpu.SMEM((1, HSPAN), i32),
            pltpu.VMEM((F, ABLK * BLK), bf16),
            pltpu.VMEM((2 * HSPAN, BLK), i32),
            pltpu.VMEM((2 * HSPAN, BLK), i32),
            pltpu.VMEM((OBLK, BLK), i32),
            pltpu.VMEM((OBLK, LEV, LEV), f32),
            pltpu.VMEM((SPAN, CAP, BLK, BLK), bf16),
            pltpu.VMEM((32 * F, BLK), f32),
            pltpu.VMEM((SPAN, CAP * F, BLK), bf16),
            pltpu.VMEM((2, CAP * F, BLK), bf16),
            pltpu.VMEM((SPAN, CAP * F, BLK), bf16),
            pltpu.VMEM((48 * F, BLK), f32),
            pltpu.VMEM((OBLK * F, BLK), f32),
            pltpu.VMEM((NTR, OBLK, BLK), f32),
            pltpu.VMEM((OBLK, BLK), f32),
            pltpu.VMEM((OBLK // 2, NTR * LEV, 2 * BLK), bf16),
            pltpu.VMEM((HSPAN, picks, BLK), bf16),
            pltpu.VMEM((HSPAN, picks, BLK), bf16),
            pltpu.VMEM((HSPAN, NTR, LEV, picks), bf16),
            pltpu.VMEM((HSPAN, NTR, LEV, picks), bf16),
            dma((9,)), dma((OBLK // PER,)), dma((OBLK // PER,)), dma(()),
            dma((SPAN,)), dma((SPAN,)), dma((2,)), dma((2,)), dma((HSPAN, NTR)), dma((HSPAN, NTR)),
        ],
        compiler_params=pltpu.CompilerParams(
            collective_id=0, has_side_effects=True, vmem_limit_bytes=24 * 1024 * 1024
        ),
    )(
        far(jnp.transpose(remap_send, (1, 0, 2))), far(jnp.transpose(remap_target, (1, 0, 2))),
        far(remap_counts), far(coupling), far(halo_rows), far(atm_flux),
        far(halo_send.reshape(2 * HSPAN, BLK)), far(halo_ghost.reshape(2 * HSPAN, BLK)),
        far(wet.reshape(OBLK, BLK)), far(tracer), far(mix_inverse),
        far(remap_weights.reshape(SPAN, CAP, BLK, BLK)),
    )
    return pl.pallas_call(
        scatter,
        name="scatter",
        out_shape=(
            jax.ShapeDtypeStruct((F, OC), f32),
            jax.ShapeDtypeStruct((NTR, LEV, OC), f32),
        ),
        in_specs=[vmem] * 6,
        out_specs=(hbm, hbm),
        scratch_shapes=[pltpu.VMEM((OBLK, NTR, LEV, BLK), f32), dma(()), dma(())],
        compiler_params=pltpu.CompilerParams(vmem_limit_bytes=16 * 1024 * 1024),
    )(*between)


def solution(mesh):
    return jax.shard_map(
        body,
        mesh=mesh,
        in_specs=(
            P(None, "patch"),
            P("patch", None, None),
            P("patch", None, None),
            P("patch", None),
            P("patch", None, None, None, None),
            P(),
            P(None, None, "patch"),
            P("patch"),
            P("patch", None, None),
            P("patch", None, None, None),
            P("patch", None, None, None),
            P("patch", None),
        ),
        out_specs=(P(None, "patch"), P(None, None, "patch")),
        check_vma=False,
    )
```

```python
import functools

import jax
import jax.numpy as jnp
from jax import lax
from jax.experimental import pallas as pl
from jax.experimental.pallas import tpu as pltpu
from jax.sharding import PartitionSpec as P

F = 8
LEV = 128
NTR = 2
BLK = 128
ABLK = 24
OBLK = 32
CAP = 8
SPAN = 5
HSPAN = 4
OC = 4096
PER = 8
FLUX_OFFSETS = (-2, -1, 0, 1, 2)
HALO_OFFSETS = (-2, -1, 1, 2)
SEND_ORDERS = ((3, 0, 2, 1), (0, 1, 3, 2), (3, 0, 2, 1), (3, 2, 0, 1))
WAIT_ORDERS = (((3, 2, 1, 0), (3, 2, 0, 1)), ((0, 1, 3, 2), (0, 1, 2, 3)))
LINE = 4
MESH = pl.DeviceIdType.MESH
f32 = jnp.float32
bf16 = jnp.bfloat16


def split2(v):
    hi = v.astype(bf16)
    lo = (v - hi.astype(f32)).astype(bf16)
    return hi, lo


def split3(v):
    hi, rest = v.astype(bf16), None
    rest = v - hi.astype(f32)
    mid = rest.astype(bf16)
    low = (rest - mid.astype(f32)).astype(bf16)
    return hi, mid, low


def couple(
    size,
    send_h, tgt_h, cnt_h, coup_h, rows_h, atm_h, hs_h, hg_h, wet_h, tracer_h, mix_h, w_h,
    x, line, last_v, last_low, last_high, quarter_o,
    send_s, tgt_s, cnt_s, coup_s, rows_s, atm_v, hs_v, hg_v, wet_v,
    m, w, blocks, outg, relay, arr, contrib, ofs, surf, scale, sent, low_t, high_t, hout, v,
    small, xsem, msem, wsem, fs, fr, rs, rr, hsend, hrecv,
):
    me = lax.axis_index("patch")

    def at(offset):
        return lax.rem(me + (offset + size), size)

    plane = size // LINE
    near = 2 * LINE - 1
    spot = lax.rem(me, plane)
    level = me // plane
    closing = (level + 1) // LINE
    relay_spot = closing + near * (1 - closing)
    mine = me - spot + relay_spot
    opening = (LINE - level) // LINE
    theirs = at(-plane) - spot + opening + near * (1 - opening)
    at_relay = me == mine

    barrier = pltpu.get_barrier_semaphore()

    def hello(device):
        pl.semaphore_signal(barrier, inc=1, device_id=(device,), device_id_type=MESH)

    for offset in HALO_OFFSETS:
        if offset < 0:
            hello(at(offset))
        else:
            pl.when(spot + offset < plane)(functools.partial(hello, at(offset)))
    pl.when(spot >= plane - 2)(functools.partial(hello, mine))
    pl.when(spot < 2)(functools.partial(hello, theirs))
    last_pair = me - spot + plane - 2
    next_pair = lax.rem(me - spot + plane, size)

    @pl.when(at_relay)
    def _():
        for c in range(2):
            hello(next_pair + c)

    chip = lax.rem(me // 2, LINE)
    top = (chip + 1) // LINE
    foot = (LINE - chip) // LINE
    upper = chip // (LINE // 2)
    core = lax.rem(me, 2)

    def choose(i):
        high, low = WAIT_ORDERS
        above = high[0][i] * (1 - core) + high[1][i] * core
        below = low[0][i] * (1 - core) + low[1][i] * core
        return above * upper + below * (1 - upper)

    order = [choose(i) for i in range(HSPAN)]
    second = (1 - foot) * (1 - upper)
    third = (1 - top) * upper
    places = (foot, second, third, top)
    sends = [sum(SEND_ORDERS[y][i] * places[y] for y in range(LINE)) for i in range(HSPAN)]

    pairs = (
        (send_h, send_s), (atm_h, atm_v), (wet_h, wet_v), (hs_h, hs_v), (hg_h, hg_v),
        (tgt_h, tgt_s), (cnt_h, cnt_s), (coup_h, coup_s), (rows_h, rows_s),
    )
    smalls = [pltpu.make_async_copy(src, dst, small.at[i]) for i, (src, dst) in enumerate(pairs)]
    for copy in smalls:
        copy.start()

    def xcopy(b, t):
        cols = pl.ds(pl.multiple_of(b * BLK, BLK), BLK)
        return pltpu.make_async_copy(tracer_h.at[t, :, cols], x.at[b, t], xsem.at[b // PER])

    def mcopy(i):
        rows = pl.ds(i * PER, PER)
        return pltpu.make_async_copy(mix_h.at[rows], m.at[rows], msem.at[i])

    wcopy = pltpu.make_async_copy(w_h, w, wsem)

    def fetch(i):
        mcopy(i).start()
        for b in range(i * PER, (i + 1) * PER):
            for t in range(NTR):
                xcopy(b, t).start()

    for copy in smalls[:3]:
        copy.wait()
    fetch(0)
    fetch(1)
    slots = SPAN * CAP
    row40 = lax.broadcasted_iota(jnp.int32, (slots, BLK), 0)
    lane40 = lax.broadcasted_iota(jnp.int32, (slots, BLK), 1)
    want = jnp.full((slots, BLK), -1, jnp.int32)
    for d in range(SPAN):
        for c in range(CAP):
            want = jnp.where(row40 == d * CAP + c, send_s[d, 0, c], want)
    chooser = jnp.where(want == lane40, 1.0, 0.0).astype(bf16)[:, :32]
    for a in range(ABLK):
        blocks[a * F : (a + 1) * F, :] = atm_v[:, a * BLK : (a + 1) * BLK].astype(f32)
    blocks[ABLK * F :, :] = jnp.zeros(((32 - ABLK) * F, BLK), f32)
    for k in range(F // 2):
        pair = jnp.concatenate(
            [blocks[pl.ds(2 * k, 32, stride=F), :], blocks[pl.ds(2 * k + 1, 32, stride=F), :]],
            axis=1,
        )
        chosen = jnp.dot(chooser, pair.astype(bf16), preferred_element_type=f32)
        for q in range(2):
            contrib[pl.ds(2 * k + q, slots, stride=F), :] = chosen[:, q * BLK : (q + 1) * BLK]
    for d in range(SPAN):
        rows = contrib[d * CAP * F : (d + 1) * CAP * F, :].astype(bf16)
        if FLUX_OFFSETS[d] == 0:
            arr[d] = rows
        else:
            outg[d] = rows

    for i in range(2, OBLK // PER):
        fetch(i)
    wcopy.start()

    def solve(i):
        mcopy(i).wait()
        chunk = x.at[pl.ds(i * PER, PER)]
        pltpu.make_async_copy(chunk, chunk, xsem.at[i]).wait()
        for b in range(i * PER, (i + 1) * PER):
            a1, a2 = split2(m[b])
            t = jnp.concatenate([x[b, 0], x[b, 1]], axis=1)
            b1, b2 = split2(t)
            lhs = jnp.concatenate(
                [jnp.concatenate([a1, a1], axis=1), jnp.concatenate([a2, a2], axis=1)], axis=0
            )
            rhs = jnp.concatenate([b1, b2], axis=0)
            both = jnp.dot(lhs, rhs, preferred_element_type=f32)
            solved = both[:LEV] + both[LEV:]
            row = wet_v[b : b + 1, :]
            wet = jnp.concatenate([row, row], axis=1) > 0
            base = jnp.where(wet, solved, t)
            x[b, 0] = base[:, :BLK]
            x[b, 1] = base[:, BLK:]

    greeted = len(HALO_OFFSETS)
    pl.when(at_relay)(functools.partial(pl.semaphore_wait, barrier, 2 * greeted))
    pl.when(spot == 0)(functools.partial(pl.semaphore_wait, barrier, greeted - 1))
    pl.when((spot != 0) & jnp.logical_not(at_relay))(
        functools.partial(pl.semaphore_wait, barrier, greeted)
    )

    def flux_copy(d):
        return pltpu.make_async_remote_copy(
            src_ref=outg.at[d], dst_ref=arr.at[d], send_sem=fs.at[d], recv_sem=fr.at[d],
            device_id=(at(FLUX_OFFSETS[d]),), device_id_type=MESH,
        )

    def to_relay(d, c):
        slot = d + 2 * c
        return pltpu.make_async_remote_copy(
            src_ref=outg.at[d], dst_ref=relay.at[slot], send_sem=fs.at[d], recv_sem=rr.at[slot],
            device_id=(theirs,), device_id_type=MESH,
        )

    def from_relay(slot):
        d, c = ((0, 0), (1, 1), (0, 1))[slot]
        return pltpu.make_async_remote_copy(
            src_ref=relay.at[slot], dst_ref=arr.at[d], send_sem=rs.at[slot], recv_sem=fr.at[d],
            device_id=(last_pair + c,), device_id_type=MESH,
        )

    flux = []
    for d in range(SPAN):
        offset = FLUX_OFFSETS[d]
        if offset == 0:
            continue
        flux.append(flux_copy(d))
        if offset > 0:
            flux[-1].start()
        else:
            pl.when(spot + offset >= 0)(flux[-1].start)
            for c in range(-offset):
                pl.when(spot == c)(to_relay(d, c).start)

    @pl.when(at_relay)
    def _():
        for slot, (d, c) in enumerate(((0, 0), (1, 0), (0, 1))):
            to_relay(d, c).wait_recv()
            from_relay(slot).start()

    for i in range(OBLK // PER):
        solve(i)
    for copy in smalls[3:]:
        copy.wait()

    lane128 = lax.broadcasted_iota(jnp.int32, (BLK, BLK), 1).astype(f32)
    block32 = lax.broadcasted_iota(jnp.int32, (OBLK, BLK), 0)
    count = jnp.zeros((OBLK, BLK), f32)
    for h in range(HSPAN):
        for r in range(2):
            ghost = hg_v[2 * h + r : 2 * h + r + 1, :]
            spread = jnp.broadcast_to(ghost & (BLK - 1), (BLK, BLK)).astype(f32)
            low = jnp.where(jnp.transpose(spread) == lane128, 1.0, 0.0).astype(bf16)
            high = jnp.where(r < rows_s[0, h], ghost >> 7, -1)
            low_t[h, r * BLK : (r + 1) * BLK, :] = low
            spread = jnp.broadcast_to(high, (BLK, BLK)).astype(f32)
            high_t[h, r * BLK : (r + 1) * BLK, :] = jnp.transpose(spread).astype(bf16)
            here = jnp.where(block32 == high, 1.0, 0.0).astype(bf16)
            count = count + jnp.dot(here, low, preferred_element_type=f32)
    quarter = 0.25 * wet_v[...].astype(f32)
    quarter_o[...] = quarter
    scale[...] = 1.0 - quarter * count

    lane = lax.broadcasted_iota(jnp.int32, (OBLK, BLK), 1)
    target = jnp.full((OBLK, BLK), -1, jnp.int32)
    used = jnp.zeros((OBLK, BLK), jnp.int32)
    for d in range(SPAN):
        used = jnp.where(lane // CAP == d, cnt_s[0, d], used)
        for c in range(CAP):
            target = jnp.where(lane == d * CAP + c, tgt_s[d, 0, c], target)
    here = (target == block32) & (lane % CAP < used)
    place = jnp.where(here, 1.0, 0.0).astype(bf16)[:, :48]
    contrib[320:384, :] = jnp.zeros((64, BLK), f32)

    wcopy.wait()
    slot = lax.broadcasted_iota(jnp.int32, (32, BLK), 0) // F
    for i in range(SPAN):
        d = i + top * (SPAN - 1 - 2 * i)
        if i != SPAN // 2:
            pltpu.make_async_remote_copy(
                src_ref=outg.at[d], dst_ref=arr.at[d], send_sem=fs.at[d], recv_sem=fr.at[d],
                device_id=(at(1),), device_id_type=MESH,
            ).wait_recv()
        for g in range(2):
            c = 4 * g
            pieces = arr[d, c * F : (c + 4) * F, :].astype(f32)
            even = jnp.where(slot % 2 == 0, pieces, 0.0)
            odd = jnp.where(slot % 2 == 1, pieces, 0.0)
            lhs = jnp.concatenate([even, odd], axis=1).astype(bf16)
            rhs = jnp.concatenate(
                [
                    jnp.concatenate([w[d, c], w[d, c + 2]], axis=1),
                    jnp.concatenate([w[d, c + 1], w[d, c + 3]], axis=1),
                ],
                axis=0,
            )
            both = jnp.dot(lhs, rhs, preferred_element_type=f32)
            rows = pl.ds(pl.multiple_of((d * CAP + c) * F, 4 * F), 4 * F)
            contrib[rows, :] = jnp.where(slot < 2, both[:, :BLK], both[:, BLK:])

    wetf = wet_v[...].astype(f32)
    acc = [jnp.zeros((OBLK, BLK), f32) for _ in range(NTR)]
    for k in range(F // 2):
        pair = jnp.concatenate(
            [contrib[pl.ds(2 * k, 48, stride=F), :], contrib[pl.ds(2 * k + 1, 48, stride=F), :]],
            axis=1,
        )
        c1, c2, c3 = split3(pair)
        total = jnp.dot(place, c1, preferred_element_type=f32)
        total = total + jnp.dot(place, c2, preferred_element_type=f32)
        total = total + jnp.dot(place, c3, preferred_element_type=f32)
        for q in range(2):
            f = 2 * k + q
            flux_f = total[:, q * BLK : (q + 1) * BLK] * wetf
            ofs[pl.ds(f, OBLK, stride=F), :] = flux_f
            for t in range(NTR):
                acc[t] = acc[t] + coup_s[t, f] * flux_f
    for t in range(NTR):
        surf[t] = acc[t]

    sub = lax.broadcasted_iota(jnp.int32, (BLK, 2 * BLK), 0)

    def halo_copy(h, t):
        offset = h - 2 + h // 2
        return pltpu.make_async_remote_copy(
            src_ref=hout.at[h, t], dst_ref=v.at[h, t],
            send_sem=hsend.at[h, t], recv_sem=hrecv.at[h, t],
            device_id=(at(offset),), device_id_type=MESH,
        )

    for n, h in enumerate(sends):
        row = jnp.concatenate([hs_v[pl.ds(2 * h, 1), :], hs_v[pl.ds(2 * h + 1, 1), :]], axis=1)
        low = jnp.where(sub == (row & (BLK - 1)), 1.0, 0.0).astype(bf16)
        high = jnp.broadcast_to((row >> 7).astype(f32), (BLK, 2 * BLK)).astype(bf16)
        for part in ((0,), (1,)) if n == 0 else ((0, 1),):
            rows = slice(part[0] * LEV, (part[-1] + 1) * LEV)
            picked = jnp.zeros((len(part) * LEV, 2 * BLK), f32)
            for k in range(OBLK // 2):
                tables, tiles = [], []
                for b in (2 * k, 2 * k + 1):
                    tables.append(jnp.where(high == jnp.array(b, bf16), low, jnp.zeros_like(low)))
                    if n == 0:
                        first = jnp.broadcast_to(m[b, :, 0:1], (LEV, BLK))
                        for t in part:
                            mixed = x[b, t] + first * surf[t, b : b + 1, :]
                            x[b, t] = mixed * scale[b : b + 1, :]
                            tiles.append(mixed.astype(bf16))
                if n == 0:
                    tile = jnp.concatenate(tiles, axis=1)
                    sent[k, rows] = tile
                else:
                    tile = sent[k, rows]
                picked = picked + jnp.dot(
                    tile, jnp.concatenate(tables, axis=0), preferred_element_type=f32
                )
            for j, t in enumerate(part):
                hout[h, t] = picked[j * LEV : (j + 1) * LEV].astype(bf16)
                halo_copy(h, t).start()

    for b in range(OBLK):
        line[:, b * BLK : (b + 1) * BLK] = ofs[b * F : (b + 1) * F, :]
    last = order[-1]
    last_low[...] = low_t[last]
    last_high[...] = high_t[last]

    for h in order[:-1]:
        for t in range(NTR):
            halo_copy(h, t).wait_recv()
        values = jnp.concatenate([v[h, 0], v[h, 1]], axis=0)
        add_values(x, values, low_t[h], high_t[h], quarter_o)
    for t in range(NTR):
        halo_copy(last, t).wait_recv()
        last_v[t * LEV : (t + 1) * LEV] = v[last, t]
    for copy in flux:
        copy.wait_send()

    @pl.when(at_relay)
    def _():
        for slot in range(3):
            from_relay(slot).wait_send()

    for h in order:
        for t in range(NTR):
            halo_copy(h, t).wait_send()


def add_values(x, values, low, high, quarter_v, out=None, ready=None):
    out = x if out is None else out
    for k in range(OBLK // 2):
        tables = []
        for b in (2 * k, 2 * k + 1):
            here = high == jnp.array(b, bf16)
            tables.append(jnp.where(here, low, jnp.zeros_like(low)))
        total = jnp.dot(values, jnp.concatenate(tables, axis=1), preferred_element_type=f32)
        for j, b in enumerate((2 * k, 2 * k + 1)):
            weight = quarter_v[b : b + 1, :]
            for t in range(NTR):
                piece = total[t * LEV : (t + 1) * LEV, j * BLK : (j + 1) * BLK]
                out[b, t] = x[b, t] + weight * piece
                if ready is not None:
                    ready(b, t)


def scatter(x, line, values_v, low_v, high_v, quarter_v, flux_o, out_o, stage, sem, fsem):
    fcopy = pltpu.make_async_copy(line, flux_o, fsem)
    fcopy.start()

    def ready(b, t):
        cols = slice(b * BLK, (b + 1) * BLK)
        pltpu.make_async_copy(stage.at[b, t], out_o.at[t, :, cols], sem).start()

    add_values(x, values_v[...], low_v[...], high_v[...], quarter_v, stage, ready)
    pltpu.make_async_copy(out_o, out_o, sem).wait()
    fcopy.wait()


def body(
    atm_flux, remap_send, remap_target, remap_counts, remap_weights, coupling,
    tracer, wet, mix_inverse, halo_send, halo_ghost, halo_rows,
):
    size = lax.axis_size("patch")
    far = lambda a: pltpu.with_memory_space_constraint(a, pltpu.HBM)
    vmem = pl.BlockSpec(memory_space=pltpu.VMEM)
    hbm = pl.BlockSpec(memory_space=pltpu.HBM)
    dma = pltpu.SemaphoreType.DMA
    i32 = jnp.int32
    picks = 2 * BLK
    between = pl.pallas_call(
        functools.partial(couple, size),
        name="couple",
        out_shape=(
            jax.ShapeDtypeStruct((OBLK, NTR, LEV, BLK), f32),
            jax.ShapeDtypeStruct((F, OC), f32),
            jax.ShapeDtypeStruct((NTR * LEV, picks), bf16),
            jax.ShapeDtypeStruct((picks, BLK), bf16),
            jax.ShapeDtypeStruct((picks, BLK), bf16),
            jax.ShapeDtypeStruct((OBLK, BLK), f32),
        ),
        in_specs=[hbm] * 12,
        out_specs=(vmem,) * 6,
        scratch_shapes=[
            pltpu.SMEM((SPAN, 1, CAP), i32),
            pltpu.SMEM((SPAN, 1, CAP), i32),
            pltpu.SMEM((1, SPAN), i32),
            pltpu.SMEM((NTR, F), f32),
            pltpu.SMEM((1, HSPAN), i32),
            pltpu.VMEM((F, ABLK * BLK), bf16),
            pltpu.VMEM((2 * HSPAN, BLK), i32),
            pltpu.VMEM((2 * HSPAN, BLK), i32),
            pltpu.VMEM((OBLK, BLK), i32),
            pltpu.VMEM((OBLK, LEV, LEV), f32),
            pltpu.VMEM((SPAN, CAP, BLK, BLK), bf16),
            pltpu.VMEM((32 * F, BLK), f32),
            pltpu.VMEM((SPAN, CAP * F, BLK), bf16),
            pltpu.VMEM((3, CAP * F, BLK), bf16),
            pltpu.VMEM((SPAN, CAP * F, BLK), bf16),
            pltpu.VMEM((48 * F, BLK), f32),
            pltpu.VMEM((OBLK * F, BLK), f32),
            pltpu.VMEM((NTR, OBLK, BLK), f32),
            pltpu.VMEM((OBLK, BLK), f32),
            pltpu.VMEM((OBLK // 2, NTR * LEV, 2 * BLK), bf16),
            pltpu.VMEM((HSPAN, picks, BLK), bf16),
            pltpu.VMEM((HSPAN, picks, BLK), bf16),
            pltpu.VMEM((HSPAN, NTR, LEV, picks), bf16),
            pltpu.VMEM((HSPAN, NTR, LEV, picks), bf16),
            dma((9,)), dma((OBLK // PER,)), dma((OBLK // PER,)), dma(()),
            dma((SPAN,)), dma((SPAN,)), dma((3,)), dma((3,)), dma((HSPAN, NTR)), dma((HSPAN, NTR)),
        ],
        compiler_params=pltpu.CompilerParams(
            collective_id=0, has_side_effects=True, vmem_limit_bytes=24 * 1024 * 1024
        ),
    )(
        far(jnp.transpose(remap_send, (1, 0, 2))), far(jnp.transpose(remap_target, (1, 0, 2))),
        far(remap_counts), far(coupling), far(halo_rows), far(atm_flux),
        far(halo_send.reshape(2 * HSPAN, BLK)), far(halo_ghost.reshape(2 * HSPAN, BLK)),
        far(wet.reshape(OBLK, BLK)), far(tracer), far(mix_inverse),
        far(remap_weights.reshape(SPAN, CAP, BLK, BLK)),
    )
    return pl.pallas_call(
        scatter,
        name="scatter",
        out_shape=(
            jax.ShapeDtypeStruct((F, OC), f32),
            jax.ShapeDtypeStruct((NTR, LEV, OC), f32),
        ),
        in_specs=[vmem] * 6,
        out_specs=(hbm, hbm),
        scratch_shapes=[pltpu.VMEM((OBLK, NTR, LEV, BLK), f32), dma(()), dma(())],
        compiler_params=pltpu.CompilerParams(vmem_limit_bytes=16 * 1024 * 1024),
    )(*between)


def solution(mesh):
    return jax.shard_map(
        body,
        mesh=mesh,
        in_specs=(
            P(None, "patch"),
            P("patch", None, None),
            P("patch", None, None),
            P("patch", None),
            P("patch", None, None, None, None),
            P(),
            P(None, None, "patch"),
            P("patch"),
            P("patch", None, None),
            P("patch", None, None, None),
            P("patch", None, None, None),
            P("patch", None),
        ),
        out_specs=(P(None, "patch"), P(None, None, "patch")),
        check_vma=False,
    )
```

```python
import functools

import jax
import jax.numpy as jnp
from jax import lax
from jax.experimental import pallas as pl
from jax.experimental.pallas import tpu as pltpu
from jax.sharding import PartitionSpec as P

F = 8
LEV = 128
NTR = 2
BLK = 128
ABLK = 24
OBLK = 32
CAP = 8
SPAN = 5
HSPAN = 4
OC = 4096
PER = 8
FLUX_OFFSETS = (-2, -1, 0, 1, 2)
HALO_OFFSETS = (-2, -1, 1, 2)
SEND_ORDERS = ((3, 0, 2, 1), (0, 1, 3, 2), (3, 0, 2, 1), (3, 2, 0, 1))
WAIT_ORDERS = (((3, 2, 1, 0), (3, 2, 0, 1)), ((0, 1, 3, 2), (0, 1, 2, 3)))
LINE = 4
MESH = pl.DeviceIdType.MESH
f32 = jnp.float32
bf16 = jnp.bfloat16


def split2(v):
    hi = v.astype(bf16)
    lo = (v - hi.astype(f32)).astype(bf16)
    return hi, lo


def split3(v):
    hi, rest = v.astype(bf16), None
    rest = v - hi.astype(f32)
    mid = rest.astype(bf16)
    low = (rest - mid.astype(f32)).astype(bf16)
    return hi, mid, low


def couple(
    size,
    send_h, tgt_h, cnt_h, coup_h, rows_h, atm_h, hs_h, hg_h, wet_h, tracer_h, mix_h, w_h,
    x, line, last_v, last_low, last_high, quarter_o,
    send_s, tgt_s, cnt_s, coup_s, rows_s, atm_v, hs_v, hg_v, wet_v,
    m, w, blocks, outg, relay, arr, contrib, ofs, surf, scale, sent, low_t, high_t, hout, v,
    small, xsem, msem, wsem, fs, fr, rs, rr, hsend, hrecv,
):
    me = lax.axis_index("patch")

    def at(offset):
        return lax.rem(me + (offset + size), size)

    plane = size // LINE
    near = 2 * LINE - 1
    spot = lax.rem(me, plane)
    level = me // plane
    opening = (LINE - level) // LINE
    mine = me - spot + near
    theirs = at(-plane) - spot + opening + near * (1 - opening)
    at_relay = spot == near
    at_stage = me == size - plane + 1
    last_pair = me - spot + plane - 2
    next_pair = lax.rem(me - spot + plane, size)

    barrier = pltpu.get_barrier_semaphore()

    def hello(device):
        pl.semaphore_signal(barrier, inc=1, device_id=(device,), device_id_type=MESH)

    for offset in HALO_OFFSETS:
        if offset < 0:
            hello(at(offset))
        else:
            pl.when(spot + offset < plane)(functools.partial(hello, at(offset)))
    pl.when(spot >= plane - 2)(functools.partial(hello, mine))
    pl.when(spot < 2)(functools.partial(hello, theirs))
    pl.when(me == size - plane + near)(functools.partial(hello, size - plane + 1))

    @pl.when(at_stage | (at_relay & (level < LINE - 1)))
    def _():
        for c in range(2):
            hello(next_pair + c)

    chip = lax.rem(me // 2, LINE)
    top = (chip + 1) // LINE
    foot = (LINE - chip) // LINE
    upper = chip // (LINE // 2)
    core = lax.rem(me, 2)

    def choose(i):
        high, low = WAIT_ORDERS
        above = high[0][i] * (1 - core) + high[1][i] * core
        below = low[0][i] * (1 - core) + low[1][i] * core
        return above * upper + below * (1 - upper)

    order = [choose(i) for i in range(HSPAN)]
    second = (1 - foot) * (1 - upper)
    third = (1 - top) * upper
    places = (foot, second, third, top)
    sends = [sum(SEND_ORDERS[y][i] * places[y] for y in range(LINE)) for i in range(HSPAN)]

    pairs = (
        (send_h, send_s), (atm_h, atm_v), (wet_h, wet_v), (hs_h, hs_v), (hg_h, hg_v),
        (tgt_h, tgt_s), (cnt_h, cnt_s), (coup_h, coup_s), (rows_h, rows_s),
    )
    smalls = [pltpu.make_async_copy(src, dst, small.at[i]) for i, (src, dst) in enumerate(pairs)]
    for copy in smalls:
        copy.start()

    def xcopy(b, t):
        cols = pl.ds(pl.multiple_of(b * BLK, BLK), BLK)
        return pltpu.make_async_copy(tracer_h.at[t, :, cols], x.at[b, t], xsem.at[b // PER])

    def mcopy(i):
        rows = pl.ds(i * PER, PER)
        return pltpu.make_async_copy(mix_h.at[rows], m.at[rows], msem.at[i])

    wcopy = pltpu.make_async_copy(w_h, w, wsem)

    def fetch(i):
        mcopy(i).start()
        for b in range(i * PER, (i + 1) * PER):
            for t in range(NTR):
                xcopy(b, t).start()

    for copy in smalls[:3]:
        copy.wait()
    fetch(0)
    fetch(1)
    slots = SPAN * CAP
    row40 = lax.broadcasted_iota(jnp.int32, (slots, BLK), 0)
    lane40 = lax.broadcasted_iota(jnp.int32, (slots, BLK), 1)
    want = jnp.full((slots, BLK), -1, jnp.int32)
    for d in range(SPAN):
        for c in range(CAP):
            want = jnp.where(row40 == d * CAP + c, send_s[d, 0, c], want)
    chooser = jnp.where(want == lane40, 1.0, 0.0).astype(bf16)[:, :32]
    for a in range(ABLK):
        blocks[a * F : (a + 1) * F, :] = atm_v[:, a * BLK : (a + 1) * BLK].astype(f32)
    blocks[ABLK * F :, :] = jnp.zeros(((32 - ABLK) * F, BLK), f32)
    for k in range(F // 2):
        pair = jnp.concatenate(
            [blocks[pl.ds(2 * k, 32, stride=F), :], blocks[pl.ds(2 * k + 1, 32, stride=F), :]],
            axis=1,
        )
        chosen = jnp.dot(chooser, pair.astype(bf16), preferred_element_type=f32)
        for q in range(2):
            contrib[pl.ds(2 * k + q, slots, stride=F), :] = chosen[:, q * BLK : (q + 1) * BLK]
    for d in range(SPAN):
        rows = contrib[d * CAP * F : (d + 1) * CAP * F, :].astype(bf16)
        if FLUX_OFFSETS[d] == 0:
            arr[d] = rows
        else:
            outg[d] = rows

    for i in range(2, OBLK // PER):
        fetch(i)
    wcopy.start()

    def solve(i):
        mcopy(i).wait()
        chunk = x.at[pl.ds(i * PER, PER)]
        pltpu.make_async_copy(chunk, chunk, xsem.at[i]).wait()
        for b in range(i * PER, (i + 1) * PER):
            a1, a2 = split2(m[b])
            t = jnp.concatenate([x[b, 0], x[b, 1]], axis=1)
            b1, b2 = split2(t)
            lhs = jnp.concatenate(
                [jnp.concatenate([a1, a1], axis=1), jnp.concatenate([a2, a2], axis=1)], axis=0
            )
            rhs = jnp.concatenate([b1, b2], axis=0)
            both = jnp.dot(lhs, rhs, preferred_element_type=f32)
            solved = both[:LEV] + both[LEV:]
            row = wet_v[b : b + 1, :]
            wet = jnp.concatenate([row, row], axis=1) > 0
            base = jnp.where(wet, solved, t)
            x[b, 0] = base[:, :BLK]
            x[b, 1] = base[:, BLK:]

    greeted = len(HALO_OFFSETS)
    closing = level == LINE - 1
    for who, amount in (
        (at_relay & jnp.logical_not(closing), 2 * greeted),
        (at_relay & closing, greeted + 2),
        (at_stage, greeted + 3),
        (spot == 0, greeted - 1),
        ((spot != 0) & jnp.logical_not(at_relay) & jnp.logical_not(at_stage), greeted),
    ):
        pl.when(who)(functools.partial(pl.semaphore_wait, barrier, amount))

    def flux_copy(d):
        return pltpu.make_async_remote_copy(
            src_ref=outg.at[d], dst_ref=arr.at[d], send_sem=fs.at[d], recv_sem=fr.at[d],
            device_id=(at(FLUX_OFFSETS[d]),), device_id_type=MESH,
        )

    def to_relay(d, c):
        slot = d + 2 * c
        return pltpu.make_async_remote_copy(
            src_ref=outg.at[d], dst_ref=relay.at[slot], send_sem=fs.at[d], recv_sem=rr.at[slot],
            device_id=(theirs,), device_id_type=MESH,
        )

    def from_relay(slot):
        d, c = ((0, 0), (1, 1), (0, 1))[slot]
        return pltpu.make_async_remote_copy(
            src_ref=relay.at[slot], dst_ref=arr.at[d], send_sem=rs.at[slot], recv_sem=fr.at[d],
            device_id=(last_pair + c,), device_id_type=MESH,
        )

    def from_stage(slot):
        return pltpu.make_async_remote_copy(
            src_ref=relay.at[slot], dst_ref=relay.at[slot],
            send_sem=rs.at[slot], recv_sem=rr.at[slot],
            device_id=(mine,), device_id_type=MESH,
        )

    flux = []
    for d in range(SPAN):
        offset = FLUX_OFFSETS[d]
        if offset == 0:
            continue
        flux.append(flux_copy(d))
        if offset > 0:
            flux[-1].start()
        else:
            pl.when(spot + offset >= 0)(flux[-1].start)
            for c in range(-offset):
                pl.when(spot == c)(to_relay(d, c).start)

    @pl.when(at_relay)
    def _():
        for slot, (d, c) in enumerate(((0, 0), (1, 0), (0, 1))):
            to_relay(d, c).wait_recv()
            from_relay(slot).start()

    @pl.when(at_stage)
    def _():
        for slot, (d, c) in enumerate(((0, 0), (1, 0), (0, 1))):
            to_relay(d, c).wait_recv()
            from_stage(slot).start()

    for i in range(OBLK // PER):
        solve(i)
    for copy in smalls[3:]:
        copy.wait()

    lane128 = lax.broadcasted_iota(jnp.int32, (BLK, BLK), 1).astype(f32)
    block32 = lax.broadcasted_iota(jnp.int32, (OBLK, BLK), 0)
    count = jnp.zeros((OBLK, BLK), f32)
    for h in range(HSPAN):
        for r in range(2):
            ghost = hg_v[2 * h + r : 2 * h + r + 1, :]
            spread = jnp.broadcast_to(ghost & (BLK - 1), (BLK, BLK)).astype(f32)
            low = jnp.where(jnp.transpose(spread) == lane128, 1.0, 0.0).astype(bf16)
            high = jnp.where(r < rows_s[0, h], ghost >> 7, -1)
            low_t[h, r * BLK : (r + 1) * BLK, :] = low
            spread = jnp.broadcast_to(high, (BLK, BLK)).astype(f32)
            high_t[h, r * BLK : (r + 1) * BLK, :] = jnp.transpose(spread).astype(bf16)
            here = jnp.where(block32 == high, 1.0, 0.0).astype(bf16)
            count = count + jnp.dot(here, low, preferred_element_type=f32)
    quarter = 0.25 * wet_v[...].astype(f32)
    quarter_o[...] = quarter
    scale[...] = 1.0 - quarter * count

    lane = lax.broadcasted_iota(jnp.int32, (OBLK, BLK), 1)
    target = jnp.full((OBLK, BLK), -1, jnp.int32)
    used = jnp.zeros((OBLK, BLK), jnp.int32)
    for d in range(SPAN):
        used = jnp.where(lane // CAP == d, cnt_s[0, d], used)
        for c in range(CAP):
            target = jnp.where(lane == d * CAP + c, tgt_s[d, 0, c], target)
    here = (target == block32) & (lane % CAP < used)
    place = jnp.where(here, 1.0, 0.0).astype(bf16)[:, :48]
    contrib[320:384, :] = jnp.zeros((64, BLK), f32)

    wcopy.wait()
    slot = lax.broadcasted_iota(jnp.int32, (32, BLK), 0) // F
    for i in range(SPAN):
        d = i + top * (SPAN - 1 - 2 * i)
        if i != SPAN // 2:
            pltpu.make_async_remote_copy(
                src_ref=outg.at[d], dst_ref=arr.at[d], send_sem=fs.at[d], recv_sem=fr.at[d],
                device_id=(at(1),), device_id_type=MESH,
            ).wait_recv()
        for g in range(2):
            c = 4 * g
            pieces = arr[d, c * F : (c + 4) * F, :].astype(f32)
            even = jnp.where(slot % 2 == 0, pieces, 0.0)
            odd = jnp.where(slot % 2 == 1, pieces, 0.0)
            lhs = jnp.concatenate([even, odd], axis=1).astype(bf16)
            rhs = jnp.concatenate(
                [
                    jnp.concatenate([w[d, c], w[d, c + 2]], axis=1),
                    jnp.concatenate([w[d, c + 1], w[d, c + 3]], axis=1),
                ],
                axis=0,
            )
            both = jnp.dot(lhs, rhs, preferred_element_type=f32)
            rows = pl.ds(pl.multiple_of((d * CAP + c) * F, 4 * F), 4 * F)
            contrib[rows, :] = jnp.where(slot < 2, both[:, :BLK], both[:, BLK:])

    wetf = wet_v[...].astype(f32)
    acc = [jnp.zeros((OBLK, BLK), f32) for _ in range(NTR)]
    for k in range(F // 2):
        pair = jnp.concatenate(
            [contrib[pl.ds(2 * k, 48, stride=F), :], contrib[pl.ds(2 * k + 1, 48, stride=F), :]],
            axis=1,
        )
        c1, c2, c3 = split3(pair)
        total = jnp.dot(place, c1, preferred_element_type=f32)
        total = total + jnp.dot(place, c2, preferred_element_type=f32)
        total = total + jnp.dot(place, c3, preferred_element_type=f32)
        for q in range(2):
            f = 2 * k + q
            flux_f = total[:, q * BLK : (q + 1) * BLK] * wetf
            ofs[pl.ds(f, OBLK, stride=F), :] = flux_f
            for t in range(NTR):
                acc[t] = acc[t] + coup_s[t, f] * flux_f
    for t in range(NTR):
        surf[t] = acc[t]

    sub = lax.broadcasted_iota(jnp.int32, (BLK, 2 * BLK), 0)

    def halo_copy(h, t):
        offset = h - 2 + h // 2
        return pltpu.make_async_remote_copy(
            src_ref=hout.at[h, t], dst_ref=v.at[h, t],
            send_sem=hsend.at[h, t], recv_sem=hrecv.at[h, t],
            device_id=(at(offset),), device_id_type=MESH,
        )

    for n, h in enumerate(sends):
        row = jnp.concatenate([hs_v[pl.ds(2 * h, 1), :], hs_v[pl.ds(2 * h + 1, 1), :]], axis=1)
        low = jnp.where(sub == (row & (BLK - 1)), 1.0, 0.0).astype(bf16)
        high = jnp.broadcast_to((row >> 7).astype(f32), (BLK, 2 * BLK)).astype(bf16)
        for part in ((0,), (1,)) if n == 0 else ((0, 1),):
            rows = slice(part[0] * LEV, (part[-1] + 1) * LEV)
            picked = jnp.zeros((len(part) * LEV, 2 * BLK), f32)
            for k in range(OBLK // 2):
                tables, tiles = [], []
                for b in (2 * k, 2 * k + 1):
                    tables.append(jnp.where(high == jnp.array(b, bf16), low, jnp.zeros_like(low)))
                    if n == 0:
                        first = jnp.broadcast_to(m[b, :, 0:1], (LEV, BLK))
                        for t in part:
                            mixed = x[b, t] + first * surf[t, b : b + 1, :]
                            x[b, t] = mixed * scale[b : b + 1, :]
                            tiles.append(mixed.astype(bf16))
                if n == 0:
                    tile = jnp.concatenate(tiles, axis=1)
                    sent[k, rows] = tile
                else:
                    tile = sent[k, rows]
                picked = picked + jnp.dot(
                    tile, jnp.concatenate(tables, axis=0), preferred_element_type=f32
                )
            for j, t in enumerate(part):
                hout[h, t] = picked[j * LEV : (j + 1) * LEV].astype(bf16)
                halo_copy(h, t).start()

    for b in range(OBLK):
        line[:, b * BLK : (b + 1) * BLK] = ofs[b * F : (b + 1) * F, :]
    last = order[-1]
    last_low[...] = low_t[last]
    last_high[...] = high_t[last]

    for h in order[:-1]:
        for t in range(NTR):
            halo_copy(h, t).wait_recv()
        values = jnp.concatenate([v[h, 0], v[h, 1]], axis=0)
        add_values(x, values, low_t[h], high_t[h], quarter_o)
    for t in range(NTR):
        halo_copy(last, t).wait_recv()
        last_v[t * LEV : (t + 1) * LEV] = v[last, t]
    for copy in flux:
        copy.wait_send()

    @pl.when(at_relay)
    def _():
        for slot in range(3):
            from_relay(slot).wait_send()

    @pl.when(at_stage)
    def _():
        for slot in range(3):
            from_stage(slot).wait_send()

    for h in order:
        for t in range(NTR):
            halo_copy(h, t).wait_send()


def add_values(x, values, low, high, quarter_v, out=None, ready=None):
    out = x if out is None else out
    for k in range(OBLK // 2):
        tables = []
        for b in (2 * k, 2 * k + 1):
            here = high == jnp.array(b, bf16)
            tables.append(jnp.where(here, low, jnp.zeros_like(low)))
        total = jnp.dot(values, jnp.concatenate(tables, axis=1), preferred_element_type=f32)
        for j, b in enumerate((2 * k, 2 * k + 1)):
            weight = quarter_v[b : b + 1, :]
            for t in range(NTR):
                piece = total[t * LEV : (t + 1) * LEV, j * BLK : (j + 1) * BLK]
                out[b, t] = x[b, t] + weight * piece
                if ready is not None:
                    ready(b, t)


def scatter(x, line, values_v, low_v, high_v, quarter_v, flux_o, out_o, stage, sem, fsem):
    fcopy = pltpu.make_async_copy(line, flux_o, fsem)
    fcopy.start()

    def ready(b, t):
        cols = slice(b * BLK, (b + 1) * BLK)
        pltpu.make_async_copy(stage.at[b, t], out_o.at[t, :, cols], sem).start()

    add_values(x, values_v[...], low_v[...], high_v[...], quarter_v, stage, ready)
    pltpu.make_async_copy(out_o, out_o, sem).wait()
    fcopy.wait()


def body(
    atm_flux, remap_send, remap_target, remap_counts, remap_weights, coupling,
    tracer, wet, mix_inverse, halo_send, halo_ghost, halo_rows,
):
    size = lax.axis_size("patch")
    far = lambda a: pltpu.with_memory_space_constraint(a, pltpu.HBM)
    vmem = pl.BlockSpec(memory_space=pltpu.VMEM)
    hbm = pl.BlockSpec(memory_space=pltpu.HBM)
    dma = pltpu.SemaphoreType.DMA
    i32 = jnp.int32
    picks = 2 * BLK
    between = pl.pallas_call(
        functools.partial(couple, size),
        name="couple",
        out_shape=(
            jax.ShapeDtypeStruct((OBLK, NTR, LEV, BLK), f32),
            jax.ShapeDtypeStruct((F, OC), f32),
            jax.ShapeDtypeStruct((NTR * LEV, picks), bf16),
            jax.ShapeDtypeStruct((picks, BLK), bf16),
            jax.ShapeDtypeStruct((picks, BLK), bf16),
            jax.ShapeDtypeStruct((OBLK, BLK), f32),
        ),
        in_specs=[hbm] * 12,
        out_specs=(vmem,) * 6,
        scratch_shapes=[
            pltpu.SMEM((SPAN, 1, CAP), i32),
            pltpu.SMEM((SPAN, 1, CAP), i32),
            pltpu.SMEM((1, SPAN), i32),
            pltpu.SMEM((NTR, F), f32),
            pltpu.SMEM((1, HSPAN), i32),
            pltpu.VMEM((F, ABLK * BLK), bf16),
            pltpu.VMEM((2 * HSPAN, BLK), i32),
            pltpu.VMEM((2 * HSPAN, BLK), i32),
            pltpu.VMEM((OBLK, BLK), i32),
            pltpu.VMEM((OBLK, LEV, LEV), f32),
            pltpu.VMEM((SPAN, CAP, BLK, BLK), bf16),
            pltpu.VMEM((32 * F, BLK), f32),
            pltpu.VMEM((SPAN, CAP * F, BLK), bf16),
            pltpu.VMEM((3, CAP * F, BLK), bf16),
            pltpu.VMEM((SPAN, CAP * F, BLK), bf16),
            pltpu.VMEM((48 * F, BLK), f32),
            pltpu.VMEM((OBLK * F, BLK), f32),
            pltpu.VMEM((NTR, OBLK, BLK), f32),
            pltpu.VMEM((OBLK, BLK), f32),
            pltpu.VMEM((OBLK // 2, NTR * LEV, 2 * BLK), bf16),
            pltpu.VMEM((HSPAN, picks, BLK), bf16),
            pltpu.VMEM((HSPAN, picks, BLK), bf16),
            pltpu.VMEM((HSPAN, NTR, LEV, picks), bf16),
            pltpu.VMEM((HSPAN, NTR, LEV, picks), bf16),
            dma((9,)), dma((OBLK // PER,)), dma((OBLK // PER,)), dma(()),
            dma((SPAN,)), dma((SPAN,)), dma((3,)), dma((3,)), dma((HSPAN, NTR)), dma((HSPAN, NTR)),
        ],
        compiler_params=pltpu.CompilerParams(
            collective_id=0, has_side_effects=True, vmem_limit_bytes=24 * 1024 * 1024
        ),
    )(
        far(jnp.transpose(remap_send, (1, 0, 2))), far(jnp.transpose(remap_target, (1, 0, 2))),
        far(remap_counts), far(coupling), far(halo_rows), far(atm_flux),
        far(halo_send.reshape(2 * HSPAN, BLK)), far(halo_ghost.reshape(2 * HSPAN, BLK)),
        far(wet.reshape(OBLK, BLK)), far(tracer), far(mix_inverse),
        far(remap_weights.reshape(SPAN, CAP, BLK, BLK)),
    )
    return pl.pallas_call(
        scatter,
        name="scatter",
        out_shape=(
            jax.ShapeDtypeStruct((F, OC), f32),
            jax.ShapeDtypeStruct((NTR, LEV, OC), f32),
        ),
        in_specs=[vmem] * 6,
        out_specs=(hbm, hbm),
        scratch_shapes=[pltpu.VMEM((OBLK, NTR, LEV, BLK), f32), dma(()), dma(())],
        compiler_params=pltpu.CompilerParams(vmem_limit_bytes=16 * 1024 * 1024),
    )(*between)


def solution(mesh):
    return jax.shard_map(
        body,
        mesh=mesh,
        in_specs=(
            P(None, "patch"),
            P("patch", None, None),
            P("patch", None, None),
            P("patch", None),
            P("patch", None, None, None, None),
            P(),
            P(None, None, "patch"),
            P("patch"),
            P("patch", None, None),
            P("patch", None, None, None),
            P("patch", None, None, None),
            P("patch", None),
        ),
        out_specs=(P(None, "patch"), P(None, None, "patch")),
        check_vma=False,
    )
```

```python
import functools

import jax
import jax.numpy as jnp
from jax import lax
from jax.experimental import pallas as pl
from jax.experimental.pallas import tpu as pltpu
from jax.sharding import PartitionSpec as P

F = 8
LEV = 128
NTR = 2
BLK = 128
ABLK = 24
OBLK = 32
CAP = 8
SPAN = 5
HSPAN = 4
OC = 4096
PER = 8
FLUX_OFFSETS = (-2, -1, 0, 1, 2)
HALO_OFFSETS = (-2, -1, 1, 2)
SEND_ORDERS = ((3, 0, 2, 1), (0, 1, 3, 2), (3, 0, 2, 1), (3, 2, 0, 1))
WAIT_ORDERS = (((3, 2, 1, 0), (3, 2, 0, 1)), ((0, 1, 3, 2), (0, 1, 2, 3)))
LINE = 4
MESH = pl.DeviceIdType.MESH
f32 = jnp.float32
bf16 = jnp.bfloat16


def split2(v):
    hi = v.astype(bf16)
    lo = (v - hi.astype(f32)).astype(bf16)
    return hi, lo


def couple(
    size,
    send_h, tgt_h, cnt_h, coup_h, rows_h, atm_h, hs_h, hg_h, wet_h, tracer_h, mix_h, w_h,
    x, line, last_v, last_low, last_high, quarter_o,
    send_s, tgt_s, cnt_s, coup_s, rows_s, atm_v, hs_v, hg_v, wet_v,
    m, w, blocks, outg, relay, arr, contrib, ofs, surf, scale, sent, low_t, high_t, hout, v,
    small, xsem, msem, wsem, fs, fr, rs, rr, hsend, hrecv,
):
    me = lax.axis_index("patch")

    def at(offset):
        return lax.rem(me + (offset + size), size)

    plane = size // LINE
    near = 2 * LINE - 1
    spot = lax.rem(me, plane)
    level = me // plane
    opening = (LINE - level) // LINE
    mine = me - spot + near
    theirs = at(-plane) - spot + opening + near * (1 - opening)
    at_relay = spot == near
    at_stage = me == size - plane + 1
    last_pair = me - spot + plane - 2
    next_pair = lax.rem(me - spot + plane, size)

    barrier = pltpu.get_barrier_semaphore()

    def hello(device):
        pl.semaphore_signal(barrier, inc=1, device_id=(device,), device_id_type=MESH)

    for offset in HALO_OFFSETS:
        if offset < 0:
            hello(at(offset))
        else:
            pl.when(spot + offset < plane)(functools.partial(hello, at(offset)))
    pl.when(spot >= plane - 2)(functools.partial(hello, mine))
    pl.when(spot < 2)(functools.partial(hello, theirs))
    pl.when(me == size - plane + near)(functools.partial(hello, size - plane + 1))

    @pl.when(at_stage | (at_relay & (level < LINE - 1)))
    def _():
        for c in range(2):
            hello(next_pair + c)

    chip = lax.rem(me // 2, LINE)
    top = (chip + 1) // LINE
    foot = (LINE - chip) // LINE
    upper = chip // (LINE // 2)
    core = lax.rem(me, 2)

    def choose(i):
        high, low = WAIT_ORDERS
        above = high[0][i] * (1 - core) + high[1][i] * core
        below = low[0][i] * (1 - core) + low[1][i] * core
        return above * upper + below * (1 - upper)

    order = [choose(i) for i in range(HSPAN)]
    second = (1 - foot) * (1 - upper)
    third = (1 - top) * upper
    places = (foot, second, third, top)
    sends = [sum(SEND_ORDERS[y][i] * places[y] for y in range(LINE)) for i in range(HSPAN)]

    pairs = (
        (send_h, send_s), (atm_h, atm_v), (wet_h, wet_v), (hs_h, hs_v), (hg_h, hg_v),
        (tgt_h, tgt_s), (cnt_h, cnt_s), (coup_h, coup_s), (rows_h, rows_s),
    )
    smalls = [pltpu.make_async_copy(src, dst, small.at[i]) for i, (src, dst) in enumerate(pairs)]
    for copy in smalls:
        copy.start()

    def xcopy(b, t):
        cols = pl.ds(pl.multiple_of(b * BLK, BLK), BLK)
        return pltpu.make_async_copy(tracer_h.at[t, :, cols], x.at[b, t], xsem.at[b // PER])

    def mcopy(i):
        rows = pl.ds(i * PER, PER)
        return pltpu.make_async_copy(mix_h.at[rows], m.at[rows], msem.at[i])

    wcopy = pltpu.make_async_copy(w_h, w, wsem)

    def fetch(i):
        mcopy(i).start()
        for b in range(i * PER, (i + 1) * PER):
            for t in range(NTR):
                xcopy(b, t).start()

    for copy in smalls[:3]:
        copy.wait()
    fetch(0)
    fetch(1)
    slots = SPAN * CAP
    row40 = lax.broadcasted_iota(jnp.int32, (slots, BLK), 0)
    lane40 = lax.broadcasted_iota(jnp.int32, (slots, BLK), 1)
    want = jnp.full((slots, BLK), -1, jnp.int32)
    for d in range(SPAN):
        for c in range(CAP):
            want = jnp.where(row40 == d * CAP + c, send_s[d, 0, c], want)
    chooser = jnp.where(want == lane40, 1.0, 0.0).astype(bf16)[:, :32]
    for a in range(ABLK):
        blocks[a * F : (a + 1) * F, :] = atm_v[:, a * BLK : (a + 1) * BLK].astype(f32)
    blocks[ABLK * F :, :] = jnp.zeros(((32 - ABLK) * F, BLK), f32)
    for k in range(F // 2):
        pair = jnp.concatenate(
            [blocks[pl.ds(2 * k, 32, stride=F), :], blocks[pl.ds(2 * k + 1, 32, stride=F), :]],
            axis=1,
        )
        chosen = jnp.dot(chooser, pair.astype(bf16), preferred_element_type=f32)
        for q in range(2):
            contrib[pl.ds(2 * k + q, slots, stride=F), :] = chosen[:, q * BLK : (q + 1) * BLK]
    for d in range(SPAN):
        rows = contrib[d * CAP * F : (d + 1) * CAP * F, :].astype(bf16)
        if FLUX_OFFSETS[d] == 0:
            arr[d] = rows
        else:
            outg[d] = rows

    for i in range(2, OBLK // PER):
        fetch(i)
    wcopy.start()

    def solve(i):
        mcopy(i).wait()
        chunk = x.at[pl.ds(i * PER, PER)]
        pltpu.make_async_copy(chunk, chunk, xsem.at[i]).wait()
        for b in range(i * PER, (i + 1) * PER):
            a1, a2 = split2(m[b])
            t = jnp.concatenate([x[b, 0], x[b, 1]], axis=1)
            b1, b2 = split2(t)
            lhs = jnp.concatenate(
                [jnp.concatenate([a1, a1], axis=1), jnp.concatenate([a2, a2], axis=1)], axis=0
            )
            rhs = jnp.concatenate([b1, b2], axis=0)
            both = jnp.dot(lhs, rhs, preferred_element_type=f32)
            solved = both[:LEV] + both[LEV:]
            row = wet_v[b : b + 1, :]
            wet = jnp.concatenate([row, row], axis=1) > 0
            base = jnp.where(wet, solved, t)
            x[b, 0] = base[:, :BLK]
            x[b, 1] = base[:, BLK:]

    greeted = len(HALO_OFFSETS)
    closing = level == LINE - 1
    for who, amount in (
        (at_relay & jnp.logical_not(closing), 2 * greeted),
        (at_relay & closing, greeted + 2),
        (at_stage, greeted + 3),
        (spot == 0, greeted - 1),
        ((spot != 0) & jnp.logical_not(at_relay) & jnp.logical_not(at_stage), greeted),
    ):
        pl.when(who)(functools.partial(pl.semaphore_wait, barrier, amount))

    def flux_copy(d):
        return pltpu.make_async_remote_copy(
            src_ref=outg.at[d], dst_ref=arr.at[d], send_sem=fs.at[d], recv_sem=fr.at[d],
            device_id=(at(FLUX_OFFSETS[d]),), device_id_type=MESH,
        )

    def to_relay(d, c):
        slot = d + 2 * c
        return pltpu.make_async_remote_copy(
            src_ref=outg.at[d], dst_ref=relay.at[slot], send_sem=fs.at[d], recv_sem=rr.at[slot],
            device_id=(theirs,), device_id_type=MESH,
        )

    def from_relay(slot):
        d, c = ((0, 0), (1, 1), (0, 1))[slot]
        return pltpu.make_async_remote_copy(
            src_ref=relay.at[slot], dst_ref=arr.at[d], send_sem=rs.at[slot], recv_sem=fr.at[d],
            device_id=(last_pair + c,), device_id_type=MESH,
        )

    def from_stage(slot):
        return pltpu.make_async_remote_copy(
            src_ref=relay.at[slot], dst_ref=relay.at[slot],
            send_sem=rs.at[slot], recv_sem=rr.at[slot],
            device_id=(mine,), device_id_type=MESH,
        )

    flux = []
    for d in range(SPAN):
        offset = FLUX_OFFSETS[d]
        if offset == 0:
            continue
        flux.append(flux_copy(d))
        if offset > 0:
            flux[-1].start()
        else:
            pl.when(spot + offset >= 0)(flux[-1].start)
            for c in range(-offset):
                pl.when(spot == c)(to_relay(d, c).start)

    @pl.when(at_relay)
    def _():
        for slot, (d, c) in enumerate(((0, 0), (1, 0), (0, 1))):
            to_relay(d, c).wait_recv()
            from_relay(slot).start()

    @pl.when(at_stage)
    def _():
        for slot, (d, c) in enumerate(((0, 0), (1, 0), (0, 1))):
            to_relay(d, c).wait_recv()
            from_stage(slot).start()

    for i in range(OBLK // PER):
        solve(i)
    for copy in smalls[3:]:
        copy.wait()

    lane128 = lax.broadcasted_iota(jnp.int32, (BLK, BLK), 1).astype(f32)
    block32 = lax.broadcasted_iota(jnp.int32, (OBLK, BLK), 0)
    count = jnp.zeros((OBLK, BLK), f32)
    for h in range(HSPAN):
        for r in range(2):
            ghost = hg_v[2 * h + r : 2 * h + r + 1, :]
            spread = jnp.broadcast_to(ghost & (BLK - 1), (BLK, BLK)).astype(f32)
            low = jnp.where(jnp.transpose(spread) == lane128, 1.0, 0.0).astype(bf16)
            high = jnp.where(r < rows_s[0, h], ghost >> 7, -1)
            low_t[h, r * BLK : (r + 1) * BLK, :] = low
            spread = jnp.broadcast_to(high, (BLK, BLK)).astype(f32)
            high_t[h, r * BLK : (r + 1) * BLK, :] = jnp.transpose(spread).astype(bf16)
            here = jnp.where(block32 == high, 1.0, 0.0).astype(bf16)
            count = count + jnp.dot(here, low, preferred_element_type=f32)
    quarter = 0.25 * wet_v[...].astype(f32)
    quarter_o[...] = quarter
    scale[...] = 1.0 - quarter * count

    lane = lax.broadcasted_iota(jnp.int32, (OBLK, BLK), 1)
    seat = lane & 63
    target = jnp.full((OBLK, BLK), -1, jnp.int32)
    used = jnp.zeros((OBLK, BLK), jnp.int32)
    for d in range(SPAN):
        used = jnp.where(seat // CAP == d, cnt_s[0, d], used)
        for c in range(CAP):
            target = jnp.where(seat == d * CAP + c, tgt_s[d, 0, c], target)
    here = (target == block32) & (lane % CAP < used)
    place = jnp.where(here, 1.0, 0.0).astype(bf16)
    contrib[320:512, :] = jnp.zeros((192, BLK), f32)

    wcopy.wait()
    slot = lax.broadcasted_iota(jnp.int32, (32, BLK), 0) // F
    for i in range(SPAN):
        d = i + top * (SPAN - 1 - 2 * i)
        if i != SPAN // 2:
            pltpu.make_async_remote_copy(
                src_ref=outg.at[d], dst_ref=arr.at[d], send_sem=fs.at[d], recv_sem=fr.at[d],
                device_id=(at(1),), device_id_type=MESH,
            ).wait_recv()
        for g in range(2):
            c = 4 * g
            pieces = arr[d, c * F : (c + 4) * F, :].astype(f32)
            even = jnp.where(slot % 2 == 0, pieces, 0.0)
            odd = jnp.where(slot % 2 == 1, pieces, 0.0)
            lhs = jnp.concatenate([even, odd], axis=1).astype(bf16)
            rhs = jnp.concatenate(
                [
                    jnp.concatenate([w[d, c], w[d, c + 2]], axis=1),
                    jnp.concatenate([w[d, c + 1], w[d, c + 3]], axis=1),
                ],
                axis=0,
            )
            both = jnp.dot(lhs, rhs, preferred_element_type=f32)
            rows = pl.ds(pl.multiple_of((d * CAP + c) * F, 4 * F), 4 * F)
            contrib[rows, :] = jnp.where(slot < 2, both[:, :BLK], both[:, BLK:])

    wetf = wet_v[...].astype(f32)
    acc = [jnp.zeros((OBLK, BLK), f32) for _ in range(NTR)]
    for k in range(F // 2):
        pair = jnp.concatenate(
            [contrib[pl.ds(2 * k, 64, stride=F), :], contrib[pl.ds(2 * k + 1, 64, stride=F), :]],
            axis=1,
        )
        halves = jnp.concatenate(split2(pair), axis=0)
        total = jnp.dot(place, halves, preferred_element_type=f32)
        for q in range(2):
            f = 2 * k + q
            flux_f = total[:, q * BLK : (q + 1) * BLK] * wetf
            ofs[pl.ds(f, OBLK, stride=F), :] = flux_f
            for t in range(NTR):
                acc[t] = acc[t] + coup_s[t, f] * flux_f
    for t in range(NTR):
        surf[t] = acc[t]

    sub = lax.broadcasted_iota(jnp.int32, (BLK, 2 * BLK), 0)

    def halo_copy(h, t):
        offset = h - 2 + h // 2
        return pltpu.make_async_remote_copy(
            src_ref=hout.at[h, t], dst_ref=v.at[h, t],
            send_sem=hsend.at[h, t], recv_sem=hrecv.at[h, t],
            device_id=(at(offset),), device_id_type=MESH,
        )

    for n, h in enumerate(sends):
        row = jnp.concatenate([hs_v[pl.ds(2 * h, 1), :], hs_v[pl.ds(2 * h + 1, 1), :]], axis=1)
        low = jnp.where(sub == (row & (BLK - 1)), 1.0, 0.0).astype(bf16)
        high = jnp.broadcast_to((row >> 7).astype(f32), (BLK, 2 * BLK)).astype(bf16)
        for part in ((0,), (1,)) if n == 0 else ((0, 1),):
            rows = slice(part[0] * LEV, (part[-1] + 1) * LEV)
            picked = jnp.zeros((len(part) * LEV, 2 * BLK), f32)
            for k in range(OBLK // 2):
                tables, tiles = [], []
                for b in (2 * k, 2 * k + 1):
                    tables.append(jnp.where(high == jnp.array(b, bf16), low, jnp.zeros_like(low)))
                    if n < 3:
                        first = jnp.broadcast_to(m[b, :, 0:1], (LEV, BLK))
                    if n == 0:
                        for t in part:
                            mixed = x[b, t] + first * surf[t, b : b + 1, :]
                            tiles.append(mixed.astype(bf16))
                    elif n < 3:
                        t = n - 1
                        mixed = x[b, t] + first * surf[t, b : b + 1, :]
                        x[b, t] = mixed * scale[b : b + 1, :]
                if n == 0:
                    tile = jnp.concatenate(tiles, axis=1)
                    sent[k, rows] = tile
                else:
                    tile = sent[k, rows]
                found = jnp.dot(
                    tile, jnp.concatenate(tables, axis=0), preferred_element_type=f32
                )
                picked = jnp.where((row >> 8) == k, found, picked)
            for j, t in enumerate(part):
                hout[h, t] = picked[j * LEV : (j + 1) * LEV].astype(bf16)
                halo_copy(h, t).start()

    for b in range(OBLK):
        line[:, b * BLK : (b + 1) * BLK] = ofs[b * F : (b + 1) * F, :]
    last = order[-1]
    last_low[...] = low_t[last]
    last_high[...] = high_t[last]

    for h in order[:-1]:
        for t in range(NTR):
            halo_copy(h, t).wait_recv()
        values = jnp.concatenate([v[h, 0], v[h, 1]], axis=0)
        add_values(x, values, low_t[h], high_t[h], quarter_o)
    for t in range(NTR):
        halo_copy(last, t).wait_recv()
        last_v[t * LEV : (t + 1) * LEV] = v[last, t]
    for copy in flux:
        copy.wait_send()

    @pl.when(at_relay)
    def _():
        for slot in range(3):
            from_relay(slot).wait_send()

    @pl.when(at_stage)
    def _():
        for slot in range(3):
            from_stage(slot).wait_send()

    for h in order:
        for t in range(NTR):
            halo_copy(h, t).wait_send()


def add_values(x, values, low, high, quarter_v, out=None, ready=None):
    out = x if out is None else out
    for k in range(OBLK // 2):
        tables = []
        for b in (2 * k, 2 * k + 1):
            here = high == jnp.array(b, bf16)
            tables.append(jnp.where(here, low, jnp.zeros_like(low)))
        total = jnp.dot(values, jnp.concatenate(tables, axis=1), preferred_element_type=f32)
        for j, b in enumerate((2 * k, 2 * k + 1)):
            weight = quarter_v[b : b + 1, :]
            for t in range(NTR):
                piece = total[t * LEV : (t + 1) * LEV, j * BLK : (j + 1) * BLK]
                out[b, t] = x[b, t] + weight * piece
                if ready is not None:
                    ready(b, t)


def scatter(x, line, values_v, low_v, high_v, quarter_v, flux_o, out_o, stage, sem, fsem):
    fcopy = pltpu.make_async_copy(line, flux_o, fsem)
    fcopy.start()

    def ready(b, t):
        cols = slice(b * BLK, (b + 1) * BLK)
        pltpu.make_async_copy(stage.at[b, t], out_o.at[t, :, cols], sem).start()

    add_values(x, values_v[...], low_v[...], high_v[...], quarter_v, stage, ready)
    pltpu.make_async_copy(out_o, out_o, sem).wait()
    fcopy.wait()


def body(
    atm_flux, remap_send, remap_target, remap_counts, remap_weights, coupling,
    tracer, wet, mix_inverse, halo_send, halo_ghost, halo_rows,
):
    size = lax.axis_size("patch")
    far = lambda a: pltpu.with_memory_space_constraint(a, pltpu.HBM)
    vmem = pl.BlockSpec(memory_space=pltpu.VMEM)
    hbm = pl.BlockSpec(memory_space=pltpu.HBM)
    dma = pltpu.SemaphoreType.DMA
    i32 = jnp.int32
    picks = 2 * BLK
    between = pl.pallas_call(
        functools.partial(couple, size),
        name="couple",
        out_shape=(
            jax.ShapeDtypeStruct((OBLK, NTR, LEV, BLK), f32),
            jax.ShapeDtypeStruct((F, OC), f32),
            jax.ShapeDtypeStruct((NTR * LEV, picks), bf16),
            jax.ShapeDtypeStruct((picks, BLK), bf16),
            jax.ShapeDtypeStruct((picks, BLK), bf16),
            jax.ShapeDtypeStruct((OBLK, BLK), f32),
        ),
        in_specs=[hbm] * 12,
        out_specs=(vmem,) * 6,
        scratch_shapes=[
            pltpu.SMEM((SPAN, 1, CAP), i32),
            pltpu.SMEM((SPAN, 1, CAP), i32),
            pltpu.SMEM((1, SPAN), i32),
            pltpu.SMEM((NTR, F), f32),
            pltpu.SMEM((1, HSPAN), i32),
            pltpu.VMEM((F, ABLK * BLK), bf16),
            pltpu.VMEM((2 * HSPAN, BLK), i32),
            pltpu.VMEM((2 * HSPAN, BLK), i32),
            pltpu.VMEM((OBLK, BLK), i32),
            pltpu.VMEM((OBLK, LEV, LEV), f32),
            pltpu.VMEM((SPAN, CAP, BLK, BLK), bf16),
            pltpu.VMEM((32 * F, BLK), f32),
            pltpu.VMEM((SPAN, CAP * F, BLK), bf16),
            pltpu.VMEM((3, CAP * F, BLK), bf16),
            pltpu.VMEM((SPAN, CAP * F, BLK), bf16),
            pltpu.VMEM((64 * F, BLK), f32),
            pltpu.VMEM((OBLK * F, BLK), f32),
            pltpu.VMEM((NTR, OBLK, BLK), f32),
            pltpu.VMEM((OBLK, BLK), f32),
            pltpu.VMEM((OBLK // 2, NTR * LEV, 2 * BLK), bf16),
            pltpu.VMEM((HSPAN, picks, BLK), bf16),
            pltpu.VMEM((HSPAN, picks, BLK), bf16),
            pltpu.VMEM((HSPAN, NTR, LEV, picks), bf16),
            pltpu.VMEM((HSPAN, NTR, LEV, picks), bf16),
            dma((9,)), dma((OBLK // PER,)), dma((OBLK // PER,)), dma(()),
            dma((SPAN,)), dma((SPAN,)), dma((3,)), dma((3,)), dma((HSPAN, NTR)), dma((HSPAN, NTR)),
        ],
        compiler_params=pltpu.CompilerParams(
            collective_id=0, has_side_effects=True, vmem_limit_bytes=24 * 1024 * 1024
        ),
    )(
        far(jnp.transpose(remap_send, (1, 0, 2))), far(jnp.transpose(remap_target, (1, 0, 2))),
        far(remap_counts), far(coupling), far(halo_rows), far(atm_flux),
        far(halo_send.reshape(2 * HSPAN, BLK)), far(halo_ghost.reshape(2 * HSPAN, BLK)),
        far(wet.reshape(OBLK, BLK)), far(tracer), far(mix_inverse),
        far(remap_weights.reshape(SPAN, CAP, BLK, BLK)),
    )
    return pl.pallas_call(
        scatter,
        name="scatter",
        out_shape=(
            jax.ShapeDtypeStruct((F, OC), f32),
            jax.ShapeDtypeStruct((NTR, LEV, OC), f32),
        ),
        in_specs=[vmem] * 6,
        out_specs=(hbm, hbm),
        scratch_shapes=[pltpu.VMEM((OBLK, NTR, LEV, BLK), f32), dma(()), dma(())],
        compiler_params=pltpu.CompilerParams(vmem_limit_bytes=16 * 1024 * 1024),
    )(*between)


def solution(mesh):
    return jax.shard_map(
        body,
        mesh=mesh,
        in_specs=(
            P(None, "patch"),
            P("patch", None, None),
            P("patch", None, None),
            P("patch", None),
            P("patch", None, None, None, None),
            P(),
            P(None, None, "patch"),
            P("patch"),
            P("patch", None, None),
            P("patch", None, None, None),
            P("patch", None, None, None),
            P("patch", None),
        ),
        out_specs=(P(None, "patch"), P(None, None, "patch")),
        check_vma=False,
    )
```

```python
import functools

import jax
import jax.numpy as jnp
from jax import lax
from jax.experimental import pallas as pl
from jax.experimental.pallas import tpu as pltpu
from jax.sharding import PartitionSpec as P

F = 8
LEV = 128
NTR = 2
BLK = 128
ABLK = 24
OBLK = 32
CAP = 8
SPAN = 5
HSPAN = 4
OC = 4096
PER = 8
FLUX_OFFSETS = (-2, -1, 0, 1, 2)
HALO_OFFSETS = (-2, -1, 1, 2)
SEND_ORDERS = ((3, 0, 2, 1), (0, 1, 3, 2), (3, 0, 2, 1), (3, 2, 0, 1))
WAIT_ORDERS = (((3, 2, 1, 0), (3, 2, 0, 1)), ((0, 1, 3, 2), (0, 1, 2, 3)))
LINE = 4
MESH = pl.DeviceIdType.MESH
f32 = jnp.float32
bf16 = jnp.bfloat16


def split2(v):
    hi = v.astype(bf16)
    lo = (v - hi.astype(f32)).astype(bf16)
    return hi, lo


def couple(
    size,
    send_h, tgt_h, cnt_h, coup_h, rows_h, atm_h, hs_h, hg_h, wet_h, tracer_h, mix_h, w_h,
    x, line, last_v, last_low, last_high, quarter_o,
    send_s, tgt_s, cnt_s, coup_s, rows_s, atm_v, hs_v, hg_v, wet_v,
    m, w, blocks, outg, relay, arr, contrib, ofs, surf, scale, sent, low_t, high_t, hout, v,
    small, xsem, msem, wsem, fs, fr, rs, rr, hsend, hrecv,
):
    me = lax.axis_index("patch")

    def at(offset):
        return lax.rem(me + (offset + size), size)

    plane = size // LINE
    near = 2 * LINE - 1
    spot = lax.rem(me, plane)
    level = me // plane
    opening = (LINE - level) // LINE
    mine = me - spot + near
    theirs = at(-plane) - spot + opening + near * (1 - opening)
    at_relay = spot == near
    at_stage = me == size - plane + 1
    last_pair = me - spot + plane - 2
    next_pair = lax.rem(me - spot + plane, size)

    barrier = pltpu.get_barrier_semaphore()

    def hello(device):
        pl.semaphore_signal(barrier, inc=1, device_id=(device,), device_id_type=MESH)

    for offset in HALO_OFFSETS:
        if offset < 0:
            hello(at(offset))
        else:
            pl.when(spot + offset < plane)(functools.partial(hello, at(offset)))
    pl.when(spot >= plane - 2)(functools.partial(hello, mine))
    pl.when(spot < 2)(functools.partial(hello, theirs))
    pl.when(me == size - plane + near)(functools.partial(hello, size - plane + 1))

    @pl.when(at_stage | (at_relay & (level < LINE - 1)))
    def _():
        for c in range(2):
            hello(next_pair + c)

    chip = lax.rem(me // 2, LINE)
    top = (chip + 1) // LINE
    foot = (LINE - chip) // LINE
    upper = chip // (LINE // 2)
    core = lax.rem(me, 2)

    def choose(i):
        high, low = WAIT_ORDERS
        above = high[0][i] * (1 - core) + high[1][i] * core
        below = low[0][i] * (1 - core) + low[1][i] * core
        return above * upper + below * (1 - upper)

    order = [choose(i) for i in range(HSPAN)]
    second = (1 - foot) * (1 - upper)
    third = (1 - top) * upper
    places = (foot, second, third, top)
    sends = [sum(SEND_ORDERS[y][i] * places[y] for y in range(LINE)) for i in range(HSPAN)]

    pairs = (
        (send_h, send_s), (atm_h, atm_v), (wet_h, wet_v), (hs_h, hs_v), (hg_h, hg_v),
        (tgt_h, tgt_s), (cnt_h, cnt_s), (coup_h, coup_s), (rows_h, rows_s),
    )
    smalls = [pltpu.make_async_copy(src, dst, small.at[i]) for i, (src, dst) in enumerate(pairs)]
    for copy in smalls:
        copy.start()

    def xcopy(b, t):
        cols = pl.ds(pl.multiple_of(b * BLK, BLK), BLK)
        return pltpu.make_async_copy(tracer_h.at[t, :, cols], x.at[b, t], xsem.at[b // PER])

    def mcopy(i):
        rows = pl.ds(i * PER, PER)
        return pltpu.make_async_copy(mix_h.at[rows], m.at[rows], msem.at[i])

    wcopy = pltpu.make_async_copy(w_h, w, wsem)

    def fetch(i):
        mcopy(i).start()
        for b in range(i * PER, (i + 1) * PER):
            for t in range(NTR):
                xcopy(b, t).start()

    for copy in smalls[:3]:
        copy.wait()
    fetch(0)
    fetch(1)
    slots = SPAN * CAP
    row40 = lax.broadcasted_iota(jnp.int32, (slots, BLK), 0)
    lane40 = lax.broadcasted_iota(jnp.int32, (slots, BLK), 1)
    want = jnp.full((slots, BLK), -1, jnp.int32)
    for d in range(SPAN):
        for c in range(CAP):
            want = jnp.where(row40 == d * CAP + c, send_s[d, 0, c], want)
    chooser = jnp.where(want == lane40, 1.0, 0.0).astype(bf16)[:, :32]
    for a in range(ABLK):
        blocks[a * F : (a + 1) * F, :] = atm_v[:, a * BLK : (a + 1) * BLK].astype(f32)
    blocks[ABLK * F :, :] = jnp.zeros(((32 - ABLK) * F, BLK), f32)
    for k in range(F // 2):
        pair = jnp.concatenate(
            [blocks[pl.ds(2 * k, 32, stride=F), :], blocks[pl.ds(2 * k + 1, 32, stride=F), :]],
            axis=1,
        )
        chosen = jnp.dot(chooser, pair.astype(bf16), preferred_element_type=f32)
        for q in range(2):
            contrib[pl.ds(2 * k + q, slots, stride=F), :] = chosen[:, q * BLK : (q + 1) * BLK]
    for d in range(SPAN):
        rows = contrib[d * CAP * F : (d + 1) * CAP * F, :].astype(bf16)
        if FLUX_OFFSETS[d] == 0:
            arr[d] = rows
        else:
            outg[d] = rows

    for i in range(2, OBLK // PER):
        fetch(i)
    wcopy.start()

    def solve(i):
        mcopy(i).wait()
        chunk = x.at[pl.ds(i * PER, PER)]
        pltpu.make_async_copy(chunk, chunk, xsem.at[i]).wait()
        for b in range(i * PER, (i + 1) * PER):
            a1, a2 = split2(m[b])
            t = jnp.concatenate([x[b, 0], x[b, 1]], axis=1)
            b1, b2 = split2(t)
            lhs = jnp.concatenate(
                [jnp.concatenate([a1, a1], axis=1), jnp.concatenate([a2, a2], axis=1)], axis=0
            )
            rhs = jnp.concatenate([b1, b2], axis=0)
            both = jnp.dot(lhs, rhs, preferred_element_type=f32)
            solved = both[:LEV] + both[LEV:]
            row = wet_v[b : b + 1, :]
            wet = jnp.concatenate([row, row], axis=1) > 0
            base = jnp.where(wet, solved, t)
            x[b, 0] = base[:, :BLK]
            x[b, 1] = base[:, BLK:]

    greeted = len(HALO_OFFSETS)
    closing = level == LINE - 1
    for who, amount in (
        (at_relay & jnp.logical_not(closing), 2 * greeted),
        (at_relay & closing, greeted + 2),
        (at_stage, greeted + 3),
        (spot == 0, greeted - 1),
        ((spot != 0) & jnp.logical_not(at_relay) & jnp.logical_not(at_stage), greeted),
    ):
        pl.when(who)(functools.partial(pl.semaphore_wait, barrier, amount))

    def flux_copy(d):
        return pltpu.make_async_remote_copy(
            src_ref=outg.at[d], dst_ref=arr.at[d], send_sem=fs.at[d], recv_sem=fr.at[d],
            device_id=(at(FLUX_OFFSETS[d]),), device_id_type=MESH,
        )

    def to_relay(d, c):
        slot = d + 2 * c
        return pltpu.make_async_remote_copy(
            src_ref=outg.at[d], dst_ref=relay.at[slot], send_sem=fs.at[d], recv_sem=rr.at[slot],
            device_id=(theirs,), device_id_type=MESH,
        )

    def from_relay(slot):
        d, c = ((0, 0), (1, 1), (0, 1))[slot]
        return pltpu.make_async_remote_copy(
            src_ref=relay.at[slot], dst_ref=arr.at[d], send_sem=rs.at[slot], recv_sem=fr.at[d],
            device_id=(last_pair + c,), device_id_type=MESH,
        )

    def from_stage(slot):
        return pltpu.make_async_remote_copy(
            src_ref=relay.at[slot], dst_ref=relay.at[slot],
            send_sem=rs.at[slot], recv_sem=rr.at[slot],
            device_id=(mine,), device_id_type=MESH,
        )

    flux = []
    for d in range(SPAN):
        offset = FLUX_OFFSETS[d]
        if offset == 0:
            continue
        flux.append(flux_copy(d))
        if offset > 0:
            flux[-1].start()
        else:
            pl.when(spot + offset >= 0)(flux[-1].start)
            for c in range(-offset):
                pl.when(spot == c)(to_relay(d, c).start)

    @pl.when(at_relay)
    def _():
        for slot, (d, c) in enumerate(((0, 0), (1, 0), (0, 1))):
            to_relay(d, c).wait_recv()
            from_relay(slot).start()

    @pl.when(at_stage)
    def _():
        for slot, (d, c) in enumerate(((0, 0), (1, 0), (0, 1))):
            to_relay(d, c).wait_recv()
            from_stage(slot).start()

    for i in range(OBLK // PER):
        solve(i)
    for copy in smalls[3:]:
        copy.wait()

    lane128 = lax.broadcasted_iota(jnp.int32, (BLK, BLK), 1).astype(f32)
    block32 = lax.broadcasted_iota(jnp.int32, (OBLK, BLK), 0)
    count = jnp.zeros((OBLK, BLK), f32)
    for h in range(HSPAN):
        for r in range(2):
            ghost = hg_v[2 * h + r : 2 * h + r + 1, :]
            spread = jnp.broadcast_to(ghost & (BLK - 1), (BLK, BLK)).astype(f32)
            low = jnp.where(jnp.transpose(spread) == lane128, 1.0, 0.0).astype(bf16)
            high = jnp.where(r < rows_s[0, h], ghost >> 7, -1)
            low_t[h, r * BLK : (r + 1) * BLK, :] = low
            spread = jnp.broadcast_to(high, (BLK, BLK)).astype(f32)
            high_t[h, r * BLK : (r + 1) * BLK, :] = jnp.transpose(spread).astype(bf16)
            here = jnp.where(block32 == high, 1.0, 0.0).astype(bf16)
            count = count + jnp.dot(here, low, preferred_element_type=f32)
    quarter = 0.25 * wet_v[...].astype(f32)
    quarter_o[...] = quarter
    scale[...] = 1.0 - quarter * count

    lane = lax.broadcasted_iota(jnp.int32, (OBLK, BLK), 1)
    seat = lane & 63
    target = jnp.full((OBLK, BLK), -1, jnp.int32)
    used = jnp.zeros((OBLK, BLK), jnp.int32)
    for d in range(SPAN):
        used = jnp.where(seat // CAP == d, cnt_s[0, d], used)
        for c in range(CAP):
            target = jnp.where(seat == d * CAP + c, tgt_s[d, 0, c], target)
    here = (target == block32) & (lane % CAP < used)
    place = jnp.where(here, 1.0, 0.0).astype(bf16)
    contrib[320:512, :] = jnp.zeros((192, BLK), f32)

    wcopy.wait()
    slot = lax.broadcasted_iota(jnp.int32, (32, BLK), 0) // F
    for i in range(SPAN):
        d = i + top * (SPAN - 1 - 2 * i)
        if i != SPAN // 2:
            pltpu.make_async_remote_copy(
                src_ref=outg.at[d], dst_ref=arr.at[d], send_sem=fs.at[d], recv_sem=fr.at[d],
                device_id=(at(1),), device_id_type=MESH,
            ).wait_recv()
        for g in range(2):
            c = 4 * g
            pieces = arr[d, c * F : (c + 4) * F, :].astype(f32)
            even = jnp.where(slot % 2 == 0, pieces, 0.0)
            odd = jnp.where(slot % 2 == 1, pieces, 0.0)
            lhs = jnp.concatenate([even, odd], axis=1).astype(bf16)
            rhs = jnp.concatenate(
                [
                    jnp.concatenate([w[d, c], w[d, c + 2]], axis=1),
                    jnp.concatenate([w[d, c + 1], w[d, c + 3]], axis=1),
                ],
                axis=0,
            )
            both = jnp.dot(lhs, rhs, preferred_element_type=f32)
            rows = pl.ds(pl.multiple_of((d * CAP + c) * F, 4 * F), 4 * F)
            contrib[rows, :] = jnp.where(slot < 2, both[:, :BLK], both[:, BLK:])

    wetf = wet_v[...].astype(f32)
    acc = [jnp.zeros((OBLK, BLK), f32) for _ in range(NTR)]
    for k in range(F // 2):
        pair = jnp.concatenate(
            [contrib[pl.ds(2 * k, 64, stride=F), :], contrib[pl.ds(2 * k + 1, 64, stride=F), :]],
            axis=1,
        )
        halves = jnp.concatenate(split2(pair), axis=0)
        total = jnp.dot(place, halves, preferred_element_type=f32)
        for q in range(2):
            f = 2 * k + q
            flux_f = total[:, q * BLK : (q + 1) * BLK] * wetf
            ofs[pl.ds(f, OBLK, stride=F), :] = flux_f
            for t in range(NTR):
                acc[t] = acc[t] + coup_s[t, f] * flux_f
    for t in range(NTR):
        surf[t] = acc[t]

    sub = lax.broadcasted_iota(jnp.int32, (BLK, 2 * BLK), 0)

    def halo_copy(h, t=None):
        offset = h - 2 + h // 2
        return pltpu.make_async_remote_copy(
            src_ref=hout.at[h] if t is None else hout.at[h, t],
            dst_ref=v.at[h] if t is None else v.at[h, t],
            send_sem=hsend.at[h], recv_sem=hrecv.at[h],
            device_id=(at(offset),), device_id_type=MESH,
        )

    for n, h in enumerate(sends):
        row = jnp.concatenate([hs_v[pl.ds(2 * h, 1), :], hs_v[pl.ds(2 * h + 1, 1), :]], axis=1)
        low = jnp.where(sub == (row & (BLK - 1)), 1.0, 0.0).astype(bf16)
        high = jnp.broadcast_to((row >> 7).astype(f32), (BLK, 2 * BLK)).astype(bf16)
        for part in ((0,), (1,)) if n == 0 else ((0, 1),):
            rows = slice(part[0] * LEV, (part[-1] + 1) * LEV)
            picked = jnp.zeros((len(part) * LEV, 2 * BLK), f32)
            for k in range(OBLK // 2):
                tables, tiles = [], []
                for b in (2 * k, 2 * k + 1):
                    tables.append(jnp.where(high == jnp.array(b, bf16), low, jnp.zeros_like(low)))
                    if n < 3:
                        first = jnp.broadcast_to(m[b, :, 0:1], (LEV, BLK))
                    if n == 0:
                        for t in part:
                            mixed = x[b, t] + first * surf[t, b : b + 1, :]
                            tiles.append(mixed.astype(bf16))
                    elif n < 3:
                        t = n - 1
                        mixed = x[b, t] + first * surf[t, b : b + 1, :]
                        x[b, t] = mixed * scale[b : b + 1, :]
                if n == 0:
                    tile = jnp.concatenate(tiles, axis=1)
                    sent[k, rows] = tile
                else:
                    tile = sent[k, rows]
                found = jnp.dot(
                    tile, jnp.concatenate(tables, axis=0), preferred_element_type=f32
                )
                picked = jnp.where((row >> 8) == k, found, picked)
            for j, t in enumerate(part):
                hout[h, t] = picked[j * LEV : (j + 1) * LEV].astype(bf16)
            halo_copy(h, part[0] if n == 0 else None).start()

    for b in range(OBLK):
        line[:, b * BLK : (b + 1) * BLK] = ofs[b * F : (b + 1) * F, :]
    last = order[-1]
    last_low[...] = low_t[last]
    last_high[...] = high_t[last]

    for h in order[:-1]:
        halo_copy(h).wait_recv()
        values = jnp.concatenate([v[h, 0], v[h, 1]], axis=0)
        add_values(x, values, low_t[h], high_t[h], quarter_o)
    halo_copy(last).wait_recv()
    for t in range(NTR):
        last_v[t * LEV : (t + 1) * LEV] = v[last, t]
    for copy in flux:
        copy.wait_send()

    @pl.when(at_relay)
    def _():
        for slot in range(3):
            from_relay(slot).wait_send()

    @pl.when(at_stage)
    def _():
        for slot in range(3):
            from_stage(slot).wait_send()

    for h in order:
        halo_copy(h).wait_send()


def add_values(x, values, low, high, quarter_v, out=None, ready=None):
    out = x if out is None else out
    for k in range(OBLK // 2):
        tables = []
        for b in (2 * k, 2 * k + 1):
            here = high == jnp.array(b, bf16)
            tables.append(jnp.where(here, low, jnp.zeros_like(low)))
        total = jnp.dot(values, jnp.concatenate(tables, axis=1), preferred_element_type=f32)
        for j, b in enumerate((2 * k, 2 * k + 1)):
            weight = quarter_v[b : b + 1, :]
            for t in range(NTR):
                piece = total[t * LEV : (t + 1) * LEV, j * BLK : (j + 1) * BLK]
                out[b, t] = x[b, t] + weight * piece
                if ready is not None:
                    ready(b, t)


def scatter(x, line, values_v, low_v, high_v, quarter_v, flux_o, out_o, stage, sem, fsem):
    fcopy = pltpu.make_async_copy(line, flux_o, fsem)
    fcopy.start()

    def ready(b, t):
        cols = slice(b * BLK, (b + 1) * BLK)
        pltpu.make_async_copy(stage.at[b, t], out_o.at[t, :, cols], sem).start()

    add_values(x, values_v[...], low_v[...], high_v[...], quarter_v, stage, ready)
    pltpu.make_async_copy(out_o, out_o, sem).wait()
    fcopy.wait()


def body(
    atm_flux, remap_send, remap_target, remap_counts, remap_weights, coupling,
    tracer, wet, mix_inverse, halo_send, halo_ghost, halo_rows,
):
    size = lax.axis_size("patch")
    far = lambda a: pltpu.with_memory_space_constraint(a, pltpu.HBM)
    vmem = pl.BlockSpec(memory_space=pltpu.VMEM)
    hbm = pl.BlockSpec(memory_space=pltpu.HBM)
    dma = pltpu.SemaphoreType.DMA
    i32 = jnp.int32
    picks = 2 * BLK
    between = pl.pallas_call(
        functools.partial(couple, size),
        name="couple",
        out_shape=(
            jax.ShapeDtypeStruct((OBLK, NTR, LEV, BLK), f32),
            jax.ShapeDtypeStruct((F, OC), f32),
            jax.ShapeDtypeStruct((NTR * LEV, picks), bf16),
            jax.ShapeDtypeStruct((picks, BLK), bf16),
            jax.ShapeDtypeStruct((picks, BLK), bf16),
            jax.ShapeDtypeStruct((OBLK, BLK), f32),
        ),
        in_specs=[hbm] * 12,
        out_specs=(vmem,) * 6,
        scratch_shapes=[
            pltpu.SMEM((SPAN, 1, CAP), i32),
            pltpu.SMEM((SPAN, 1, CAP), i32),
            pltpu.SMEM((1, SPAN), i32),
            pltpu.SMEM((NTR, F), f32),
            pltpu.SMEM((1, HSPAN), i32),
            pltpu.VMEM((F, ABLK * BLK), bf16),
            pltpu.VMEM((2 * HSPAN, BLK), i32),
            pltpu.VMEM((2 * HSPAN, BLK), i32),
            pltpu.VMEM((OBLK, BLK), i32),
            pltpu.VMEM((OBLK, LEV, LEV), f32),
            pltpu.VMEM((SPAN, CAP, BLK, BLK), bf16),
            pltpu.VMEM((32 * F, BLK), f32),
            pltpu.VMEM((SPAN, CAP * F, BLK), bf16),
            pltpu.VMEM((3, CAP * F, BLK), bf16),
            pltpu.VMEM((SPAN, CAP * F, BLK), bf16),
            pltpu.VMEM((64 * F, BLK), f32),
            pltpu.VMEM((OBLK * F, BLK), f32),
            pltpu.VMEM((NTR, OBLK, BLK), f32),
            pltpu.VMEM((OBLK, BLK), f32),
            pltpu.VMEM((OBLK // 2, NTR * LEV, 2 * BLK), bf16),
            pltpu.VMEM((HSPAN, picks, BLK), bf16),
            pltpu.VMEM((HSPAN, picks, BLK), bf16),
            pltpu.VMEM((HSPAN, NTR, LEV, picks), bf16),
            pltpu.VMEM((HSPAN, NTR, LEV, picks), bf16),
            dma((9,)), dma((OBLK // PER,)), dma((OBLK // PER,)), dma(()),
            dma((SPAN,)), dma((SPAN,)), dma((3,)), dma((3,)), dma((HSPAN,)), dma((HSPAN,)),
        ],
        compiler_params=pltpu.CompilerParams(
            collective_id=0, has_side_effects=True, vmem_limit_bytes=24 * 1024 * 1024
        ),
    )(
        far(jnp.transpose(remap_send, (1, 0, 2))), far(jnp.transpose(remap_target, (1, 0, 2))),
        far(remap_counts), far(coupling), far(halo_rows), far(atm_flux),
        far(halo_send.reshape(2 * HSPAN, BLK)), far(halo_ghost.reshape(2 * HSPAN, BLK)),
        far(wet.reshape(OBLK, BLK)), far(tracer), far(mix_inverse),
        far(remap_weights.reshape(SPAN, CAP, BLK, BLK)),
    )
    return pl.pallas_call(
        scatter,
        name="scatter",
        out_shape=(
            jax.ShapeDtypeStruct((F, OC), f32),
            jax.ShapeDtypeStruct((NTR, LEV, OC), f32),
        ),
        in_specs=[vmem] * 6,
        out_specs=(hbm, hbm),
        scratch_shapes=[pltpu.VMEM((OBLK, NTR, LEV, BLK), f32), dma(()), dma(())],
        compiler_params=pltpu.CompilerParams(vmem_limit_bytes=16 * 1024 * 1024),
    )(*between)


def solution(mesh):
    return jax.shard_map(
        body,
        mesh=mesh,
        in_specs=(
            P(None, "patch"),
            P("patch", None, None),
            P("patch", None, None),
            P("patch", None),
            P("patch", None, None, None, None),
            P(),
            P(None, None, "patch"),
            P("patch"),
            P("patch", None, None),
            P("patch", None, None, None),
            P("patch", None, None, None),
            P("patch", None),
        ),
        out_specs=(P(None, "patch"), P(None, None, "patch")),
        check_vma=False,
    )
```

```python
import functools

import jax
import jax.numpy as jnp
from jax import lax
from jax.experimental import pallas as pl
from jax.experimental.pallas import tpu as pltpu
from jax.sharding import PartitionSpec as P

F = 8
LEV = 128
NTR = 2
BLK = 128
ABLK = 24
OBLK = 32
CAP = 8
SPAN = 5
HSPAN = 4
OC = 4096
PER = 8
FLUX_OFFSETS = (-2, -1, 0, 1, 2)
HALO_OFFSETS = (-2, -1, 1, 2)
SEND_ORDERS = ((3, 0, 2, 1), (0, 1, 3, 2), (3, 0, 2, 1), (3, 2, 0, 1))
WAIT_ORDERS = (((3, 2, 1, 0), (3, 2, 0, 1)), ((0, 1, 3, 2), (0, 1, 2, 3)))
LINE = 4
MESH = pl.DeviceIdType.MESH
f32 = jnp.float32
bf16 = jnp.bfloat16


def split2(v):
    hi = v.astype(bf16)
    lo = (v - hi.astype(f32)).astype(bf16)
    return hi, lo


def couple(
    size,
    send_h, tgt_h, cnt_h, coup_h, rows_h, atm_h, hs_h, hg_h, wet_h, tracer_h, mix_h, w_h,
    x, line, last_v, last_low, last_high, quarter_o,
    send_s, tgt_s, cnt_s, coup_s, rows_s, atm_v, hs_v, hg_v, wet_v,
    m, w, blocks, outg, relay, arr, contrib, ofs, surf, scale, sent, low_t, high_t, hout, v,
    small, xsem, msem, wsem, fs, fr, rs, rr, hsend, hrecv,
):
    me = lax.axis_index("patch")

    def at(offset):
        return lax.rem(me + (offset + size), size)

    plane = size // LINE
    near = 2 * LINE - 1
    spot = lax.rem(me, plane)
    level = me // plane
    opening = (LINE - level) // LINE
    mine = me - spot + near
    theirs = at(-plane) - spot + opening + near * (1 - opening)
    at_relay = spot == near
    at_stage = me == size - plane + 1
    last_pair = me - spot + plane - 2
    next_pair = lax.rem(me - spot + plane, size)

    barrier = pltpu.get_barrier_semaphore()

    def hello(device):
        pl.semaphore_signal(barrier, inc=1, device_id=(device,), device_id_type=MESH)

    for offset in HALO_OFFSETS:
        if offset < 0:
            hello(at(offset))
        else:
            pl.when(spot + offset < plane)(functools.partial(hello, at(offset)))
    pl.when(spot >= plane - 2)(functools.partial(hello, mine))
    pl.when(spot < 2)(functools.partial(hello, theirs))
    pl.when(me == size - plane + near)(functools.partial(hello, size - plane + 1))

    @pl.when(at_stage | (at_relay & (level < LINE - 1)))
    def _():
        for c in range(2):
            hello(next_pair + c)

    chip = lax.rem(me // 2, LINE)
    top = (chip + 1) // LINE
    foot = (LINE - chip) // LINE
    upper = chip // (LINE // 2)
    core = lax.rem(me, 2)

    def choose(i):
        high, low = WAIT_ORDERS
        above = high[0][i] * (1 - core) + high[1][i] * core
        below = low[0][i] * (1 - core) + low[1][i] * core
        return above * upper + below * (1 - upper)

    order = [choose(i) for i in range(HSPAN)]
    second = (1 - foot) * (1 - upper)
    third = (1 - top) * upper
    places = (foot, second, third, top)
    sends = [sum(SEND_ORDERS[y][i] * places[y] for y in range(LINE)) for i in range(HSPAN)]

    pairs = (
        (send_h, send_s), (atm_h, atm_v), (wet_h, wet_v), (hs_h, hs_v), (hg_h, hg_v),
        (tgt_h, tgt_s), (cnt_h, cnt_s), (coup_h, coup_s), (rows_h, rows_s),
    )
    smalls = [pltpu.make_async_copy(src, dst, small.at[i]) for i, (src, dst) in enumerate(pairs)]
    for copy in smalls:
        copy.start()

    def xcopy(b, t):
        cols = pl.ds(pl.multiple_of(b * BLK, BLK), BLK)
        return pltpu.make_async_copy(tracer_h.at[t, :, cols], x.at[b, t], xsem.at[b // PER])

    def mcopy(i):
        rows = pl.ds(i * PER, PER)
        return pltpu.make_async_copy(mix_h.at[rows], m.at[rows], msem.at[i])

    wcopy = pltpu.make_async_copy(w_h, w, wsem)

    def fetch(i):
        mcopy(i).start()
        for b in range(i * PER, (i + 1) * PER):
            for t in range(NTR):
                xcopy(b, t).start()

    for copy in smalls[:3]:
        copy.wait()
    fetch(0)
    fetch(1)
    slots = SPAN * CAP
    row40 = lax.broadcasted_iota(jnp.int32, (slots, BLK), 0)
    lane40 = lax.broadcasted_iota(jnp.int32, (slots, BLK), 1)
    want = jnp.full((slots, BLK), -1, jnp.int32)
    for d in range(SPAN):
        for c in range(CAP):
            want = jnp.where(row40 == d * CAP + c, send_s[d, 0, c], want)
    chooser = jnp.where(want == lane40, 1.0, 0.0).astype(bf16)[:, :32]
    for a in range(ABLK):
        blocks[a * F : (a + 1) * F, :] = atm_v[:, a * BLK : (a + 1) * BLK].astype(f32)
    blocks[ABLK * F :, :] = jnp.zeros(((32 - ABLK) * F, BLK), f32)
    for k in range(F // 2):
        pair = jnp.concatenate(
            [blocks[pl.ds(2 * k, 32, stride=F), :], blocks[pl.ds(2 * k + 1, 32, stride=F), :]],
            axis=1,
        )
        chosen = jnp.dot(chooser, pair.astype(bf16), preferred_element_type=f32)
        for q in range(2):
            contrib[pl.ds(2 * k + q, slots, stride=F), :] = chosen[:, q * BLK : (q + 1) * BLK]
    for d in range(SPAN):
        rows = contrib[d * CAP * F : (d + 1) * CAP * F, :].astype(bf16)
        if FLUX_OFFSETS[d] == 0:
            arr[d] = rows
        else:
            outg[d] = rows

    for i in range(2, OBLK // PER):
        fetch(i)
    wcopy.start()

    def solve(i):
        mcopy(i).wait()
        chunk = x.at[pl.ds(i * PER, PER)]
        pltpu.make_async_copy(chunk, chunk, xsem.at[i]).wait()
        for b in range(i * PER, (i + 1) * PER):
            a1, a2 = split2(m[b])
            t = jnp.concatenate([x[b, 0], x[b, 1]], axis=1)
            b1, b2 = split2(t)
            lhs = jnp.concatenate(
                [jnp.concatenate([a1, a1], axis=1), jnp.concatenate([a2, a2], axis=1)], axis=0
            )
            rhs = jnp.concatenate([b1, b2], axis=0)
            both = jnp.dot(lhs, rhs, preferred_element_type=f32)
            solved = both[:LEV] + both[LEV:]
            row = wet_v[b : b + 1, :]
            wet = jnp.concatenate([row, row], axis=1) > 0
            base = jnp.where(wet, solved, t)
            x[b, 0] = base[:, :BLK]
            x[b, 1] = base[:, BLK:]

    greeted = len(HALO_OFFSETS)
    closing = level == LINE - 1
    for who, amount in (
        (at_relay & jnp.logical_not(closing), 2 * greeted),
        (at_relay & closing, greeted + 2),
        (at_stage, greeted + 3),
        (spot == 0, greeted - 1),
        ((spot != 0) & jnp.logical_not(at_relay) & jnp.logical_not(at_stage), greeted),
    ):
        pl.when(who)(functools.partial(pl.semaphore_wait, barrier, amount))

    def flux_copy(d):
        return pltpu.make_async_remote_copy(
            src_ref=outg.at[d], dst_ref=arr.at[d], send_sem=fs.at[d], recv_sem=fr.at[d],
            device_id=(at(FLUX_OFFSETS[d]),), device_id_type=MESH,
        )

    def to_relay(d, c):
        slot = d + 2 * c
        return pltpu.make_async_remote_copy(
            src_ref=outg.at[d], dst_ref=relay.at[slot], send_sem=fs.at[d], recv_sem=rr.at[slot],
            device_id=(theirs,), device_id_type=MESH,
        )

    def from_relay(slot):
        d, c = ((0, 0), (1, 1), (0, 1))[slot]
        return pltpu.make_async_remote_copy(
            src_ref=relay.at[slot], dst_ref=arr.at[d], send_sem=rs.at[slot], recv_sem=fr.at[d],
            device_id=(last_pair + c,), device_id_type=MESH,
        )

    def from_stage(slot):
        return pltpu.make_async_remote_copy(
            src_ref=relay.at[slot], dst_ref=relay.at[slot],
            send_sem=rs.at[slot], recv_sem=rr.at[slot],
            device_id=(mine,), device_id_type=MESH,
        )

    both = pl.ds(0, 2)
    to_relay_both = pltpu.make_async_remote_copy(
        src_ref=outg.at[both], dst_ref=relay.at[both], send_sem=fs.at[0], recv_sem=rr.at[0],
        device_id=(theirs,), device_id_type=MESH,
    )
    from_stage_both = pltpu.make_async_remote_copy(
        src_ref=relay.at[both], dst_ref=relay.at[both], send_sem=rs.at[0], recv_sem=rr.at[0],
        device_id=(mine,), device_id_type=MESH,
    )

    flux = []
    for d in range(SPAN):
        offset = FLUX_OFFSETS[d]
        if offset == 0:
            continue
        flux.append(flux_copy(d))
        if offset > 0:
            flux[-1].start()
        else:
            pl.when(spot + offset >= 0)(flux[-1].start)
            if d == 0:
                pl.when(spot == 0)(to_relay_both.start)
                pl.when(spot == 1)(to_relay(0, 1).start)

    @pl.when(at_relay)
    def _():
        to_relay_both.wait_recv()
        from_relay(0).start()
        from_relay(1).start()
        to_relay(0, 1).wait_recv()
        from_relay(2).start()

    @pl.when(at_stage)
    def _():
        to_relay_both.wait_recv()
        from_stage_both.start()
        to_relay(0, 1).wait_recv()
        from_stage(2).start()

    for i in range(OBLK // PER):
        solve(i)
    for copy in smalls[3:]:
        copy.wait()

    lane128 = lax.broadcasted_iota(jnp.int32, (BLK, BLK), 1).astype(f32)
    block32 = lax.broadcasted_iota(jnp.int32, (OBLK, BLK), 0)
    count = jnp.zeros((OBLK, BLK), f32)
    for h in range(HSPAN):
        for r in range(2):
            ghost = hg_v[2 * h + r : 2 * h + r + 1, :]
            spread = jnp.broadcast_to(ghost & (BLK - 1), (BLK, BLK)).astype(f32)
            low = jnp.where(jnp.transpose(spread) == lane128, 1.0, 0.0).astype(bf16)
            high = jnp.where(r < rows_s[0, h], ghost >> 7, -1)
            low_t[h, r * BLK : (r + 1) * BLK, :] = low
            spread = jnp.broadcast_to(high, (BLK, BLK)).astype(f32)
            high_t[h, r * BLK : (r + 1) * BLK, :] = jnp.transpose(spread).astype(bf16)
            here = jnp.where(block32 == high, 1.0, 0.0).astype(bf16)
            count = count + jnp.dot(here, low, preferred_element_type=f32)
    quarter = 0.25 * wet_v[...].astype(f32)
    quarter_o[...] = quarter
    scale[...] = 1.0 - quarter * count

    lane = lax.broadcasted_iota(jnp.int32, (OBLK, BLK), 1)
    seat = lane & 63
    target = jnp.full((OBLK, BLK), -1, jnp.int32)
    used = jnp.zeros((OBLK, BLK), jnp.int32)
    for d in range(SPAN):
        used = jnp.where(seat // CAP == d, cnt_s[0, d], used)
        for c in range(CAP):
            target = jnp.where(seat == d * CAP + c, tgt_s[d, 0, c], target)
    here = (target == block32) & (lane % CAP < used)
    place = jnp.where(here, 1.0, 0.0).astype(bf16)
    contrib[320:512, :] = jnp.zeros((192, BLK), f32)

    wcopy.wait()
    slot = lax.broadcasted_iota(jnp.int32, (32, BLK), 0) // F
    for i in range(SPAN):
        d = i + top * (SPAN - 1 - 2 * i)
        if i != SPAN // 2:
            pltpu.make_async_remote_copy(
                src_ref=outg.at[d], dst_ref=arr.at[d], send_sem=fs.at[d], recv_sem=fr.at[d],
                device_id=(at(1),), device_id_type=MESH,
            ).wait_recv()
        for g in range(2):
            c = 4 * g
            pieces = arr[d, c * F : (c + 4) * F, :].astype(f32)
            even = jnp.where(slot % 2 == 0, pieces, 0.0)
            odd = jnp.where(slot % 2 == 1, pieces, 0.0)
            lhs = jnp.concatenate([even, odd], axis=1).astype(bf16)
            rhs = jnp.concatenate(
                [
                    jnp.concatenate([w[d, c], w[d, c + 2]], axis=1),
                    jnp.concatenate([w[d, c + 1], w[d, c + 3]], axis=1),
                ],
                axis=0,
            )
            both = jnp.dot(lhs, rhs, preferred_element_type=f32)
            rows = pl.ds(pl.multiple_of((d * CAP + c) * F, 4 * F), 4 * F)
            contrib[rows, :] = jnp.where(slot < 2, both[:, :BLK], both[:, BLK:])

    wetf = wet_v[...].astype(f32)
    acc = [jnp.zeros((OBLK, BLK), f32) for _ in range(NTR)]
    for k in range(F // 2):
        pair = jnp.concatenate(
            [contrib[pl.ds(2 * k, 64, stride=F), :], contrib[pl.ds(2 * k + 1, 64, stride=F), :]],
            axis=1,
        )
        halves = jnp.concatenate(split2(pair), axis=0)
        total = jnp.dot(place, halves, preferred_element_type=f32)
        for q in range(2):
            f = 2 * k + q
            flux_f = total[:, q * BLK : (q + 1) * BLK] * wetf
            ofs[pl.ds(f, OBLK, stride=F), :] = flux_f
            for t in range(NTR):
                acc[t] = acc[t] + coup_s[t, f] * flux_f
    for t in range(NTR):
        surf[t] = acc[t]

    sub = lax.broadcasted_iota(jnp.int32, (BLK, 2 * BLK), 0)

    def halo_copy(h, t=None):
        offset = h - 2 + h // 2
        return pltpu.make_async_remote_copy(
            src_ref=hout.at[h] if t is None else hout.at[h, t],
            dst_ref=v.at[h] if t is None else v.at[h, t],
            send_sem=hsend.at[h], recv_sem=hrecv.at[h],
            device_id=(at(offset),), device_id_type=MESH,
        )

    for n, h in enumerate(sends):
        row = jnp.concatenate([hs_v[pl.ds(2 * h, 1), :], hs_v[pl.ds(2 * h + 1, 1), :]], axis=1)
        low = jnp.where(sub == (row & (BLK - 1)), 1.0, 0.0).astype(bf16)
        high = jnp.broadcast_to((row >> 7).astype(f32), (BLK, 2 * BLK)).astype(bf16)
        for part in ((0,), (1,)) if n == 0 else ((0, 1),):
            rows = slice(part[0] * LEV, (part[-1] + 1) * LEV)
            picked = jnp.zeros((len(part) * LEV, 2 * BLK), f32)
            for k in range(OBLK // 2):
                tables, tiles = [], []
                for b in (2 * k, 2 * k + 1):
                    tables.append(jnp.where(high == jnp.array(b, bf16), low, jnp.zeros_like(low)))
                    if n < 3:
                        first = jnp.broadcast_to(m[b, :, 0:1], (LEV, BLK))
                    if n == 0:
                        for t in part:
                            mixed = x[b, t] + first * surf[t, b : b + 1, :]
                            tiles.append(mixed.astype(bf16))
                    elif n < 3:
                        t = n - 1
                        mixed = x[b, t] + first * surf[t, b : b + 1, :]
                        x[b, t] = mixed * scale[b : b + 1, :]
                if n == 0:
                    tile = jnp.concatenate(tiles, axis=1)
                    sent[k, rows] = tile
                else:
                    tile = sent[k, rows]
                found = jnp.dot(
                    tile, jnp.concatenate(tables, axis=0), preferred_element_type=f32
                )
                picked = jnp.where((row >> 8) == k, found, picked)
            for j, t in enumerate(part):
                hout[h, t] = picked[j * LEV : (j + 1) * LEV].astype(bf16)
            halo_copy(h, part[0] if n == 0 else None).start()

    for b in range(OBLK):
        line[:, b * BLK : (b + 1) * BLK] = ofs[b * F : (b + 1) * F, :]
    last = order[-1]
    last_low[...] = low_t[last]
    last_high[...] = high_t[last]

    for h in order[:-1]:
        halo_copy(h).wait_recv()
        values = jnp.concatenate([v[h, 0], v[h, 1]], axis=0)
        add_values(x, values, low_t[h], high_t[h], quarter_o)
    halo_copy(last).wait_recv()
    for t in range(NTR):
        last_v[t * LEV : (t + 1) * LEV] = v[last, t]
    pl.when(spot == 0)(to_relay_both.wait_send)
    for copy in flux[:2]:
        pl.when(spot != 0)(copy.wait_send)
    for copy in flux[2:]:
        copy.wait_send()

    @pl.when(at_relay)
    def _():
        for slot in range(3):
            from_relay(slot).wait_send()

    @pl.when(at_stage)
    def _():
        from_stage_both.wait_send()
        from_stage(2).wait_send()

    for h in order:
        halo_copy(h).wait_send()


def add_values(x, values, low, high, quarter_v, out=None, ready=None):
    out = x if out is None else out
    for k in range(OBLK // 2):
        tables = []
        for b in (2 * k, 2 * k + 1):
            here = high == jnp.array(b, bf16)
            tables.append(jnp.where(here, low, jnp.zeros_like(low)))
        total = jnp.dot(values, jnp.concatenate(tables, axis=1), preferred_element_type=f32)
        for j, b in enumerate((2 * k, 2 * k + 1)):
            weight = quarter_v[b : b + 1, :]
            for t in range(NTR):
                piece = total[t * LEV : (t + 1) * LEV, j * BLK : (j + 1) * BLK]
                out[b, t] = x[b, t] + weight * piece
                if ready is not None:
                    ready(b, t)


def scatter(x, line, values_v, low_v, high_v, quarter_v, flux_o, out_o, stage, sem, fsem):
    fcopy = pltpu.make_async_copy(line, flux_o, fsem)
    fcopy.start()

    def ready(b, t):
        cols = slice(b * BLK, (b + 1) * BLK)
        pltpu.make_async_copy(stage.at[b, t], out_o.at[t, :, cols], sem).start()

    add_values(x, values_v[...], low_v[...], high_v[...], quarter_v, stage, ready)
    pltpu.make_async_copy(out_o, out_o, sem).wait()
    fcopy.wait()


def body(
    atm_flux, remap_send, remap_target, remap_counts, remap_weights, coupling,
    tracer, wet, mix_inverse, halo_send, halo_ghost, halo_rows,
):
    size = lax.axis_size("patch")
    far = lambda a: pltpu.with_memory_space_constraint(a, pltpu.HBM)
    vmem = pl.BlockSpec(memory_space=pltpu.VMEM)
    hbm = pl.BlockSpec(memory_space=pltpu.HBM)
    dma = pltpu.SemaphoreType.DMA
    i32 = jnp.int32
    picks = 2 * BLK
    between = pl.pallas_call(
        functools.partial(couple, size),
        name="couple",
        out_shape=(
            jax.ShapeDtypeStruct((OBLK, NTR, LEV, BLK), f32),
            jax.ShapeDtypeStruct((F, OC), f32),
            jax.ShapeDtypeStruct((NTR * LEV, picks), bf16),
            jax.ShapeDtypeStruct((picks, BLK), bf16),
            jax.ShapeDtypeStruct((picks, BLK), bf16),
            jax.ShapeDtypeStruct((OBLK, BLK), f32),
        ),
        in_specs=[hbm] * 12,
        out_specs=(vmem,) * 6,
        scratch_shapes=[
            pltpu.SMEM((SPAN, 1, CAP), i32),
            pltpu.SMEM((SPAN, 1, CAP), i32),
            pltpu.SMEM((1, SPAN), i32),
            pltpu.SMEM((NTR, F), f32),
            pltpu.SMEM((1, HSPAN), i32),
            pltpu.VMEM((F, ABLK * BLK), bf16),
            pltpu.VMEM((2 * HSPAN, BLK), i32),
            pltpu.VMEM((2 * HSPAN, BLK), i32),
            pltpu.VMEM((OBLK, BLK), i32),
            pltpu.VMEM((OBLK, LEV, LEV), f32),
            pltpu.VMEM((SPAN, CAP, BLK, BLK), bf16),
            pltpu.VMEM((32 * F, BLK), f32),
            pltpu.VMEM((SPAN, CAP * F, BLK), bf16),
            pltpu.VMEM((3, CAP * F, BLK), bf16),
            pltpu.VMEM((SPAN, CAP * F, BLK), bf16),
            pltpu.VMEM((64 * F, BLK), f32),
            pltpu.VMEM((OBLK * F, BLK), f32),
            pltpu.VMEM((NTR, OBLK, BLK), f32),
            pltpu.VMEM((OBLK, BLK), f32),
            pltpu.VMEM((OBLK // 2, NTR * LEV, 2 * BLK), bf16),
            pltpu.VMEM((HSPAN, picks, BLK), bf16),
            pltpu.VMEM((HSPAN, picks, BLK), bf16),
            pltpu.VMEM((HSPAN, NTR, LEV, picks), bf16),
            pltpu.VMEM((HSPAN, NTR, LEV, picks), bf16),
            dma((9,)), dma((OBLK // PER,)), dma((OBLK // PER,)), dma(()),
            dma((SPAN,)), dma((SPAN,)), dma((3,)), dma((3,)), dma((HSPAN,)), dma((HSPAN,)),
        ],
        compiler_params=pltpu.CompilerParams(
            collective_id=0, has_side_effects=True, vmem_limit_bytes=24 * 1024 * 1024
        ),
    )(
        far(jnp.transpose(remap_send, (1, 0, 2))), far(jnp.transpose(remap_target, (1, 0, 2))),
        far(remap_counts), far(coupling), far(halo_rows), far(atm_flux),
        far(halo_send.reshape(2 * HSPAN, BLK)), far(halo_ghost.reshape(2 * HSPAN, BLK)),
        far(wet.reshape(OBLK, BLK)), far(tracer), far(mix_inverse),
        far(remap_weights.reshape(SPAN, CAP, BLK, BLK)),
    )
    return pl.pallas_call(
        scatter,
        name="scatter",
        out_shape=(
            jax.ShapeDtypeStruct((F, OC), f32),
            jax.ShapeDtypeStruct((NTR, LEV, OC), f32),
        ),
        in_specs=[vmem] * 6,
        out_specs=(hbm, hbm),
        scratch_shapes=[pltpu.VMEM((OBLK, NTR, LEV, BLK), f32), dma(()), dma(())],
        compiler_params=pltpu.CompilerParams(vmem_limit_bytes=16 * 1024 * 1024),
    )(*between)


def solution(mesh):
    return jax.shard_map(
        body,
        mesh=mesh,
        in_specs=(
            P(None, "patch"),
            P("patch", None, None),
            P("patch", None, None),
            P("patch", None),
            P("patch", None, None, None, None),
            P(),
            P(None, None, "patch"),
            P("patch"),
            P("patch", None, None),
            P("patch", None, None, None),
            P("patch", None, None, None),
            P("patch", None),
        ),
        out_specs=(P(None, "patch"), P(None, None, "patch")),
        check_vma=False,
    )
```
